32 devices in a mesh: gx: 4 (over y, core), gy: 8 (over z, x).
Axes of the slice: x: 2, y: 2, z: 4, core: 2. Of those that a mesh axis runs over, the one named last changes fastest.
Arguments:
- forcing: float32 [2, 20, 64, 1024], P(None, None, 'gx', 'gy'), may hold values from -6 to 6
- viscosity: float32 [20, 64, 1024], P(None, 'gx', 'gy'), may hold values from 0.5 to 8
- spread: float32 [20, 64, 1024], P(None, 'gx', 'gy'), may hold values from 0.2 to 2
- coupling: float32 [64, 1024], P('gx', 'gy'), may hold values from -0.5 to 0.5
- friction: float32 [64, 1024], P('gx', 'gy'), may hold values from 0.05 to 5
- ice_mask: int32 [64, 1024], P('gx', 'gy'), may hold values 0 or 1
- aggregates: int32 [64, 1024], P('gx', 'gy'), may hold values from 0 to 127, as said below
Outputs:
- solution: float32 [2, 20, 64, 1024], P(None, None, 'gx', 'gy')
- residual: float32 [2, 20, 64, 1024], P(None, None, 'gx', 'gy')
The draws below stay inside these ranges and needn't reach their ends.
Inputs may be any that keep to these rules, and one draw needn't show every extreme that they name: `aggregates`: within each device block of 16 x 128 columns, every number from 0 to 127 names some columns of that block.
All inputs are finite; a program needn't handle non-finite values. No bound on the sum of `ice_mask` on one device may be relied on, other than what follows from the above.
Results may differ from the reference program's by a relative error of at most 0.0013.
Values sent between devices are 32-bit elements; how exact they have to be, the bound alone decides.
No kernel may reach another device: no remote copies, remote signals or barrier semaphores. Data moves between devices by JAX's collectives and lax.ppermute only.
A program may use at most 128 MiB of HBM per device.

```python
import math
import jax
import jax.numpy as jnp
from jax import lax

CX = 16
CY = 128
L = 20
ITERS = 3
SWEEPS = 2
CSWEEPS = 4
AGG_DEV = 128
NX = 64
NY = 1024
N_GX = 4
N_GY = 8


def draw_aggregates(key, part):
    local_rows = lax.broadcasted_iota(jnp.int32, (NX, NY), 0) % CX
    local_cols = lax.broadcasted_iota(jnp.int32, (NX, NY), 1) % CY
    move_code = jax.random.randint(key, (NX, NY), 0, 12)
    row_step = jnp.where(move_code == 0, 4, jnp.where(move_code == 1, -4, 0))
    col_step = jnp.where(move_code == 2, 4, jnp.where(move_code == 3, -4, 0))
    centre = (local_rows % 4 == 1) & (local_cols % 4 == 1)
    row_step = jnp.where(centre, 0, row_step)
    col_step = jnp.where(centre, 0, col_step)
    moved_row = jnp.clip(local_rows + row_step, 0, CX - 1)
    moved_col = jnp.clip(local_cols + col_step, 0, CY - 1)
    return (moved_row // 4 * (CY // 4) + moved_col // 4).astype(jnp.int32)


def draw_forcing(key, part):
    rough_key = jax.random.fold_in(key, 11)
    phase_key = jax.random.fold_in(key, 12)
    amp_key = jax.random.fold_in(key, 13)
    first = (lax.broadcasted_iota(jnp.float32, (NX, NY), 0) + 0.5) / NX
    second = (lax.broadcasted_iota(jnp.float32, (NX, NY), 1) + 0.5) / NY
    phases = jax.random.uniform(phase_key, (2, 2), jnp.float32, 0.0, 2.0 * math.pi)
    amounts = jax.random.uniform(amp_key, (2,), jnp.float32, 0.5, 1.0)
    shape_first = jnp.cos(2.0 * math.pi * first + phases[0, 0]) * jnp.cos(2.0 * math.pi * second + phases[0, 1])
    shape_second = jnp.cos(2.0 * math.pi * first + phases[1, 0]) * jnp.cos(4.0 * math.pi * second + phases[1, 1])
    rough = jax.random.truncated_normal(rough_key, -5.0, 5.0, (2, L, NX, NY), jnp.float32)
    smooth = jnp.stack([amounts[0] * 0.6 * (1.0 + 0.5 * shape_first), amounts[1] * 0.4 * shape_second])
    return (rough + smooth[:, None]).astype(jnp.float32)


def place_ends(drawn, rng, low, high):
    longest = drawn.shape.index(max(drawn.shape))
    spots = []
    for shift in (0, 1):
        where = [jax.random.randint(jax.random.fold_in(rng, axis), (), 0, length) for axis, length in enumerate(drawn.shape)]
        where[longest] = (where[longest] + shift) % drawn.shape[longest]
        spots.append(tuple(where))
    return drawn.at[spots[0]].set(low).at[spots[1]].set(high)


def level_of(key, extent, pieces, low, high):
    def one(position, blocks):
        heights = jax.random.uniform(jax.random.fold_in(jax.random.fold_in(key, 6), position), (blocks,), jnp.float32, low / len(pieces), high / len(pieces))
        return jnp.repeat(jnp.exp(heights), extent[position] // blocks).reshape((-1,) + (1,) * (len(extent) - position - 1))

    factor_of = one(*pieces[0])
    for cut in pieces[1:]:
        factor_of = factor_of * one(*cut)
    return factor_of


def setup_inputs(seed: int = 0) -> dict:
    splits = jax.random.split(jax.random.key(seed), 8)
    return {
        "forcing": draw_forcing(jax.random.fold_in(splits[7], 71), 0),
        "viscosity": jnp.clip(jnp.exp(math.log(8.0) - 2.7725887 * jax.random.uniform(splits[1], (L, NX, NY), jnp.float32) ** level_of(splits[1], (L, NX, NY), ((1, 4), (2, 8)), -0.2, 0.2)), 0.5, 8.0),
        "spread": jnp.clip(jnp.exp(math.log(2.0) - 2.3025851 * jax.random.uniform(splits[2], (L, NX, NY), jnp.float32) ** level_of(splits[2], (L, NX, NY), ((1, 4), (2, 8)), -0.2, 0.2)), 0.2, 2.0),
        "coupling": jnp.clip(jax.random.uniform(splits[3], (NX, NY), jnp.float32, -0.5, 0.5) * level_of(splits[3], (NX, NY), ((0, 4), (1, 8)), -0.4, 0.0), -0.5, 0.5),
        "friction": jnp.clip(jnp.exp(math.log(5.0) - 4.6051702 * jax.random.uniform(splits[4], (NX, NY), jnp.float32) ** level_of(splits[4], (NX, NY), ((0, 4), (1, 8)), -0.2, 0.2)), 0.05, 5.0),
        "ice_mask": place_ends((jax.random.randint(splits[5], (NX, NY), 0, 32) < 31).astype(jnp.int32), jax.random.fold_in(splits[5], 1), 0, 1),
        "aggregates": draw_aggregates(jax.random.fold_in(splits[7], 71), 0),
    }


LINE_WEIGHT = 0.8
POINT_WEIGHT = 0.7
COARSE_WEIGHT = 0.7

def beside_all(padded):
    return (padded[..., 2:, 1:-1], padded[..., :-2, 1:-1], padded[..., 1:-1, 2:], padded[..., 1:-1, :-2])

def fine_coefficients(viscosity, spread, coupling, friction, ice_float, mask_padded):
    east_mask, west_mask, north_mask, south_mask = beside_all(mask_padded)
    vertical = 0.5 * (viscosity[:-1] + viscosity[1:]) * ice_float
    face_total = jnp.pad(vertical, ((0, 1), (0, 0), (0, 0))) + jnp.pad(vertical, ((1, 0), (0, 0), (0, 0)))
    bottom = jnp.pad(friction[None], ((0, viscosity.shape[0] - 1), (0, 0), (0, 0)))
    diagonal = ice_float * (face_total + 4.0 * spread + bottom) + (1.0 - ice_float)
    owned_spread = spread * ice_float
    return (diagonal, vertical, owned_spread * east_mask, owned_spread * west_mask, owned_spread * north_mask, owned_spread * south_mask, bottom * coupling * ice_float)

def group_layers(level_coefs, group_size):
    diagonal, vertical, to_east, to_west, to_north, to_south, crossed = level_coefs
    group_count = diagonal.shape[0] // group_size

    def fold_layers(values):
        return values.reshape((group_count, group_size) + values.shape[1:]).sum(axis=1)
    padded = jnp.concatenate([vertical, jnp.zeros_like(diagonal[:1])], axis=0)
    blocks = padded.reshape((group_count, group_size) + padded.shape[1:])
    inner_sum = blocks[:, :group_size - 1].sum(axis=1)
    return (fold_layers(diagonal) - 2.0 * inner_sum, blocks[:-1, group_size - 1], fold_layers(to_east), fold_layers(to_west), fold_layers(to_north), fold_layers(to_south), fold_layers(crossed))

def apply_stencil(level_coefs, grid_field, padded):
    diagonal, vertical, to_east, to_west, to_north, to_south, crossed = level_coefs
    east_value, west_value, north_value, south_value = beside_all(padded)
    result = diagonal * grid_field + crossed * grid_field[::-1] - (to_east * east_value + to_west * west_value + to_north * north_value + to_south * south_value)
    if vertical.shape[0] > 0:
        upward = vertical * grid_field[:, 1:]
        downward = vertical * grid_field[:, :-1]
        result = result - (jnp.pad(upward, ((0, 0), (0, 1), (0, 0), (0, 0))) + jnp.pad(downward, ((0, 0), (1, 0), (0, 0), (0, 0))))
    return result

def line_factor(level_coefs):
    diagonal, vertical = (level_coefs[0], level_coefs[1])
    inverse = [1.0 / diagonal[0]]
    upper = []
    for layer_at in range(1, diagonal.shape[0]):
        ratio_value = -vertical[layer_at - 1] * inverse[-1]
        upper.append(ratio_value)
        inverse.append(1.0 / (diagonal[layer_at] + vertical[layer_at - 1] * ratio_value))
    return (inverse, upper, vertical)

def line_solve(factor, right_side):
    inverse, upper, vertical = factor
    layers = len(inverse)
    forward = [right_side[:, 0] * inverse[0]]
    for layer_at in range(1, layers):
        forward.append((right_side[:, layer_at] + vertical[layer_at - 1] * forward[-1]) * inverse[layer_at])
    backward = [forward[-1]]
    for layer_at in range(layers - 2, -1, -1):
        backward.append(forward[layer_at] - upper[layer_at] * backward[-1])
    return jnp.stack(backward[::-1], axis=1)

def group_sum(grid_field, group_size):
    return grid_field.reshape((2, grid_field.shape[1] // group_size, group_size) + grid_field.shape[2:]).sum(axis=2)

def expand_layers(grid_field, group_size):
    return jnp.repeat(grid_field, group_size, axis=1)

def point_diagonal(column_coefs, group_ids, group_count):
    ids_padded = jnp.pad(group_ids, 1, constant_values=-1)
    east_id, west_id, north_id, south_id = beside_all(ids_padded)
    inner_sum = jnp.where(east_id == group_ids, column_coefs[2][0], 0.0) + jnp.where(west_id == group_ids, column_coefs[3][0], 0.0) + jnp.where(north_id == group_ids, column_coefs[4][0], 0.0) + jnp.where(south_id == group_ids, column_coefs[5][0], 0.0)
    return jax.ops.segment_sum((column_coefs[0][0] - inner_sum).reshape(-1), group_ids.reshape(-1), num_segments=group_count)

def coarse_coefficients(column_coefs, blocks_first, blocks_second):
    diagonal, vertical, to_east, to_west, to_north, to_south, crossed = column_coefs

    def split_block(values):
        plane = values[0]
        return plane.reshape(blocks_first, plane.shape[0] // blocks_first, blocks_second, plane.shape[1] // blocks_second)
    east_block = split_block(to_east)
    west_block = split_block(to_west)
    north_block = split_block(to_north)
    south_block = split_block(to_south)
    inner_sum = east_block[:, :-1].sum(axis=(1, 3)) + west_block[:, 1:].sum(axis=(1, 3)) + north_block[:, :, :, :-1].sum(axis=(1, 3)) + south_block[:, :, :, 1:].sum(axis=(1, 3))
    return (split_block(diagonal).sum(axis=(1, 3)) - inner_sum, split_block(crossed).sum(axis=(1, 3)), east_block[:, -1].sum(axis=2), west_block[:, 0].sum(axis=2), north_block[:, :, :, -1].sum(axis=1), south_block[:, :, :, 0].sum(axis=1))

def coarse_apply(block_table, grid_field, padded):
    diagonal, crossed, to_east, to_west, to_north, to_south = block_table
    east_value, west_value, north_value, south_value = beside_all(padded)
    return diagonal * grid_field + crossed * grid_field[::-1] - (to_east * east_value + to_west * west_value + to_north * north_value + to_south * south_value)

def coarse_jacobi(block_table, right_side, widen_rim):
    answer = COARSE_WEIGHT * right_side / block_table[0]
    for sweep_at in range(CSWEEPS - 1):
        answer = answer + COARSE_WEIGHT * (right_side - coarse_apply(block_table, answer, widen_rim(answer))) / block_table[0]
    return answer

def least_squares(columns, initial_norm):
    steps_count = len(columns)
    matrix_rows = [[columns[column_at][row_at] for column_at in range(steps_count)] for row_at in range(steps_count + 1)]
    target = [initial_norm] + [jnp.zeros_like(initial_norm) for row_at in range(steps_count)]
    for pivot_at in range(steps_count):
        top_value = matrix_rows[pivot_at][pivot_at]
        low_value = matrix_rows[pivot_at + 1][pivot_at]
        radius = jnp.sqrt(top_value * top_value + low_value * low_value)
        cosine = top_value / radius
        sine_value = low_value / radius
        for column_at in range(pivot_at, steps_count):
            upper_entry = matrix_rows[pivot_at][column_at]
            lower_entry = matrix_rows[pivot_at + 1][column_at]
            matrix_rows[pivot_at][column_at] = cosine * upper_entry + sine_value * lower_entry
            matrix_rows[pivot_at + 1][column_at] = cosine * lower_entry - sine_value * upper_entry
        upper_entry = target[pivot_at]
        lower_entry = target[pivot_at + 1]
        target[pivot_at] = cosine * upper_entry + sine_value * lower_entry
        target[pivot_at + 1] = cosine * lower_entry - sine_value * upper_entry
    weights = [None] * steps_count
    for pivot_at in reversed(range(steps_count)):
        partial_sum = target[pivot_at]
        for column_at in range(pivot_at + 1, steps_count):
            partial_sum = partial_sum - matrix_rows[pivot_at][column_at] * weights[column_at]
        weights[pivot_at] = partial_sum / matrix_rows[pivot_at][pivot_at]
    return weights

def reference(forcing, viscosity, spread, coupling, friction, ice_mask, aggregates):
    ice_float = ice_mask.astype(jnp.float32)
    fine_coefs = fine_coefficients(viscosity, spread, coupling, friction, ice_float, jnp.pad(ice_float, 1))
    middle = group_layers(fine_coefs, 2)
    column = group_layers(middle, L // 2)
    stencils = [fine_coefs, middle, column]
    factors = [line_factor(level_coefs) for level_coefs in stencils]
    device_rows = lax.broadcasted_iota(jnp.int32, (NX, NY), 0) // CX
    device_cols = lax.broadcasted_iota(jnp.int32, (NX, NY), 1) // CY
    group_ids = (aggregates + (device_rows * N_GY + device_cols) * AGG_DEV).astype(jnp.int32)
    total_groups = N_GX * N_GY * AGG_DEV
    ids_flat = group_ids.reshape(-1)
    point_diag = point_diagonal(column, group_ids, total_groups)
    block_table = coarse_coefficients(column, N_GX, N_GY)

    def apply_level(level_number, grid_field):
        padded = jnp.pad(grid_field, ((0, 0), (0, 0), (1, 1), (1, 1)))
        return apply_stencil(stencils[level_number], grid_field, padded)

    def restrict_points(grid_field):
        flattened = grid_field.reshape(2, -1)
        return jnp.stack([jax.ops.segment_sum(flattened[0], ids_flat, num_segments=total_groups), jax.ops.segment_sum(flattened[1], ids_flat, num_segments=total_groups)])

    def prolong_points(values):
        return values[:, ids_flat].reshape(2, 1, NX, NY)

    def point_apply(values):
        return restrict_points(apply_level(2, prolong_points(values)))

    def local_widen(values):
        return jnp.pad(values, ((0, 0), (1, 1), (1, 1)))

    def coarse_correction(values):
        coarse_rhs = values.reshape(2, N_GX, N_GY, AGG_DEV).sum(axis=3)
        answer = coarse_jacobi(block_table, coarse_rhs, local_widen)
        return jnp.repeat(answer.reshape(2, -1), AGG_DEV, axis=1)

    def point_cycle(right_side):
        answer = POINT_WEIGHT * right_side / point_diag
        for sweep_at in range(SWEEPS - 1):
            answer = answer + POINT_WEIGHT * (right_side - point_apply(answer)) / point_diag
        answer = answer + coarse_correction(right_side - point_apply(answer))
        for sweep_at in range(SWEEPS):
            answer = answer + POINT_WEIGHT * (right_side - point_apply(answer)) / point_diag
        return answer

    def line_cycle(level_number, right_side):
        factor = factors[level_number]
        answer = LINE_WEIGHT * line_solve(factor, right_side)
        for sweep_at in range(SWEEPS - 1):
            answer = answer + LINE_WEIGHT * line_solve(factor, right_side - apply_level(level_number, answer))
        leftover = right_side - apply_level(level_number, answer)
        if level_number == 0:
            answer = answer + expand_layers(line_cycle(1, group_sum(leftover, 2)), 2)
        elif level_number == 1:
            depth_count = leftover.shape[1]
            answer = answer + expand_layers(line_cycle(2, group_sum(leftover, depth_count)), depth_count)
        else:
            answer = answer + prolong_points(point_cycle(restrict_points(leftover)))
        for sweep_at in range(SWEEPS):
            answer = answer + LINE_WEIGHT * line_solve(factor, right_side - apply_level(level_number, answer))
        return answer
    initial_norm = jnp.sqrt(jnp.sum(forcing * forcing))
    basis = [forcing / initial_norm]
    stored = []
    columns = []
    for step_at in range(ITERS):
        search = line_cycle(0, basis[step_at])
        stored.append(search)
        image = apply_level(0, search)
        projected = [jnp.sum(vector * image) for vector in basis]
        for index_at in range(len(basis)):
            image = image - projected[index_at] * basis[index_at]
        height = jnp.sqrt(jnp.sum(image * image))
        columns.append(projected + [height] + [jnp.zeros_like(height) for row_at in range(ITERS - 1 - step_at)])
        if step_at + 1 < ITERS:
            basis.append(image / height)
    weights = least_squares(columns, initial_norm)
    solution = weights[0] * stored[0]
    for index_at in range(1, ITERS):
        solution = solution + weights[index_at] * stored[index_at]
    residual = forcing - apply_level(0, solution)
    return (solution, residual)
```

```python
import functools

import jax
import jax.numpy as jnp
from jax import lax
from jax.experimental import pallas as pl
from jax.experimental.pallas import tpu as pltpu
from jax.sharding import PartitionSpec as P

ITERS = 3
LINE_WEIGHT = 0.8
POINT_WEIGHT = 0.7
COARSE_WEIGHT = 0.7
CSWEEPS = 4
REACH = 13 * ITERS + 1

VMEM = pl.BlockSpec(memory_space=pltpu.VMEM)
SMEM = pl.BlockSpec(memory_space=pltpu.SMEM)
F32 = jnp.float32


def call(kernel, outs, args, scratch=(), name=None):
    specs = [SMEM if a.dtype == jnp.int32 and a.ndim == 1 else VMEM for a in args]
    return pl.pallas_call(
        kernel,
        out_shape=[jax.ShapeDtypeStruct(s, F32) for s in outs],
        in_specs=specs,
        out_specs=[VMEM] * len(outs),
        scratch_shapes=[pltpu.VMEM(s, F32) for s in scratch],
        name=name,
    )(*args)


class Dims:
    def __init__(self, ngx, ngy, layers, cx, cy):
        self.ngx, self.ngy, self.n = ngx, ngy, ngx * ngy
        self.layers, self.cx, self.cy = layers, cx, cy
        self.rows = ngx * cx
        self.strip = cy // ngx
        self.halo = (cy - self.strip) // 2
        self.groups = self.rows // 8
        self.slots = cy // REACH
        self.packed = -(-self.groups // self.slots)
        self.planes = 4 * layers + 4
        self.parts = -(-2 * ngx // 8) * 8


def lanes(shape):
    return lax.broadcasted_iota(jnp.int32, shape, len(shape) - 1)


def turn(x, shift, axis):
    return pltpu.roll(x, shift, axis)


class Level:
    def __init__(self, d, n, g, s, inv, face, cross, mask, mu, fw):
        self.d, self.n, self.g, self.s, self.inv, self.face = d, n, g, s, inv, face
        self.cross, self.mask, self.mu, self.fw = cross, mask, mu, fw

    def clear_rim(self):
        rows, cy = self.d.rows, self.d.cy
        for v in range(2):
            self.mu[v, :, 0:8, :] = jnp.zeros((self.n, 8, cy), F32)
            self.mu[v, :, 8 + rows : 16 + rows, :] = jnp.zeros((self.n, 8, cy), F32)

    def put_masked(self, v, k, value):
        self.mu[v, k, 8 : 8 + self.d.rows, :] = self.mask[...] * value

    def beside(self, v, k):
        rows, cy = self.d.rows, self.d.cy
        here = self.mu[v, k, 8 : 8 + rows, :]
        return (
            self.mu[v, k, 7 : 7 + rows, :]
            + self.mu[v, k, 9 : 9 + rows, :]
            + (turn(here, 1, 1) + turn(here, cy - 1, 1))
        )

    def apply(self, u, v, k, bottom=False):
        out = self.g[k] * u[v, k] - self.s[k] * self.beside(v, k)
        if self.n > 1:
            above = jnp.minimum(k + 1, self.n - 1)
            below = jnp.maximum(k - 1, 0)
            out = out - (self.face[k + 1] * u[v, above] + self.face[k] * u[v, below])
        if bottom:
            out = out + self.cross[...] * u[1 - v, k]
        return out

    def sweep(self, r, u, first=False):
        n = self.n
        start = []
        for v in range(2):
            right = r[v, 0]
            if not first:
                right = right - self.apply(u, v, 0, True)
            start.append(right * self.inv[0])
        for v in range(2):
            self.fw[v, 0] = start[v]

        def forward(k, carry):
            out = []
            for v in range(2):
                right = r[v, k]
                if not first:
                    right = right - self.apply(u, v, k)
                value = (right + self.face[k] * carry[v]) * self.inv[k]
                self.fw[v, k] = value
                out.append(value)
            return tuple(out)

        last = lax.fori_loop(1, n, forward, tuple(start)) if n > 1 else tuple(start)

        def store(v, k, value):
            new = LINE_WEIGHT * value
            if not first:
                new = u[v, k] + new
            u[v, k] = new
            self.put_masked(v, k, new)

        for v in range(2):
            store(v, n - 1, last[v])

        def backward(t, carry):
            k = n - 1 - t
            out = []
            factor = self.face[k + 1] * self.inv[k]
            for v in range(2):
                value = self.fw[v, k] + factor * carry[v]
                store(v, k, value)
                out.append(value)
            return tuple(out)

        if n > 1:
            lax.fori_loop(1, n, backward, last)


def level_set(d, coefs, mu0, fw0, mu1, fw1, mu2, fw2):
    g0, s0, i0, f0, g1, s1, i1, f1, low = coefs
    cross, mask = low.at[3], low.at[4]
    rows = d.rows
    one = lambda at: low.at[at : at + 1]
    return (
        Level(d, d.layers, g0, s0, i0, f0, cross, mask, mu0, fw0),
        Level(d, d.layers // 2, g1, s1, i1, f1, cross, mask, mu1, fw1),
        Level(d, 1, one(0), one(1), one(2), None, cross, mask, mu2, fw2),
    )


def coef_shapes(d):
    n0, n1, r, c = d.layers, d.layers // 2, d.rows, d.cy
    plane = lambda n: (n, r, c)
    return [
        plane(n0), plane(n0), plane(n0), plane(n0 + 1),
        plane(n1), plane(n1), plane(n1), plane(n1 + 1),
        plane(6),
    ]


def field(d, n):
    return (2, n, d.rows, d.cy)


def work_shapes(d):
    out = []
    for n in (d.layers, d.layers // 2, 1):
        out += [(2, n, d.rows + 16, d.cy), field(d, n)]
    return out


def own_lanes(d, shape):
    lane = lanes(shape)
    return (lane >= d.halo) & (lane < d.halo + d.strip)


def segment_acc(d, ids_ref, fetch, count):
    cy = d.cy
    wanted = lax.broadcasted_iota(jnp.int32, (cy, cy), 0).astype(F32)
    acc = [jnp.zeros((cy, cy), F32) for _ in range(count)]
    for r in range(d.cx):
        hit = ids_ref[r : r + 1, :] == wanted
        for t in range(count):
            acc[t] = acc[t] + jnp.where(hit, fetch(t, r), 0.0)
    return acc


def restrict_strip(d, strip_ids, e_ref, pack, chunk):
    lane = lanes((d.cx, d.cy))
    for v in range(2):
        out = jnp.zeros((d.cx, d.cy), F32)
        for g in range(d.ngx):
            shift = (d.strip * g - d.halo) % d.cy
            part = turn(e_ref[v, g * d.cx : (g + 1) * d.cx, :], shift, 1)
            out = jnp.where(lane // d.strip == g, part, out)
        pack[v] = out
    acc = segment_acc(d, strip_ids, lambda t, r: pack[t, r : r + 1, :], 2)
    for v in range(2):
        sums = acc[v].T.reshape(d.ngx, d.strip, d.cy).sum(axis=1)
        chunk[v * d.ngx : (v + 1) * d.ngx, :] = sums


def descend(d, levels, r0, u0, r1, u1, r2, u2, strip_ids, e2, pack, chunk):
    l0, l1, l2 = levels
    half = l0.n // 2
    l0.sweep(r0, u0, first=True)
    l0.sweep(r0, u0)

    def residual_pair(kk, bottom):
        for v in range(2):
            low = r0[v, 2 * kk] - l0.apply(u0, v, 2 * kk, bottom)
            high = r0[v, 2 * kk + 1] - l0.apply(u0, v, 2 * kk + 1)
            r1[v, kk] = low + high

    residual_pair(0, True)
    lax.fori_loop(1, half, lambda k, c: (residual_pair(k, False), c)[1], 0)
    l1.sweep(r1, u1, first=True)
    l1.sweep(r1, u1)
    zero = tuple(r1[v, 0] - l1.apply(u1, v, 0, True) for v in range(2))
    total = lax.fori_loop(
        1,
        half,
        lambda k, c: tuple(c[v] + (r1[v, k] - l1.apply(u1, v, k)) for v in range(2)),
        zero,
    )
    for v in range(2):
        r2[v, 0] = total[v]
    l2.sweep(r2, u2, first=True)
    l2.sweep(r2, u2)
    for v in range(2):
        e2[v] = r2[v, 0] - l2.apply(u2, v, 0, True)
    restrict_strip(d, strip_ids, e2, pack, chunk)


def ascend(d, levels, r0, u0, r1, u1, r2, u2):
    l0, l1, l2 = levels
    for v in range(2):
        l2.put_masked(v, 0, u2[v, 0])
    for _ in range(2):
        l2.sweep(r2, u2)

    def add1(k, c):
        for v in range(2):
            value = u1[v, k] + u2[v, 0]
            u1[v, k] = value
            l1.put_masked(v, k, value)
        return c

    lax.fori_loop(0, l1.n, add1, 0)
    for _ in range(2):
        l1.sweep(r1, u1)

    def add0(k, c):
        for v in range(2):
            for p in range(2):
                value = u0[v, 2 * k + p] + u1[v, k]
                u0[v, 2 * k + p] = value
                l0.put_masked(v, 2 * k + p, value)
        return c

    lax.fori_loop(0, l1.n, add0, 0)
    for _ in range(2):
        l0.sweep(r0, u0)


def pick(row, ids):
    return jnp.take_along_axis(
        jnp.broadcast_to(row, ids.shape), ids, axis=1, mode="promise_in_bounds"
    )


def spread_chunk(d, out, chunk):
    value = chunk[...]
    for i in range(d.n):
        out[i] = value


def pack_kernel(d, place, gathered, out):
    first = place[3]

    def body(p, c):
        lane = lanes((8, d.cy))
        for o in range(d.packed):
            value = jnp.zeros((8, d.cy), F32)
            for s in range(d.slots):
                rg = o * d.slots + s
                if rg >= d.groups:
                    break
                block, at = rg * 8 // d.cx, rg * 8 % d.cx
                x = gathered[block, p, at : at + 8, :]
                x = turn(x, lax.rem(REACH * s - first + d.cy, d.cy), 1)
                keep = (lane >= REACH * s) & (lane < REACH * (s + 1))
                value = jnp.where(keep, x, value)
            out[p, o] = value
        return c

    lax.fori_loop(0, d.planes, body, 0)


def setup_kernel(d, place, gathered, packed, left, right, mine, *rest):
    (f, g0, s0, i0, f0, g1, s1, i1, f1, low, blk, strip_ids) = rest[:12]
    (u0, r1, u1, r2, u2, big) = rest[12:18]
    (win, chunk, e2, pack, mu0, fw0, mu1, fw1, mu2, fw2) = rest[18:]
    n0, n1, rows, cy, cx = d.layers, d.layers // 2, d.rows, d.cy, d.cx
    gx, off, is_left = place[1], place[4], place[5]

    def window(p, put):
        lane = lanes((8, cy))
        off_own = lax.rem(off + cy, cy)
        own = jnp.where(is_left == 1, (lane >= off).astype(jnp.int32), (lane < cy + off).astype(jnp.int32)) == 1
        lo = jnp.where(is_left == 1, off - REACH, cy + off)
        near = (lane >= lo) & (lane < lo + REACH)
        for rg in range(d.groups):
            block, at = rg * 8 // cx, rg * 8 % cx
            mid = turn(gathered[block, p, at : at + 8, :], off_own, 1)
            o, s = rg // d.slots, rg % d.slots
            side = turn(packed[p, o], lax.rem(lo - REACH * s + 2 * cy, cy), 1)
            put(rg, jnp.where(own, mid, jnp.where(near, side, 0.0)))

    def put_forcing(p, c):
        for v in range(2):
            def put(rg, value, v=v):
                f[v, p, rg * 8 : rg * 8 + 8, :] = value
            window(v * n0 + p, put)
        return c

    lax.fori_loop(0, n0, put_forcing, 0)

    def put_rest(p, c):
        def put(rg, value):
            win[p, rg * 8 : rg * 8 + 8, :] = value
        window(2 * n0 + p, put)
        return c

    lax.fori_loop(0, 2 * n0 + 4, put_rest, 0)

    cpl, frc, msk = win[2 * n0], win[2 * n0 + 1], win[2 * n0 + 2]
    low[4] = msk
    low[5] = win[2 * n0 + 3]
    low[3] = frc * cpl * msk
    mask = low.at[4]
    nil = jnp.zeros((rows, cy), F32)
    f0[0] = nil
    f0[n0] = nil

    def faces(k, c):
        f0[k + 1] = 0.5 * (win[k] + win[k + 1]) * mask[...]
        return c

    lax.fori_loop(0, n0 - 1, faces, 0)

    def diag(k, extra):
        m = mask[...]
        sp = win[n0 + k]
        s0[k] = sp * m
        inner = f0[k] + f0[k + 1] + 4.0 * sp
        if extra is not None:
            inner = inner + extra
        value = m * inner + (1.0 - m)
        g0[k] = value
        return value

    i0[0] = 1.0 / diag(0, frc)

    def factor0(k, prev):
        face = f0[k]
        inv = 1.0 / (diag(k, None) - face * face * prev)
        i0[k] = inv
        return inv

    lax.fori_loop(1, n0, factor0, i0[0])

    def fold(k, total):
        g1[k] = g0[2 * k] + g0[2 * k + 1] - 2.0 * f0[2 * k + 1]
        s = s0[2 * k] + s0[2 * k + 1]
        s1[k] = s
        f1[k] = f0[2 * k]
        return total + s

    low[1] = lax.fori_loop(0, n1, fold, nil)
    f1[n1] = nil
    i1[0] = 1.0 / g1[0]

    def factor1(k, prev):
        face = f1[k]
        inv = 1.0 / (g1[k] - face * face * prev)
        i1[k] = inv
        return inv

    lax.fori_loop(1, n1, factor1, i1[0])
    diag2 = 4.0 * low[1] + mask[...] * win[2 * n0 + 1] + n0 * (1.0 - mask[...])
    low[0] = diag2
    low[2] = 1.0 / diag2

    def column_sum(block):
        def add(k, t):
            return t + gathered[block, 3 * n0 + k]
        total = lax.fori_loop(0, n0, add, jnp.zeros((cx, cy), F32))
        return total * gathered[block, 4 * n0 + 2]

    prev_at, next_at = jnp.maximum(gx - 1, 0), jnp.minimum(gx + 1, d.ngx - 1)
    has_prev, has_next = (gx > 0).astype(F32), (gx < d.ngx - 1).astype(F32)
    m, ids, s2 = mine[0], mine[1], mine[2]
    fr, cp = gathered[gx, 4 * n0 + 1], gathered[gx, 4 * n0]
    row = lax.broadcasted_iota(jnp.int32, (cx, cy), 0)
    lane = lanes((cx, cy))
    prev = (gathered[prev_at, 4 * n0 + 2] * has_prev, gathered[prev_at, 4 * n0 + 3], column_sum(prev_at) * has_prev)
    after = (gathered[next_at, 4 * n0 + 2] * has_next, gathered[next_at, 4 * n0 + 3], column_sum(next_at) * has_next)
    inside = (row > 0, row < cx - 1, lane > 0, lane < cy - 1)

    def around(t, q):
        return (
            jnp.where(inside[0], turn(q, 1, 0), turn(prev[t], 1, 0)),
            jnp.where(inside[1], turn(q, cx - 1, 0), turn(after[t], cx - 1, 0)),
            jnp.where(inside[2], turn(q, 1, 1), turn(left[t], 1, 1)),
            jnp.where(inside[3], turn(q, cy - 1, 1), turn(right[t], cy - 1, 1)),
        )

    m_d, ids_d, s_d = around(0, m), around(1, ids), around(2, s2)
    g2b = 4.0 * s2 + m * fr + n0 * (1.0 - m)
    cb = fr * cp * m
    blk[0], blk[1], blk[2], blk[7] = g2b, s2, cb, ids
    weight3, weight4 = g2b, g2b
    for t in range(4):
        blk[3 + t] = m_d[t]
        blk[8 + t] = ids_d[t]
        weight3 = weight3 - jnp.where(inside[t] & (ids_d[t] == ids), s2 * m_d[t], 0.0)
        weight4 = weight4 - jnp.where(inside[t], s_d[t] * m, 0.0)
        blk[15 + t] = jnp.where(inside[t], 0.0, s_d[t] * m)
    blk[12], blk[13], blk[14] = weight3, cb, weight4
    chunk[...] = jnp.zeros(chunk.shape, F32)
    for t in range(7):
        acc = segment_acc(d, blk.at[7], lambda _, r: blk[12 + t, r : r + 1, :], 1)
        chunk[d.parts + t : d.parts + t + 1, :] = acc[0].T.sum(axis=0, keepdims=True)

    packed_ids = jnp.zeros((cx, cy), F32)
    for g in range(d.ngx):
        part = turn(low[5, g * cx : (g + 1) * cx, :], (d.strip * g - d.halo) % cy, 1)
        packed_ids = jnp.where(lane // d.strip == g, part, packed_ids)
    strip_ids[...] = packed_ids

    def square(k, t):
        return t + f[0, k] * f[0, k] + f[1, k] * f[1, k]

    total = lax.fori_loop(0, n0, square, nil)
    total = jnp.where(own_lanes(d, (rows, cy)), total, 0.0)
    chunk[d.parts + 7 : d.parts + 8, :] = total.sum(axis=0, keepdims=True)

    levels = level_set(d, (g0, s0, i0, f0, g1, s1, i1, f1, low), mu0, fw0, mu1, fw1, mu2, fw2)
    for one in levels:
        one.clear_rim()
    descend(d, levels, f, u0, r1, u1, r2, u2, strip_ids, e2, pack, chunk)
    spread_chunk(d, big, chunk)


def apply_own(d, place, y, blk, tmp, chunk):
    me, n, ngy = place[0], d.n, d.ngy
    shape = (d.cx, d.cy)
    row = lax.broadcasted_iota(jnp.int32, shape, 0)
    lane = lanes(shape)
    inside = (row > 0, row < d.cx - 1, lane > 0, lane < d.cy - 1)
    at = (
        jnp.maximum(me - ngy, 0),
        jnp.minimum(me + ngy, n - 1),
        jnp.maximum(me - 1, 0),
        jnp.minimum(me + 1, n - 1),
    )
    ids = blk[7].astype(jnp.int32)
    mine = [y[v, pl.ds(me, 1), :] for v in range(2)]
    here = [pick(mine[v], ids) for v in range(2)]
    side = [jnp.zeros(shape, F32), jnp.zeros(shape, F32)]
    for t in range(4):
        ids_t = blk[8 + t].astype(jnp.int32)
        for v in range(2):
            outer = pick(y[v, pl.ds(at[t], 1), :], ids_t)
            value = jnp.where(inside[t], pick(mine[v], ids_t), outer)
            side[v] = side[v] + blk[3 + t] * value
    for v in range(2):
        tmp[v] = blk[0] * here[v] + blk[2] * here[1 - v] - blk[1] * side[v]
    acc = segment_acc(d, blk.at[7], lambda t, r: tmp[t, r : r + 1, :], 2)
    for v in range(2):
        chunk[v : v + 1, :] = acc[v].T.sum(axis=0, keepdims=True)


def point_first(d, place, parts, table, blk, dots, y, r3, big, tmp, chunk):
    n, ngx, ngy = d.n, d.ngx, d.ngy
    for v in range(2):
        for g in range(ngx):
            total = parts[0:ngy, v * ngx + g, :]
            for i in range(1, ngx):
                total = total + parts[i * ngy : (i + 1) * ngy, v * ngx + g, :]
            r3[v, g * ngy : (g + 1) * ngy, :] = total
    diag = table[:, d.parts, :]
    for v in range(2):
        y[v] = POINT_WEIGHT * r3[v] / diag
    chunk[2:8, :] = dots[2:8, :]
    apply_own(d, place, y, blk, tmp, chunk)
    spread_chunk(d, big, chunk)


def point_middle(d, place, parts, table, blk, y_in, r3, y, big, tmp, chunk):
    n, ngy = d.n, d.ngy
    base = d.parts
    diag = table[:, base, :]
    cross = table[:, base + 1, :]
    inner = table[:, base + 2, :]
    sides = [table[:, base + 3 + t, :] for t in range(4)]
    shape = (n, d.cy)

    def total(x):
        return jnp.broadcast_to(x.sum(axis=1, keepdims=True), shape)

    def couple(values):
        return (
            turn(values[1], ngy, 0)
            + turn(values[0], n - ngy, 0)
            + turn(values[3], 1, 0)
            + turn(values[2], n - 1, 0)
        )

    y2 = [y_in[v] + POINT_WEIGHT * (r3[v] - parts[:, v, :]) / diag for v in range(2)]
    right = []
    for v in range(2):
        local = total(r3[v] - (inner * y2[v] + cross * y2[1 - v]))
        right.append(local + couple([total(s * y2[v]) for s in sides]))
    diag4, cross4 = total(inner), total(cross)
    sides4 = [total(s) for s in sides]
    x = [COARSE_WEIGHT * right[v] / diag4 for v in range(2)]
    for _ in range(CSWEEPS - 1):
        x = [
            x[v]
            + COARSE_WEIGHT
            * (right[v] - (diag4 * x[v] + cross4 * x[1 - v] - couple([s * x[v] for s in sides4])))
            / diag4
            for v in range(2)
        ]
    for v in range(2):
        y[v] = y2[v] + x[v]
    chunk[...] = jnp.zeros(chunk.shape, F32)
    apply_own(d, place, y, blk, tmp, chunk)
    spread_chunk(d, big, chunk)


def point_last(d, place, parts, table, blk, y_in, r3, y, big, tmp, chunk):
    diag = table[:, d.parts, :]
    for v in range(2):
        y[v] = y_in[v] + POINT_WEIGHT * (r3[v] - parts[:, v, :]) / diag
    chunk[...] = jnp.zeros(chunk.shape, F32)
    apply_own(d, place, y, blk, tmp, chunk)
    spread_chunk(d, big, chunk)


def correct_columns(d, place, parts, table, y_in, r3, y, low, u2):
    diag = table[:, d.parts, :]
    for v in range(2):
        y[v] = y_in[v] + POINT_WEIGHT * (r3[v] - parts[:, v, :]) / diag
    gy, off, is_left = place[2], place[4], place[5]
    shape = (d.cx, d.cy)
    lane = lanes(shape)
    own = jnp.where(is_left == 1, (lane >= off).astype(jnp.int32), (lane < d.cy + off).astype(jnp.int32)) == 1
    other = jnp.where(is_left == 1, jnp.maximum(gy - 1, 0), jnp.minimum(gy + 1, d.ngy - 1))
    for g in range(d.ngx):
        at = slice(g * d.cx, (g + 1) * d.cx)
        ids = low[5, at, :].astype(jnp.int32)
        for v in range(2):
            here = pick(y[v, pl.ds(g * d.ngy + gy, 1), :], ids)
            there = pick(y[v, pl.ds(g * d.ngy + other, 1), :], ids)
            u2[v, 0, at, :] = u2[v, 0, at, :] + jnp.where(own, here, there)


def grid_total(d, dots, row):
    x = dots[:, row, :].sum(axis=0, keepdims=True)
    return jnp.broadcast_to(x.sum(axis=1, keepdims=True), (1, d.cy))


def column_of(d, dots, step):
    inner = [grid_total(d, dots, 2 + i) for i in range(step + 1)]
    square = grid_total(d, dots, 3 + step)
    for value in inner:
        square = square - value * value
    return inner + [jnp.sqrt(square)]


def step_kernel(d, step, last, *refs):
    it = iter(refs)
    take = lambda count: [next(it) for _ in range(count)]
    (place,) = take(1)
    coefs = take(9)
    (strip_ids, r_in, u0i, r1i, u1i, r2i, u2i) = take(7)
    (parts, table, y_in, r3, dots) = take(5)
    olds_v = take(step)
    olds_z = take(step)
    (v_out, z_out, col) = take(3)
    if last:
        (dots_out, big) = take(2)
        w = take(1)[0]
        u0n = None
    else:
        (w, u0n, r1n, u1n, r2n, u2n, dots_out, big) = take(8)
    (u0, u1, u2, y, chunk, e2, pack, mu0, fw0, mu1, fw1, mu2, fw2) = take(13)
    low = coefs[8]
    levels = level_set(d, coefs, mu0, fw0, mu1, fw1, mu2, fw2)
    for one in levels:
        one.clear_rim()
    n0, n1 = d.layers, d.layers // 2

    for v in range(2):
        u2[v, 0] = u2i[v, 0]
    correct_columns(d, place, parts, table, y_in, r3, y, low, u2)

    def copy1(k, c):
        for v in range(2):
            u1[v, k] = u1i[v, k]
        return c

    def copy0(k, c):
        for v in range(2):
            u0[v, k] = u0i[v, k]
        return c

    lax.fori_loop(0, n1, copy1, 0)
    lax.fori_loop(0, n0, copy0, 0)
    ascend(d, levels, r_in, u0, r1i, u1, r2i, u2)

    if step == 0:
        norm = jnp.sqrt(grid_total(d, table, d.parts + 7))
        inner, height = [], norm
        col[...] = jnp.broadcast_to(norm, col.shape)
    else:
        column = column_of(d, dots, step - 1)
        inner, height = column[:-1], column[-1]
        for t, value in enumerate(column):
            col[t : t + 1, :] = value
    scale = 1.0 / height
    l0 = levels[0]

    def scaled(k, c):
        for v in range(2):
            vec, z = r_in[v, k], u0[v, k]
            for t in range(step):
                vec = vec - inner[t] * olds_v[t][v, k]
                z = z - inner[t] * olds_z[t][v, k]
            v_out[v, k] = vec * scale
            z = z * scale
            z_out[v, k] = z
            l0.put_masked(v, k, z)
        return c

    lax.fori_loop(0, n0, scaled, 0)
    basis = list(olds_v) + [v_out]

    def image(k, acc, bottom=False):
        acc = list(acc)
        for v in range(2):
            value = l0.apply(z_out, v, k, bottom)
            w[v, k] = value
            for t, vec in enumerate(basis):
                acc[t] = acc[t] + vec[v, k] * value
            acc[-1] = acc[-1] + value * value
        return tuple(acc)

    nil = jnp.zeros((d.rows, d.cy), F32)
    acc = image(0, (nil,) * (step + 2), True)
    acc = lax.fori_loop(1, n0, image, acc)
    own = own_lanes(d, (d.rows, d.cy))
    dots_out[...] = jnp.zeros(dots_out.shape, F32)
    for t in range(step + 2):
        dots_out[2 + t : 3 + t, :] = jnp.where(own, acc[t], 0.0).sum(axis=0, keepdims=True)
    if last:
        spread_chunk(d, big, dots_out)
    else:
        descend(d, levels, w, u0n, r1n, u1n, r2n, u2n, strip_ids, e2, pack, chunk)
        spread_chunk(d, big, chunk)


def least_squares(columns, initial_norm):
    count = len(columns)
    rows = [[columns[c][r] for c in range(count)] for r in range(count + 1)]
    target = [initial_norm] + [jnp.zeros_like(initial_norm) for _ in range(count)]
    for p in range(count):
        top, low = rows[p][p], rows[p + 1][p]
        radius = jnp.sqrt(top * top + low * low)
        cosine, sine = top / radius, low / radius
        for c in range(p, count):
            upper, lower = rows[p][c], rows[p + 1][c]
            rows[p][c] = cosine * upper + sine * lower
            rows[p + 1][c] = cosine * lower - sine * upper
        upper, lower = target[p], target[p + 1]
        target[p] = cosine * upper + sine * lower
        target[p + 1] = cosine * lower - sine * upper
    weights = [None] * count
    for p in reversed(range(count)):
        partial = target[p]
        for c in range(p + 1, count):
            partial = partial - rows[p][c] * weights[c]
        weights[p] = partial / rows[p][p]
    return weights


def final_kernel(d, g0, s0, i0, f0, low, f, dots, *refs):
    cols, zs = refs[:ITERS], refs[ITERS : 2 * ITERS]
    out, x, res, mu0 = refs[2 * ITERS :]
    n0 = d.layers
    norm = cols[0][0:1, :]
    nil = jnp.zeros_like(norm)
    columns = []
    for j in range(ITERS):
        if j + 1 < ITERS:
            column = [cols[j + 1][t : t + 1, :] for t in range(j + 2)]
        else:
            column = column_of(d, dots, j)
        columns.append(column + [nil] * (ITERS - 1 - j))
    weights = least_squares(columns, norm)
    l0 = Level(d, n0, g0, s0, i0, f0, low.at[3], low.at[4], mu0, None)
    l0.clear_rim()

    def combine(k, c):
        for v in range(2):
            value = weights[0] * zs[0][v, k]
            for j in range(1, ITERS):
                value = value + weights[j] * zs[j][v, k]
            x[v, k] = value
            l0.put_masked(v, k, value)
        return c

    lax.fori_loop(0, n0, combine, 0)

    def rest(k, bottom):
        for v in range(2):
            res[v, k] = f[v, k] - l0.apply(x, v, k, bottom)

    rest(0, True)
    lax.fori_loop(1, n0, lambda k, c: (rest(k, False), c)[1], 0)

    per = 4 * n0 // d.ngx
    lane = lanes((d.cx, d.cy))
    for q in range(d.ngx):
        shift = (d.strip * q - d.halo) % d.cy
        keep = lane // d.strip == q

        def place_plane(p, c, q=q, shift=shift, keep=keep):
            plane = q * per + p
            for dest in range(d.ngx):
                at = slice(dest * d.cx, (dest + 1) * d.cx)
                source = x if (q * per) < 2 * n0 else res
                local = plane if (q * per) < 2 * n0 else plane - 2 * n0
                v = (q * per) // n0 % 2
                value = turn(source[v, local - v * n0, at, :], shift, 1)
                if q == 0:
                    out[dest, p] = value
                else:
                    out[dest, p] = jnp.where(keep, value, out[dest, p])
            return c

        lax.fori_loop(0, per, place_plane, 0)


def unpack_kernel(d, got, solution_out, residual_out):
    n0 = d.layers
    per = 4 * n0 // d.ngx
    lane = lanes((d.cx, d.cy))
    for q in range(d.ngx):
        def body(p, c, q=q):
            value = None
            for src in range(d.ngx):
                part = turn(got[src, p], (d.strip * (src - q)) % d.cy, 1)
                value = part if value is None else jnp.where(lane // d.strip == src, part, value)
            first = q * per
            target = solution_out if first < 2 * n0 else residual_out
            v = first // n0 % 2
            target[v, first % n0 + p] = value
            return c

        lax.fori_loop(0, per, body, 0)


def body(forcing, viscosity, spread, coupling, friction, ice_mask, aggregates):
    ngx, ngy = lax.axis_size("gx"), lax.axis_size("gy")
    layers, cx, cy = viscosity.shape
    d = Dims(ngx, ngy, layers, cx, cy)
    both = ("gx", "gy")
    gx, gy = lax.axis_index("gx"), lax.axis_index("gy")
    is_left = gx < ngx // 2
    off = d.halo - d.strip * gx
    first = jnp.where(is_left, cy - REACH, 0)
    place = jnp.stack([gx * ngy + gy, gx, gy, first, off, is_left.astype(jnp.int32)]).astype(jnp.int32)

    mask_f, ids_f = ice_mask.astype(F32), aggregates.astype(F32)
    stacked = jnp.concatenate(
        [
            forcing.reshape(2 * layers, cx, cy),
            viscosity,
            spread,
            jnp.stack([coupling, friction, mask_f, ids_f]),
        ]
    )
    mine = jnp.stack([mask_f, ids_f, spread.sum(axis=0) * mask_f])
    east = [(i, i + 1) for i in range(ngy - 1)]
    west = [(i + 1, i) for i in range(ngy - 1)]
    left = lax.ppermute(mine, "gy", east)
    right = lax.ppermute(mine, "gy", west)
    gathered = lax.all_gather(stacked, "gx")
    (packed,) = call(
        functools.partial(pack_kernel, d),
        [(d.planes, d.packed, 8, cy)],
        [place, gathered],
        name="pack",
    )
    pairs = []
    for i in range(ngx):
        for j in range(ngy):
            to = j + 1 if i < ngx // 2 else j - 1
            if 0 <= to < ngy:
                pairs.append((i * ngy + j, i * ngy + to))
    packed = lax.ppermute(packed, both, pairs)

    n0, n1, rows = layers, layers // 2, d.rows
    fields = [field(d, n0), field(d, n1), field(d, n1), field(d, 1), field(d, 1)]
    big_shape = lambda count: (d.n, count, cy)
    wide = d.parts + 8
    state_work = [(2, rows, cy), (2, cx, cy)] + work_shapes(d)
    outs = call(
        functools.partial(setup_kernel, d),
        [field(d, n0)] + coef_shapes(d) + [(19, cx, cy), (cx, cy)] + fields + [big_shape(wide)],
        [place, gathered, packed, left, right, mine],
        [(2 * n0 + 4, rows, cy), (wide, cy)] + state_work,
        name="setup",
    )
    f, coefs, blk, strip_ids, state, big = (
        outs[0], outs[1:10], outs[10], outs[11], outs[12:17], outs[17],
    )

    def share(x):
        return lax.all_to_all(x, both, 0, 0)

    table = parts = share(big)
    dots = jnp.zeros((8, cy), F32)
    vs, zs, cols = [], [], []
    pair = (2, d.n, cy)
    small = [(2, cx, cy), (8, cy)]
    r_in = f
    for step in range(ITERS):
        y, r3, big = call(
            functools.partial(point_first, d),
            [pair, pair, big_shape(8)],
            [place, parts, table, blk, dots],
            small,
            name="point_first",
        )
        with_dots = parts = share(big)
        y, big = call(
            functools.partial(point_middle, d),
            [pair, big_shape(8)],
            [place, parts, table, blk, y, r3],
            small,
            name="point_middle",
        )
        parts = share(big)
        y, big = call(
            functools.partial(point_last, d),
            [pair, big_shape(8)],
            [place, parts, table, blk, y, r3],
            small,
            name="point_last",
        )
        parts = share(big)
        last = step + 1 == ITERS
        outs_shapes = [field(d, n0), field(d, n0), (8, cy)]
        if last:
            outs_shapes += [(8, cy), big_shape(8)]
        else:
            outs_shapes += [field(d, n0)] + fields + [(8, cy), big_shape(d.parts)]
        scratch = [field(d, n0)] if last else []
        scratch += [field(d, n0), field(d, n1), field(d, 1), pair, (d.parts, cy)] + state_work
        outs = call(
            functools.partial(step_kernel, d, step, last),
            outs_shapes,
            [place, *coefs, strip_ids, r_in, *state, parts, table, y, r3, with_dots, *vs, *zs],
            scratch,
            name="step",
        )
        vs.append(outs[0])
        zs.append(outs[1])
        cols.append(outs[2])
        if last:
            dots_all = share(outs[4])
        else:
            r_in, state, dots = outs[3], outs[4:9], outs[9]
            parts = share(outs[10])

    (out,) = call(
        functools.partial(final_kernel, d),
        [(ngx, 4 * n0 // ngx, cx, cy)],
        [*coefs[:4], coefs[8], f, dots_all, *cols, *zs],
        [field(d, n0), field(d, n0), (2, n0, rows + 16, cy)],
        name="final",
    )
    got = lax.all_to_all(out, "gx", 0, 0)
    return tuple(
        call(
            functools.partial(unpack_kernel, d),
            [forcing.shape, forcing.shape],
            [got],
            name="unpack",
        )
    )


def solution(mesh):
    return jax.shard_map(
        body,
        mesh=mesh,
        in_specs=(
            P(None, None, "gx", "gy"),
            P(None, "gx", "gy"),
            P(None, "gx", "gy"),
            P("gx", "gy"),
            P("gx", "gy"),
            P("gx", "gy"),
            P("gx", "gy"),
        ),
        out_specs=(P(None, None, "gx", "gy"), P(None, None, "gx", "gy")),
        check_vma=False,
    )
```

```python
import functools

import jax
import jax.numpy as jnp
from jax import lax
from jax.experimental import pallas as pl
from jax.experimental.pallas import tpu as pltpu
from jax.sharding import PartitionSpec as P

ITERS = 3
LINE_WEIGHT = 0.8
POINT_WEIGHT = 0.7
COARSE_WEIGHT = 0.7
CSWEEPS = 4
REACH = 13 * ITERS + 1

VMEM = pl.BlockSpec(memory_space=pltpu.VMEM)
SMEM = pl.BlockSpec(memory_space=pltpu.SMEM)
F32 = jnp.float32


MOST_VMEM = 60 * 1024 * 1024
UNROLL = 3
PIECES = 3


def size_of(shape):
    count = 4
    for extent in shape[:-2]:
        count *= extent
    return count * (-(-shape[-2] // 8) * 8) * (-(-shape[-1] // 128) * 128)


def call(kernel, outs, args, scratch=(), name=None):
    specs = [SMEM if a.dtype == jnp.int32 and a.ndim == 1 else VMEM for a in args]
    shapes = [a.shape for a in args if a.ndim > 1] + list(outs) + list(scratch)
    room = sum(size_of(shape) for shape in shapes) * 9 // 8 + 4 * 1024 * 1024
    return pl.pallas_call(
        kernel,
        out_shape=[jax.ShapeDtypeStruct(s, F32) for s in outs],
        in_specs=specs,
        out_specs=[VMEM] * len(outs),
        scratch_shapes=[pltpu.VMEM(s, F32) for s in scratch],
        compiler_params=pltpu.CompilerParams(vmem_limit_bytes=min(room, MOST_VMEM)),
        name=name,
    )(*args)


class Dims:
    def __init__(self, ngx, ngy, layers, cx, cy):
        self.ngx, self.ngy, self.n = ngx, ngy, ngx * ngy
        self.layers, self.cx, self.cy = layers, cx, cy
        self.rows = ngx * cx
        self.strip = cy // ngx
        self.halo = (cy - self.strip) // 2
        self.groups = self.rows // 8
        self.slots = cy // REACH
        self.packed = -(-self.groups // self.slots)
        self.planes = 4 * layers + 4
        self.parts = -(-2 * ngx // 8) * 8
        self.piece = self.planes // PIECES
        assert self.piece * PIECES == self.planes and self.piece >= layers + 4


def loop(lo, hi, step, init, by=UNROLL):
    trips = (hi - lo) // by

    def trip(t, carry):
        for q in range(by):
            carry = step(lo + t * by + q, carry)
        return carry

    carry = lax.fori_loop(0, trips, trip, init)
    for k in range(lo + trips * by, hi):
        carry = step(k, carry)
    return carry


def lanes(shape):
    return lax.broadcasted_iota(jnp.int32, shape, len(shape) - 1)


def turn(x, shift, axis):
    return pltpu.roll(x, shift, axis)


class Level:
    def __init__(self, d, n, g, s, inv, face, cross, mask, mu, fw):
        self.d, self.n, self.g, self.s, self.inv, self.face = d, n, g, s, inv, face
        self.cross, self.mask, self.mu, self.fw = cross, mask, mu, fw

    def clear_rim(self):
        rows, cy = self.d.rows, self.d.cy
        for v in range(2):
            self.mu[v, :, 0:8, :] = jnp.zeros((self.n, 8, cy), F32)
            self.mu[v, :, 8 + rows : 16 + rows, :] = jnp.zeros((self.n, 8, cy), F32)

    def put_masked(self, v, k, value):
        self.mu[v, k, 8 : 8 + self.d.rows, :] = self.mask[...] * value

    def beside(self, v, k):
        rows, cy = self.d.rows, self.d.cy
        here = self.mu[v, k, 8 : 8 + rows, :]
        return (
            self.mu[v, k, 7 : 7 + rows, :]
            + self.mu[v, k, 9 : 9 + rows, :]
            + (turn(here, 1, 1) + turn(here, cy - 1, 1))
        )

    def apply(self, u, v, k, bottom=False):
        out = self.g[k] * u[v, k] - self.s[k] * self.beside(v, k)
        if self.n > 1:
            pick_int = isinstance(k, int)
            above = min(k + 1, self.n - 1) if pick_int else jnp.minimum(k + 1, self.n - 1)
            below = max(k - 1, 0) if pick_int else jnp.maximum(k - 1, 0)
            out = out - (self.face[k + 1] * u[v, above] + self.face[k] * u[v, below])
        if bottom:
            out = out + self.cross[...] * u[1 - v, k]
        return out

    def sweep(self, r, u, first=False):
        n = self.n
        start = []
        for v in range(2):
            right = r[v, 0]
            if not first:
                right = right - self.apply(u, v, 0, True)
            start.append(right * self.inv[0])
        for v in range(2):
            self.fw[v, 0] = start[v]

        def forward(k, carry):
            out = []
            for v in range(2):
                right = r[v, k]
                if not first:
                    right = right - self.apply(u, v, k)
                value = (right + self.face[k] * carry[v]) * self.inv[k]
                self.fw[v, k] = value
                out.append(value)
            return tuple(out)

        last = loop(1, n, forward, tuple(start)) if n > 1 else tuple(start)

        def store(v, k, value):
            new = LINE_WEIGHT * value
            if not first:
                new = u[v, k] + new
            u[v, k] = new
            self.put_masked(v, k, new)

        for v in range(2):
            store(v, n - 1, last[v])

        def backward(t, carry):
            k = n - 1 - t
            out = []
            factor = self.face[k + 1] * self.inv[k]
            for v in range(2):
                value = self.fw[v, k] + factor * carry[v]
                store(v, k, value)
                out.append(value)
            return tuple(out)

        if n > 1:
            loop(1, n, backward, last)


def level_set(d, coefs, mu0, fw0, mu1, fw1, mu2, fw2):
    g0, s0, i0, f0, g1, s1, i1, f1, low = coefs
    cross, mask = low.at[3], low.at[4]
    rows = d.rows
    one = lambda at: low.at[at : at + 1]
    return (
        Level(d, d.layers, g0, s0, i0, f0, cross, mask, mu0, fw0),
        Level(d, d.layers // 2, g1, s1, i1, f1, cross, mask, mu1, fw1),
        Level(d, 1, one(0), one(1), one(2), None, cross, mask, mu2, fw2),
    )


def coef_shapes(d):
    n0, n1, r, c = d.layers, d.layers // 2, d.rows, d.cy
    plane = lambda n: (n, r, c)
    return [
        plane(n0), plane(n0), plane(n0), plane(n0 + 1),
        plane(n1), plane(n1), plane(n1), plane(n1 + 1),
        plane(6),
    ]


def field(d, n):
    return (2, n, d.rows, d.cy)


def work_shapes(d):
    out = []
    for n in (d.layers, d.layers // 2, 1):
        out += [(2, n, d.rows + 16, d.cy), field(d, n)]
    return out


def own_lanes(d, shape):
    lane = lanes(shape)
    return (lane >= d.halo) & (lane < d.halo + d.strip)


def segment_acc(d, ids_ref, fetch, count):
    cy = d.cy
    wanted = lax.broadcasted_iota(jnp.int32, (cy, cy), 0).astype(F32)
    acc = [jnp.zeros((cy, cy), F32) for _ in range(count)]
    for r in range(d.cx):
        hit = ids_ref[r : r + 1, :] == wanted
        for t in range(count):
            acc[t] = acc[t] + jnp.where(hit, fetch(t, r), 0.0)
    return acc


def restrict_strip(d, strip_ids, e_ref, pack, chunk):
    lane = lanes((d.cx, d.cy))
    for v in range(2):
        out = jnp.zeros((d.cx, d.cy), F32)
        for g in range(d.ngx):
            shift = (d.strip * g - d.halo) % d.cy
            part = turn(e_ref[v, g * d.cx : (g + 1) * d.cx, :], shift, 1)
            out = jnp.where(lane // d.strip == g, part, out)
        pack[v] = out
    acc = segment_acc(d, strip_ids, lambda t, r: pack[t, r : r + 1, :], 2)
    for v in range(2):
        sums = acc[v].T.reshape(d.ngx, d.strip, d.cy).sum(axis=1)
        chunk[v * d.ngx : (v + 1) * d.ngx, :] = sums


def descend(d, levels, r0, u0, r1, u1, r2, u2, strip_ids, e2, pack, chunk):
    l0, l1, l2 = levels
    half = l0.n // 2
    l0.sweep(r0, u0, first=True)
    l0.sweep(r0, u0)

    def residual_pair(kk, bottom):
        for v in range(2):
            low = r0[v, 2 * kk] - l0.apply(u0, v, 2 * kk, bottom)
            high = r0[v, 2 * kk + 1] - l0.apply(u0, v, 2 * kk + 1)
            r1[v, kk] = low + high

    residual_pair(0, True)
    loop(1, half, lambda k, c: (residual_pair(k, False), c)[1], 0)
    l1.sweep(r1, u1, first=True)
    l1.sweep(r1, u1)
    zero = tuple(r1[v, 0] - l1.apply(u1, v, 0, True) for v in range(2))
    total = loop(
        1,
        half,
        lambda k, c: tuple(c[v] + (r1[v, k] - l1.apply(u1, v, k)) for v in range(2)),
        zero,
    )
    for v in range(2):
        r2[v, 0] = total[v]
    l2.sweep(r2, u2, first=True)
    l2.sweep(r2, u2)
    for v in range(2):
        e2[v] = r2[v, 0] - l2.apply(u2, v, 0, True)
    restrict_strip(d, strip_ids, e2, pack, chunk)


def ascend(d, levels, r0, u0, u0i, r1, u1, u1i, r2, u2):
    l0, l1, l2 = levels
    for v in range(2):
        l2.put_masked(v, 0, u2[v, 0])
    for _ in range(2):
        l2.sweep(r2, u2)

    def add1(k, c):
        for v in range(2):
            value = u1i[v, k] + u2[v, 0]
            u1[v, k] = value
            l1.put_masked(v, k, value)
        return c

    loop(0, l1.n, add1, 0)
    for _ in range(2):
        l1.sweep(r1, u1)

    def add0(k, c):
        for v in range(2):
            for p in range(2):
                value = u0i[v, 2 * k + p] + u1[v, k]
                u0[v, 2 * k + p] = value
                l0.put_masked(v, 2 * k + p, value)
        return c

    loop(0, l1.n, add0, 0)
    for _ in range(2):
        l0.sweep(r0, u0)


def pick(row, ids):
    return jnp.take_along_axis(
        jnp.broadcast_to(row, ids.shape), ids, axis=1, mode="promise_in_bounds"
    )


def spread_chunk(d, out, chunk):
    value = chunk[...]
    for i in range(d.n):
        out[i] = value


def pack_kernel(d, place, gathered, out):
    first = place[3]

    def body(p, c):
        lane = lanes((8, d.cy))
        for o in range(d.packed):
            value = jnp.zeros((8, d.cy), F32)
            for s in range(d.slots):
                rg = o * d.slots + s
                if rg >= d.groups:
                    break
                block, at = rg * 8 // d.cx, rg * 8 % d.cx
                x = gathered[block, p, at : at + 8, :]
                x = turn(x, lax.rem(REACH * s - first + d.cy, d.cy), 1)
                keep = (lane >= REACH * s) & (lane < REACH * (s + 1))
                value = jnp.where(keep, x, value)
            out[p, o] = value
        return c

    loop(0, d.piece, body, 0)


def segments(d):
    n0, out = d.layers, []
    for piece in range(PIECES):
        at, end = piece * d.piece, (piece + 1) * d.piece
        while at < end:
            part = min(at // n0, 2)
            stop = min(end, (part + 1) * n0 if part < 2 else d.planes)
            out.append((piece, at - piece * d.piece, stop - at, part if part < 2 else None, at - part * n0))
            at = stop
    return out


def setup_kernel(d, place, *rest):
    all_gathered, all_packed, rest = rest[:PIECES], rest[PIECES : 2 * PIECES], rest[2 * PIECES :]
    left, right, mine = rest[:3]
    rest = rest[3:]
    (f, g0, s0, i0, f0, g1, s1, i1, f1, low, blk, strip_ids) = rest[:12]
    (u0, r1, u1, r2, u2, big) = rest[12:18]
    (win, chunk, e2, pack, mu0, fw0, mu1, fw1, mu2, fw2) = rest[18:]
    n0, n1, rows, cy, cx = d.layers, d.layers // 2, d.rows, d.cy, d.cx
    gx, off, is_left = place[1], place[4], place[5]

    def window(gathered, packed, p, put):
        lane = lanes((8, cy))
        off_own = lax.rem(off + cy, cy)
        own = jnp.where(is_left == 1, (lane >= off).astype(jnp.int32), (lane < cy + off).astype(jnp.int32)) == 1
        lo = jnp.where(is_left == 1, off - REACH, cy + off)
        near = (lane >= lo) & (lane < lo + REACH)
        for rg in range(d.groups):
            block, at = rg * 8 // cx, rg * 8 % cx
            mid = turn(gathered[block, p, at : at + 8, :], off_own, 1)
            o, s = rg // d.slots, rg % d.slots
            side = turn(packed[p, o], lax.rem(lo - REACH * s + 2 * cy, cy), 1)
            put(slice(rg * 8, rg * 8 + 8), jnp.where(own, mid, jnp.where(near, side, 0.0)))

    for piece, first, count, v, there in segments(d):
        def fill(t, c, piece=piece, first=first, v=v, there=there):
            def put(at, value):
                if v is None:
                    win[there + t, at, :] = value
                else:
                    f[v, there + t, at, :] = value
            window(all_gathered[piece], all_packed[piece], first + t, put)
            return c

        loop(0, count, fill, 0)

    gathered = all_gathered[PIECES - 1]
    base = d.planes - d.piece

    cpl, frc, msk = win[2 * n0], win[2 * n0 + 1], win[2 * n0 + 2]
    low[4] = msk
    low[5] = win[2 * n0 + 3]
    low[3] = frc * cpl * msk
    mask = low.at[4]
    nil = jnp.zeros((rows, cy), F32)
    f0[0] = nil
    f0[n0] = nil

    def faces(k, c):
        f0[k + 1] = 0.5 * (win[k] + win[k + 1]) * mask[...]
        return c

    loop(0, n0 - 1, faces, 0)

    def diag(k, extra):
        m = mask[...]
        sp = win[n0 + k]
        s0[k] = sp * m
        inner = f0[k] + f0[k + 1] + 4.0 * sp
        if extra is not None:
            inner = inner + extra
        value = m * inner + (1.0 - m)
        g0[k] = value
        return value

    i0[0] = 1.0 / diag(0, frc)

    def factor0(k, prev):
        face = f0[k]
        inv = 1.0 / (diag(k, None) - face * face * prev)
        i0[k] = inv
        return inv

    loop(1, n0, factor0, i0[0])

    def fold(k, total):
        g1[k] = g0[2 * k] + g0[2 * k + 1] - 2.0 * f0[2 * k + 1]
        s = s0[2 * k] + s0[2 * k + 1]
        s1[k] = s
        f1[k] = f0[2 * k]
        return total + s

    low[1] = loop(0, n1, fold, nil)
    f1[n1] = nil
    i1[0] = 1.0 / g1[0]

    def factor1(k, prev):
        face = f1[k]
        inv = 1.0 / (g1[k] - face * face * prev)
        i1[k] = inv
        return inv

    loop(1, n1, factor1, i1[0])
    diag2 = 4.0 * low[1] + mask[...] * win[2 * n0 + 1] + n0 * (1.0 - mask[...])
    low[0] = diag2
    low[2] = 1.0 / diag2

    def column_sum(block):
        def add(k, t):
            return t + gathered[block, 3 * n0 + k - base]
        total = loop(0, n0, add, jnp.zeros((cx, cy), F32))
        return total * gathered[block, 4 * n0 + 2 - base]

    prev_at, next_at = jnp.maximum(gx - 1, 0), jnp.minimum(gx + 1, d.ngx - 1)
    has_prev, has_next = (gx > 0).astype(F32), (gx < d.ngx - 1).astype(F32)
    m, ids, s2 = mine[0], mine[1], mine[2]
    fr, cp = gathered[gx, 4 * n0 + 1 - base], gathered[gx, 4 * n0 - base]
    row = lax.broadcasted_iota(jnp.int32, (cx, cy), 0)
    lane = lanes((cx, cy))
    prev = (gathered[prev_at, 4 * n0 + 2 - base] * has_prev, gathered[prev_at, 4 * n0 + 3 - base], column_sum(prev_at) * has_prev)
    after = (gathered[next_at, 4 * n0 + 2 - base] * has_next, gathered[next_at, 4 * n0 + 3 - base], column_sum(next_at) * has_next)
    inside = (row > 0, row < cx - 1, lane > 0, lane < cy - 1)

    def around(t, q):
        return (
            jnp.where(inside[0], turn(q, 1, 0), turn(prev[t], 1, 0)),
            jnp.where(inside[1], turn(q, cx - 1, 0), turn(after[t], cx - 1, 0)),
            jnp.where(inside[2], turn(q, 1, 1), turn(left[t], 1, 1)),
            jnp.where(inside[3], turn(q, cy - 1, 1), turn(right[t], cy - 1, 1)),
        )

    m_d, ids_d, s_d = around(0, m), around(1, ids), around(2, s2)
    g2b = 4.0 * s2 + m * fr + n0 * (1.0 - m)
    cb = fr * cp * m
    blk[0], blk[1], blk[2], blk[7] = g2b, s2, cb, ids
    weight3, weight4 = g2b, g2b
    for t in range(4):
        blk[3 + t] = m_d[t]
        blk[8 + t] = ids_d[t]
        weight3 = weight3 - jnp.where(inside[t] & (ids_d[t] == ids), s2 * m_d[t], 0.0)
        weight4 = weight4 - jnp.where(inside[t], s_d[t] * m, 0.0)
        blk[15 + t] = jnp.where(inside[t], 0.0, s_d[t] * m)
    blk[12], blk[13], blk[14] = weight3, cb, weight4
    chunk[...] = jnp.zeros(chunk.shape, F32)
    for t in range(7):
        acc = segment_acc(d, blk.at[7], lambda _, r: blk[12 + t, r : r + 1, :], 1)
        chunk[d.parts + t : d.parts + t + 1, :] = acc[0].T.sum(axis=0, keepdims=True)

    packed_ids = jnp.zeros((cx, cy), F32)
    for g in range(d.ngx):
        part = turn(low[5, g * cx : (g + 1) * cx, :], (d.strip * g - d.halo) % cy, 1)
        packed_ids = jnp.where(lane // d.strip == g, part, packed_ids)
    strip_ids[...] = packed_ids

    def square(k, t):
        return t + f[0, k] * f[0, k] + f[1, k] * f[1, k]

    total = loop(0, n0, square, nil)
    total = jnp.where(own_lanes(d, (rows, cy)), total, 0.0)
    chunk[d.parts + 7 : d.parts + 8, :] = total.sum(axis=0, keepdims=True)

    levels = level_set(d, (g0, s0, i0, f0, g1, s1, i1, f1, low), mu0, fw0, mu1, fw1, mu2, fw2)
    for one in levels:
        one.clear_rim()
    descend(d, levels, f, u0, r1, u1, r2, u2, strip_ids, e2, pack, chunk)
    spread_chunk(d, big, chunk)


def apply_own(d, place, y, blk, tmp, chunk):
    me, n, ngy = place[0], d.n, d.ngy
    shape = (d.cx, d.cy)
    row = lax.broadcasted_iota(jnp.int32, shape, 0)
    lane = lanes(shape)
    inside = (row > 0, row < d.cx - 1, lane > 0, lane < d.cy - 1)
    at = (
        jnp.maximum(me - ngy, 0),
        jnp.minimum(me + ngy, n - 1),
        jnp.maximum(me - 1, 0),
        jnp.minimum(me + 1, n - 1),
    )
    ids = blk[7].astype(jnp.int32)
    mine = [y[v, pl.ds(me, 1), :] for v in range(2)]
    here = [pick(mine[v], ids) for v in range(2)]
    side = [jnp.zeros(shape, F32), jnp.zeros(shape, F32)]
    for t in range(4):
        ids_t = blk[8 + t].astype(jnp.int32)
        for v in range(2):
            outer = pick(y[v, pl.ds(at[t], 1), :], ids_t)
            value = jnp.where(inside[t], pick(mine[v], ids_t), outer)
            side[v] = side[v] + blk[3 + t] * value
    for v in range(2):
        tmp[v] = blk[0] * here[v] + blk[2] * here[1 - v] - blk[1] * side[v]
    acc = segment_acc(d, blk.at[7], lambda t, r: tmp[t, r : r + 1, :], 2)
    for v in range(2):
        chunk[v : v + 1, :] = acc[v].T.sum(axis=0, keepdims=True)


def point_first(d, place, parts, table, blk, dots, y, r3, big, tmp, chunk):
    n, ngx, ngy = d.n, d.ngx, d.ngy
    for v in range(2):
        for g in range(ngx):
            total = parts[0:ngy, v * ngx + g, :]
            for i in range(1, ngx):
                total = total + parts[i * ngy : (i + 1) * ngy, v * ngx + g, :]
            r3[v, g * ngy : (g + 1) * ngy, :] = total
    diag = table[:, d.parts, :]
    for v in range(2):
        y[v] = POINT_WEIGHT * r3[v] / diag
    chunk[2:8, :] = dots[2:8, :]
    apply_own(d, place, y, blk, tmp, chunk)
    spread_chunk(d, big, chunk)


def point_middle(d, place, parts, table, blk, y_in, r3, y, big, tmp, chunk):
    n, ngy = d.n, d.ngy
    base = d.parts
    diag = table[:, base, :]
    cross = table[:, base + 1, :]
    inner = table[:, base + 2, :]
    sides = [table[:, base + 3 + t, :] for t in range(4)]
    shape = (n, d.cy)

    def total(x):
        return jnp.broadcast_to(x.sum(axis=1, keepdims=True), shape)

    def couple(values):
        return (
            turn(values[1], ngy, 0)
            + turn(values[0], n - ngy, 0)
            + turn(values[3], 1, 0)
            + turn(values[2], n - 1, 0)
        )

    y2 = [y_in[v] + POINT_WEIGHT * (r3[v] - parts[:, v, :]) / diag for v in range(2)]
    right = []
    for v in range(2):
        local = total(r3[v] - (inner * y2[v] + cross * y2[1 - v]))
        right.append(local + couple([total(s * y2[v]) for s in sides]))
    diag4, cross4 = total(inner), total(cross)
    sides4 = [total(s) for s in sides]
    x = [COARSE_WEIGHT * right[v] / diag4 for v in range(2)]
    for _ in range(CSWEEPS - 1):
        x = [
            x[v]
            + COARSE_WEIGHT
            * (right[v] - (diag4 * x[v] + cross4 * x[1 - v] - couple([s * x[v] for s in sides4])))
            / diag4
            for v in range(2)
        ]
    for v in range(2):
        y[v] = y2[v] + x[v]
    chunk[...] = jnp.zeros(chunk.shape, F32)
    apply_own(d, place, y, blk, tmp, chunk)
    spread_chunk(d, big, chunk)


def point_last(d, place, parts, table, blk, y_in, r3, y, big, tmp, chunk):
    diag = table[:, d.parts, :]
    for v in range(2):
        y[v] = y_in[v] + POINT_WEIGHT * (r3[v] - parts[:, v, :]) / diag
    chunk[...] = jnp.zeros(chunk.shape, F32)
    apply_own(d, place, y, blk, tmp, chunk)
    spread_chunk(d, big, chunk)


def correct_columns(d, place, parts, table, y_in, r3, y, low, u2):
    diag = table[:, d.parts, :]
    for v in range(2):
        y[v] = y_in[v] + POINT_WEIGHT * (r3[v] - parts[:, v, :]) / diag
    gy, off, is_left = place[2], place[4], place[5]
    shape = (d.cx, d.cy)
    lane = lanes(shape)
    own = jnp.where(is_left == 1, (lane >= off).astype(jnp.int32), (lane < d.cy + off).astype(jnp.int32)) == 1
    other = jnp.where(is_left == 1, jnp.maximum(gy - 1, 0), jnp.minimum(gy + 1, d.ngy - 1))
    for g in range(d.ngx):
        at = slice(g * d.cx, (g + 1) * d.cx)
        ids = low[5, at, :].astype(jnp.int32)
        for v in range(2):
            here = pick(y[v, pl.ds(g * d.ngy + gy, 1), :], ids)
            there = pick(y[v, pl.ds(g * d.ngy + other, 1), :], ids)
            u2[v, 0, at, :] = u2[v, 0, at, :] + jnp.where(own, here, there)


def grid_total(d, dots, row):
    x = dots[:, row, :].sum(axis=0, keepdims=True)
    return jnp.broadcast_to(x.sum(axis=1, keepdims=True), (1, d.cy))


def column_of(d, dots, step):
    inner = [grid_total(d, dots, 2 + i) for i in range(step + 1)]
    square = grid_total(d, dots, 3 + step)
    for value in inner:
        square = square - value * value
    return inner + [jnp.sqrt(square)]


def step_kernel(d, step, last, *refs):
    it = iter(refs)
    take = lambda count: [next(it) for _ in range(count)]
    (place,) = take(1)
    coefs = take(9)
    (strip_ids, r_in, u0i, r1i, u1i, r2i, u2i) = take(7)
    (parts, table, y_in, r3, dots) = take(5)
    olds_v = take(step)
    olds_z = take(step)
    (v_out, z_out, col) = take(3)
    if last:
        (dots_out, big) = take(2)
        w = take(1)[0]
        u0n = None
    else:
        (w, u0n, r1n, u1n, r2n, u2n, dots_out, big) = take(8)
    (u0, u1, u2, y, chunk, e2, pack, mu0, fw0, mu1, fw1, mu2, fw2) = take(13)
    low = coefs[8]
    levels = level_set(d, coefs, mu0, fw0, mu1, fw1, mu2, fw2)
    for one in levels:
        one.clear_rim()
    n0, n1 = d.layers, d.layers // 2

    for v in range(2):
        u2[v, 0] = u2i[v, 0]
    correct_columns(d, place, parts, table, y_in, r3, y, low, u2)

    ascend(d, levels, r_in, u0, u0i, r1i, u1, u1i, r2i, u2)

    if step == 0:
        norm = jnp.sqrt(grid_total(d, table, d.parts + 7))
        inner, height = [], norm
        col[...] = jnp.broadcast_to(norm, col.shape)
    else:
        column = column_of(d, dots, step - 1)
        inner, height = column[:-1], column[-1]
        for t, value in enumerate(column):
            col[t : t + 1, :] = value
    scale = 1.0 / height
    l0 = levels[0]

    def scaled(k, c):
        for v in range(2):
            vec, z = r_in[v, k], u0[v, k]
            for t in range(step):
                vec = vec - inner[t] * olds_v[t][v, k]
                z = z - inner[t] * olds_z[t][v, k]
            v_out[v, k] = vec * scale
            z = z * scale
            z_out[v, k] = z
            l0.put_masked(v, k, z)
        return c

    loop(0, n0, scaled, 0)
    basis = list(olds_v) + [v_out]

    def image(k, acc, bottom=False):
        acc = list(acc)
        for v in range(2):
            value = l0.apply(z_out, v, k, bottom)
            w[v, k] = value
            for t, vec in enumerate(basis):
                acc[t] = acc[t] + vec[v, k] * value
            acc[-1] = acc[-1] + value * value
        return tuple(acc)

    nil = jnp.zeros((d.rows, d.cy), F32)
    acc = image(0, (nil,) * (step + 2), True)
    acc = loop(1, n0, image, acc)
    own = own_lanes(d, (d.rows, d.cy))
    dots_out[...] = jnp.zeros(dots_out.shape, F32)
    for t in range(step + 2):
        dots_out[2 + t : 3 + t, :] = jnp.where(own, acc[t], 0.0).sum(axis=0, keepdims=True)
    if last:
        spread_chunk(d, big, dots_out)
    else:
        descend(d, levels, w, u0n, r1n, u1n, r2n, u2n, strip_ids, e2, pack, chunk)
        spread_chunk(d, big, chunk)


def least_squares(columns, initial_norm):
    count = len(columns)
    rows = [[columns[c][r] for c in range(count)] for r in range(count + 1)]
    target = [initial_norm] + [jnp.zeros_like(initial_norm) for _ in range(count)]
    for p in range(count):
        top, low = rows[p][p], rows[p + 1][p]
        radius = jnp.sqrt(top * top + low * low)
        cosine, sine = top / radius, low / radius
        for c in range(p, count):
            upper, lower = rows[p][c], rows[p + 1][c]
            rows[p][c] = cosine * upper + sine * lower
            rows[p + 1][c] = cosine * lower - sine * upper
        upper, lower = target[p], target[p + 1]
        target[p] = cosine * upper + sine * lower
        target[p + 1] = cosine * lower - sine * upper
    weights = [None] * count
    for p in reversed(range(count)):
        partial = target[p]
        for c in range(p + 1, count):
            partial = partial - rows[p][c] * weights[c]
        weights[p] = partial / rows[p][p]
    return weights


def final_kernel(d, g0, s0, i0, f0, low, f, dots, *refs):
    cols, zs = refs[:ITERS], refs[ITERS : 2 * ITERS]
    out, x, res, mu0 = refs[2 * ITERS :]
    n0 = d.layers
    norm = cols[0][0:1, :]
    nil = jnp.zeros_like(norm)
    columns = []
    for j in range(ITERS):
        if j + 1 < ITERS:
            column = [cols[j + 1][t : t + 1, :] for t in range(j + 2)]
        else:
            column = column_of(d, dots, j)
        columns.append(column + [nil] * (ITERS - 1 - j))
    weights = least_squares(columns, norm)
    l0 = Level(d, n0, g0, s0, i0, f0, low.at[3], low.at[4], mu0, None)
    l0.clear_rim()

    def combine(k, c):
        for v in range(2):
            value = weights[0] * zs[0][v, k]
            for j in range(1, ITERS):
                value = value + weights[j] * zs[j][v, k]
            x[v, k] = value
            l0.put_masked(v, k, value)
        return c

    loop(0, n0, combine, 0)

    def rest(k, bottom):
        for v in range(2):
            res[v, k] = f[v, k] - l0.apply(x, v, k, bottom)

    rest(0, True)
    loop(1, n0, lambda k, c: (rest(k, False), c)[1], 0)

    per = 4 * n0 // d.ngx
    lane = lanes((d.cx, d.cy))
    for q in range(d.ngx):
        shift = (d.strip * q - d.halo) % d.cy
        keep = lane // d.strip == q

        def place_plane(p, c, q=q, shift=shift, keep=keep):
            plane = q * per + p
            for dest in range(d.ngx):
                at = slice(dest * d.cx, (dest + 1) * d.cx)
                source = x if (q * per) < 2 * n0 else res
                local = plane if (q * per) < 2 * n0 else plane - 2 * n0
                v = (q * per) // n0 % 2
                value = turn(source[v, local - v * n0, at, :], shift, 1)
                if q == 0:
                    out[dest, p] = value
                else:
                    out[dest, p] = jnp.where(keep, value, out[dest, p])
            return c

        loop(0, per, place_plane, 0)


def unpack_kernel(d, got, solution_out, residual_out):
    n0 = d.layers
    per = 4 * n0 // d.ngx
    lane = lanes((d.cx, d.cy))
    for q in range(d.ngx):
        def body(p, c, q=q):
            value = None
            for src in range(d.ngx):
                part = turn(got[src, p], (d.strip * (src - q)) % d.cy, 1)
                value = part if value is None else jnp.where(lane // d.strip == src, part, value)
            first = q * per
            target = solution_out if first < 2 * n0 else residual_out
            v = first // n0 % 2
            target[v, first % n0 + p] = value
            return c

        loop(0, per, body, 0)


def body(forcing, viscosity, spread, coupling, friction, ice_mask, aggregates):
    ngx, ngy = lax.axis_size("gx"), lax.axis_size("gy")
    layers, cx, cy = viscosity.shape
    d = Dims(ngx, ngy, layers, cx, cy)
    both = ("gx", "gy")
    gx, gy = lax.axis_index("gx"), lax.axis_index("gy")
    is_left = gx < ngx // 2
    off = d.halo - d.strip * gx
    first = jnp.where(is_left, cy - REACH, 0)
    place = jnp.stack([gx * ngy + gy, gx, gy, first, off, is_left.astype(jnp.int32)]).astype(jnp.int32)

    mask_f, ids_f = ice_mask.astype(F32), aggregates.astype(F32)
    stacked = jnp.concatenate(
        [
            forcing.reshape(2 * layers, cx, cy),
            viscosity,
            spread,
            jnp.stack([coupling, friction, mask_f, ids_f]),
        ]
    )
    mine = jnp.stack([mask_f, ids_f, spread.sum(axis=0) * mask_f])
    east = [(i, i + 1) for i in range(ngy - 1)]
    west = [(i + 1, i) for i in range(ngy - 1)]
    left = lax.ppermute(mine, "gy", east)
    right = lax.ppermute(mine, "gy", west)
    pairs = []
    for i in range(ngx):
        for j in range(ngy):
            to = j + 1 if i < ngx // 2 else j - 1
            if 0 <= to < ngy:
                pairs.append((i * ngy + j, i * ngy + to))
    gathered, packed = [], []
    for t in range(PIECES):
        got = lax.all_gather(stacked[t * d.piece : (t + 1) * d.piece], "gx")
        (sent,) = call(
            functools.partial(pack_kernel, d),
            [(d.piece, d.packed, 8, cy)],
            [place, got],
            name="pack",
        )
        gathered.append(got)
        packed.append(lax.ppermute(sent, both, pairs))

    n0, n1, rows = layers, layers // 2, d.rows
    fields = [field(d, n0), field(d, n1), field(d, n1), field(d, 1), field(d, 1)]
    big_shape = lambda count: (d.n, count, cy)
    wide = d.parts + 8
    state_work = [(2, rows, cy), (2, cx, cy)] + work_shapes(d)
    outs = call(
        functools.partial(setup_kernel, d),
        [field(d, n0)] + coef_shapes(d) + [(19, cx, cy), (cx, cy)] + fields + [big_shape(wide)],
        [place, *gathered, *packed, left, right, mine],
        [(2 * n0 + 4, rows, cy), (wide, cy)] + state_work,
        name="setup",
    )
    f, coefs, blk, strip_ids, state, big = (
        outs[0], outs[1:10], outs[10], outs[11], outs[12:17], outs[17],
    )

    def share(x):
        return lax.all_to_all(x, both, 0, 0)

    table = parts = share(big)
    dots = jnp.zeros((8, cy), F32)
    vs, zs, cols = [], [], []
    pair = (2, d.n, cy)
    small = [(2, cx, cy), (8, cy)]
    r_in = f
    for step in range(ITERS):
        y, r3, big = call(
            functools.partial(point_first, d),
            [pair, pair, big_shape(8)],
            [place, parts, table, blk, dots],
            small,
            name="point_first",
        )
        with_dots = parts = share(big)
        y, big = call(
            functools.partial(point_middle, d),
            [pair, big_shape(8)],
            [place, parts, table, blk, y, r3],
            small,
            name="point_middle",
        )
        parts = share(big)
        y, big = call(
            functools.partial(point_last, d),
            [pair, big_shape(8)],
            [place, parts, table, blk, y, r3],
            small,
            name="point_last",
        )
        parts = share(big)
        last = step + 1 == ITERS
        outs_shapes = [field(d, n0), field(d, n0), (8, cy)]
        if last:
            outs_shapes += [(8, cy), big_shape(8)]
        else:
            outs_shapes += [field(d, n0)] + fields + [(8, cy), big_shape(d.parts)]
        scratch = [field(d, n0)] if last else []
        scratch += [field(d, n0), field(d, n1), field(d, 1), pair, (d.parts, cy)] + state_work
        outs = call(
            functools.partial(step_kernel, d, step, last),
            outs_shapes,
            [place, *coefs, strip_ids, r_in, *state, parts, table, y, r3, with_dots, *vs, *zs],
            scratch,
            name="step",
        )
        vs.append(outs[0])
        zs.append(outs[1])
        cols.append(outs[2])
        if last:
            dots_all = share(outs[4])
        else:
            r_in, state, dots = outs[3], outs[4:9], outs[9]
            parts = share(outs[10])

    (out,) = call(
        functools.partial(final_kernel, d),
        [(ngx, 4 * n0 // ngx, cx, cy)],
        [*coefs[:4], coefs[8], f, dots_all, *cols, *zs],
        [field(d, n0), field(d, n0), (2, n0, rows + 16, cy)],
        name="final",
    )
    got = lax.all_to_all(out, "gx", 0, 0)
    return tuple(
        call(
            functools.partial(unpack_kernel, d),
            [forcing.shape, forcing.shape],
            [got],
            name="unpack",
        )
    )


def solution(mesh):
    return jax.shard_map(
        body,
        mesh=mesh,
        in_specs=(
            P(None, None, "gx", "gy"),
            P(None, "gx", "gy"),
            P(None, "gx", "gy"),
            P("gx", "gy"),
            P("gx", "gy"),
            P("gx", "gy"),
            P("gx", "gy"),
        ),
        out_specs=(P(None, None, "gx", "gy"), P(None, None, "gx", "gy")),
        check_vma=False,
    )
```

```python
import functools

import jax
import jax.numpy as jnp
from jax import lax
from jax.experimental import pallas as pl
from jax.experimental.pallas import tpu as pltpu
from jax.sharding import PartitionSpec as P

ITERS = 3
LINE_WEIGHT = 0.8
POINT_WEIGHT = 0.7
COARSE_WEIGHT = 0.7
CSWEEPS = 4
REACH = 13 * ITERS + 1

VMEM = pl.BlockSpec(memory_space=pltpu.VMEM)
SMEM = pl.BlockSpec(memory_space=pltpu.SMEM)
F32 = jnp.float32


MOST_VMEM = 60 * 1024 * 1024
UNROLL = 3
PIECES = 3


def size_of(shape):
    count = 4
    for extent in shape[:-2]:
        count *= extent
    return count * (-(-shape[-2] // 8) * 8) * (-(-shape[-1] // 128) * 128)


def call(kernel, outs, args, scratch=(), name=None):
    specs = [SMEM if a.dtype == jnp.int32 and a.ndim == 1 else VMEM for a in args]
    shapes = [a.shape for a in args if a.ndim > 1] + list(outs) + list(scratch)
    room = sum(size_of(shape) for shape in shapes) * 9 // 8 + 4 * 1024 * 1024
    return pl.pallas_call(
        kernel,
        out_shape=[jax.ShapeDtypeStruct(s, F32) for s in outs],
        in_specs=specs,
        out_specs=[VMEM] * len(outs),
        scratch_shapes=[pltpu.VMEM(s, F32) for s in scratch],
        compiler_params=pltpu.CompilerParams(vmem_limit_bytes=min(room, MOST_VMEM)),
        name=name,
    )(*args)


class Dims:
    def __init__(self, ngx, ngy, layers, cx, cy):
        self.ngx, self.ngy, self.n = ngx, ngy, ngx * ngy
        self.layers, self.cx, self.cy = layers, cx, cy
        self.rows = ngx * cx
        self.strip = cy // ngx
        self.halo = (cy - self.strip) // 2
        self.groups = self.rows // 8
        self.slots = cy // REACH
        self.packed = -(-self.groups // self.slots)
        self.window = 4 * layers + 4
        self.planes = self.window + 6
        self.parts = -(-2 * ngx // 8) * 8
        self.piece = self.planes // PIECES
        assert self.piece * PIECES == self.planes and self.piece >= layers + 10


def loop(lo, hi, step, init, by=UNROLL):
    trips = (hi - lo) // by

    def trip(t, carry):
        for q in range(by):
            carry = step(lo + t * by + q, carry)
        return carry

    carry = lax.fori_loop(0, trips, trip, init)
    for k in range(lo + trips * by, hi):
        carry = step(k, carry)
    return carry


def lanes(shape):
    return lax.broadcasted_iota(jnp.int32, shape, len(shape) - 1)


def turn(x, shift, axis):
    return pltpu.roll(x, shift, axis)


class Level:
    def __init__(self, d, n, g, s, inv, face, cross, mask, mu, fw):
        self.d, self.n, self.g, self.s, self.inv, self.face = d, n, g, s, inv, face
        self.cross, self.mask, self.mu, self.fw = cross, mask, mu, fw

    def clear_rim(self):
        rows, cy = self.d.rows, self.d.cy
        for v in range(2):
            self.mu[v, :, 0:8, :] = jnp.zeros((self.n, 8, cy), F32)
            self.mu[v, :, 8 + rows : 16 + rows, :] = jnp.zeros((self.n, 8, cy), F32)

    def put_masked(self, v, k, value):
        self.mu[v, k, 8 : 8 + self.d.rows, :] = self.mask[...] * value

    def beside(self, v, k):
        rows, cy = self.d.rows, self.d.cy
        here = self.mu[v, k, 8 : 8 + rows, :]
        return (
            self.mu[v, k, 7 : 7 + rows, :]
            + self.mu[v, k, 9 : 9 + rows, :]
            + (turn(here, 1, 1) + turn(here, cy - 1, 1))
        )

    def apply(self, u, v, k, bottom=False):
        out = self.g[k] * u[v, k] - self.s[k] * self.beside(v, k)
        if self.n > 1:
            pick_int = isinstance(k, int)
            above = min(k + 1, self.n - 1) if pick_int else jnp.minimum(k + 1, self.n - 1)
            below = max(k - 1, 0) if pick_int else jnp.maximum(k - 1, 0)
            out = out - (self.face[k + 1] * u[v, above] + self.face[k] * u[v, below])
        if bottom:
            out = out + self.cross[...] * u[1 - v, k]
        return out

    def sweep(self, r, u, first=False):
        n = self.n
        start = []
        for v in range(2):
            right = r[v, 0]
            if not first:
                right = right - self.apply(u, v, 0, True)
            start.append(right * self.inv[0])
        for v in range(2):
            self.fw[v, 0] = start[v]

        def forward(k, carry):
            out = []
            for v in range(2):
                right = r[v, k]
                if not first:
                    right = right - self.apply(u, v, k)
                value = (right + self.face[k] * carry[v]) * self.inv[k]
                self.fw[v, k] = value
                out.append(value)
            return tuple(out)

        last = loop(1, n, forward, tuple(start)) if n > 1 else tuple(start)

        def store(v, k, value):
            new = LINE_WEIGHT * value
            if not first:
                new = u[v, k] + new
            u[v, k] = new
            self.put_masked(v, k, new)

        for v in range(2):
            store(v, n - 1, last[v])

        def backward(t, carry):
            k = n - 1 - t
            out = []
            factor = self.face[k + 1] * self.inv[k]
            for v in range(2):
                value = self.fw[v, k] + factor * carry[v]
                store(v, k, value)
                out.append(value)
            return tuple(out)

        if n > 1:
            loop(1, n, backward, last)


def level_set(d, coefs, mu0, fw0, mu1, fw1, mu2, fw2):
    g0, s0, i0, f0, g1, s1, i1, f1, low = coefs
    cross, mask = low.at[3], low.at[4]
    rows = d.rows
    one = lambda at: low.at[at : at + 1]
    return (
        Level(d, d.layers, g0, s0, i0, f0, cross, mask, mu0, fw0),
        Level(d, d.layers // 2, g1, s1, i1, f1, cross, mask, mu1, fw1),
        Level(d, 1, one(0), one(1), one(2), None, cross, mask, mu2, fw2),
    )


def coef_shapes(d):
    n0, n1, r, c = d.layers, d.layers // 2, d.rows, d.cy
    plane = lambda n: (n, r, c)
    return [
        plane(n0), plane(n0), plane(n0), plane(n0 + 1),
        plane(n1), plane(n1), plane(n1), plane(n1 + 1),
        plane(6),
    ]


def field(d, n):
    return (2, n, d.rows, d.cy)


def work_shapes(d):
    out = []
    for n in (d.layers, d.layers // 2, 1):
        out += [(2, n, d.rows + 16, d.cy), field(d, n)]
    return out


def own_lanes(d, shape):
    lane = lanes(shape)
    return (lane >= d.halo) & (lane < d.halo + d.strip)


def segment_acc(d, ids_row, fetch, count):
    cy = d.cy
    wanted = lax.broadcasted_iota(jnp.int32, (cy, cy), 0).astype(F32)
    acc = [jnp.zeros((cy, cy), F32) for _ in range(count)]
    for r in range(d.cx):
        hit = ids_row(r) == wanted
        for t in range(count):
            acc[t] = acc[t] + jnp.where(hit, fetch(t, r), 0.0)
    return acc


def restrict_strip(d, strip_ids, e_ref, pack, chunk):
    lane = lanes((d.cx, d.cy))
    for v in range(2):
        out = jnp.zeros((d.cx, d.cy), F32)
        for g in range(d.ngx):
            shift = (d.strip * g - d.halo) % d.cy
            part = turn(e_ref[v, g * d.cx : (g + 1) * d.cx, :], shift, 1)
            out = jnp.where(lane // d.strip == g, part, out)
        pack[v] = out
    acc = segment_acc(d, lambda r: strip_ids[r : r + 1, :], lambda t, r: pack[t, r : r + 1, :], 2)
    for v in range(2):
        sums = acc[v].T.reshape(d.ngx, d.strip, d.cy).sum(axis=1)
        chunk[v * d.ngx : (v + 1) * d.ngx, :] = sums


def descend(d, levels, r0, u0, r1, u1, r2, u2, strip_ids, e2, pack, chunk):
    l0, l1, l2 = levels
    half = l0.n // 2
    l0.sweep(r0, u0, first=True)
    l0.sweep(r0, u0)

    def residual_pair(kk, bottom):
        for v in range(2):
            low = r0[v, 2 * kk] - l0.apply(u0, v, 2 * kk, bottom)
            high = r0[v, 2 * kk + 1] - l0.apply(u0, v, 2 * kk + 1)
            r1[v, kk] = low + high

    residual_pair(0, True)
    loop(1, half, lambda k, c: (residual_pair(k, False), c)[1], 0)
    l1.sweep(r1, u1, first=True)
    l1.sweep(r1, u1)
    zero = tuple(r1[v, 0] - l1.apply(u1, v, 0, True) for v in range(2))
    total = loop(
        1,
        half,
        lambda k, c: tuple(c[v] + (r1[v, k] - l1.apply(u1, v, k)) for v in range(2)),
        zero,
    )
    for v in range(2):
        r2[v, 0] = total[v]
    l2.sweep(r2, u2, first=True)
    l2.sweep(r2, u2)
    for v in range(2):
        e2[v] = r2[v, 0] - l2.apply(u2, v, 0, True)
    restrict_strip(d, strip_ids, e2, pack, chunk)


def ascend(d, levels, r0, u0, u0i, r1, u1, u1i, r2, u2):
    l0, l1, l2 = levels
    for v in range(2):
        l2.put_masked(v, 0, u2[v, 0])
    for _ in range(2):
        l2.sweep(r2, u2)

    def add1(k, c):
        for v in range(2):
            value = u1i[v, k] + u2[v, 0]
            u1[v, k] = value
            l1.put_masked(v, k, value)
        return c

    loop(0, l1.n, add1, 0)
    for _ in range(2):
        l1.sweep(r1, u1)

    def add0(k, c):
        for v in range(2):
            for p in range(2):
                value = u0i[v, 2 * k + p] + u1[v, k]
                u0[v, 2 * k + p] = value
                l0.put_masked(v, 2 * k + p, value)
        return c

    loop(0, l1.n, add0, 0)
    for _ in range(2):
        l0.sweep(r0, u0)


def pick(row, ids):
    return jnp.take_along_axis(
        jnp.broadcast_to(row, ids.shape), ids, axis=1, mode="promise_in_bounds"
    )


def spread_chunk(d, out, chunk):
    value = chunk[...]
    for i in range(d.n):
        out[i] = value


def pack_planes(d, place, gathered, count, put):
    first = place[3]

    def body(p, c):
        lane = lanes((8, d.cy))
        for o in range(d.packed):
            value = jnp.zeros((8, d.cy), F32)
            for s in range(d.slots):
                rg = o * d.slots + s
                if rg >= d.groups:
                    break
                block, at = rg * 8 // d.cx, rg * 8 % d.cx
                x = gathered[block, p, at : at + 8, :]
                x = turn(x, lax.rem(REACH * s - first + d.cy, d.cy), 1)
                keep = (lane >= REACH * s) & (lane < REACH * (s + 1))
                value = jnp.where(keep, x, value)
            put(p * d.packed + o, value)
        return c

    loop(0, count, body, 0)


def pack_kernel(d, count, place, *refs):
    *pieces, out = refs
    for t, piece in enumerate(pieces):
        def put(at, value, t=t):
            out[t * d.piece * d.packed + at] = value
        pack_planes(d, place, piece, count, put)


def segments(d):
    n0, out = d.layers, []
    for piece in range(PIECES):
        at, end = piece * d.piece, min((piece + 1) * d.piece, d.window)
        while at < end:
            part = min(at // n0, 2)
            stop = min(end, (part + 1) * n0 if part < 2 else d.window)
            out.append((piece, at - piece * d.piece, stop - at, part if part < 2 else None, at - part * n0))
            at = stop
    return out


def setup_kernel(d, place, *rest):
    all_gathered, bulk, last_ref, rest = rest[:PIECES], rest[PIECES], rest[PIECES + 1], rest[PIECES + 2 :]
    (f, g0, s0, i0, f0, g1, s1, i1, f1, low, strip_ids) = rest[:11]
    (u0, r1, u1, r2, u2, big) = rest[11:17]
    (win, chunk, e2, pack, mu0, fw0, mu1, fw1, mu2, fw2) = rest[17:]
    n0, n1, rows, cy, cx = d.layers, d.layers // 2, d.rows, d.cy, d.cx
    off, is_left = place[4], place[5]
    if d.parts > 2 * d.ngx:
        chunk[...] = jnp.zeros(chunk.shape, F32)

    def window(gathered, packed, p, put):
        lane = lanes((8, cy))
        off_own = lax.rem(off + cy, cy)
        own = jnp.where(is_left == 1, (lane >= off).astype(jnp.int32), (lane < cy + off).astype(jnp.int32)) == 1
        lo = jnp.where(is_left == 1, off - REACH, cy + off)
        near = (lane >= lo) & (lane < lo + REACH)
        for rg in range(d.groups):
            block, at = rg * 8 // cx, rg * 8 % cx
            mid = turn(gathered[block, p, at : at + 8, :], off_own, 1)
            o, s = rg // d.slots, rg % d.slots
            side = turn(packed[p * d.packed + o], lax.rem(lo - REACH * s + 2 * cy, cy), 1)
            put(slice(rg * 8, rg * 8 + 8), jnp.where(own, mid, jnp.where(near, side, 0.0)))

    for piece, first, count, v, there in segments(d):
        def fill(t, c, piece=piece, first=first, v=v, there=there):
            def put(at, value):
                if v is None:
                    win[there + t, at, :] = value
                else:
                    f[v, there + t, at, :] = value
            packed = last_ref if piece == PIECES - 1 else bulk.at[pl.ds(piece * d.piece * d.packed, d.piece * d.packed)]
            window(all_gathered[piece], packed, first + t, put)
            return c

        loop(0, count, fill, 0)

    cpl, frc, msk = win[2 * n0], win[2 * n0 + 1], win[2 * n0 + 2]
    low[4] = msk
    low[5] = win[2 * n0 + 3]
    low[3] = frc * cpl * msk
    mask = low.at[4]
    nil = jnp.zeros((rows, cy), F32)
    f0[0] = nil
    f0[n0] = nil

    def faces(k, c):
        f0[k + 1] = 0.5 * (win[k] + win[k + 1]) * mask[...]
        return c

    loop(0, n0 - 1, faces, 0)

    def diag(k, extra):
        m = mask[...]
        sp = win[n0 + k]
        s0[k] = sp * m
        inner = f0[k] + f0[k + 1] + 4.0 * sp
        if extra is not None:
            inner = inner + extra
        value = m * inner + (1.0 - m)
        g0[k] = value
        return value

    i0[0] = 1.0 / diag(0, frc)

    def factor0(k, prev):
        face = f0[k]
        inv = 1.0 / (diag(k, None) - face * face * prev)
        i0[k] = inv
        return inv

    loop(1, n0, factor0, i0[0])

    def fold(k, total):
        g1[k] = g0[2 * k] + g0[2 * k + 1] - 2.0 * f0[2 * k + 1]
        s = s0[2 * k] + s0[2 * k + 1]
        s1[k] = s
        f1[k] = f0[2 * k]
        return total + s

    low[1] = loop(0, n1, fold, nil)
    f1[n1] = nil
    i1[0] = 1.0 / g1[0]

    def factor1(k, prev):
        face = f1[k]
        inv = 1.0 / (g1[k] - face * face * prev)
        i1[k] = inv
        return inv

    loop(1, n1, factor1, i1[0])
    diag2 = 4.0 * low[1] + mask[...] * win[2 * n0 + 1] + n0 * (1.0 - mask[...])
    low[0] = diag2
    low[2] = 1.0 / diag2

    lane = lanes((cx, cy))
    packed_ids = jnp.zeros((cx, cy), F32)
    for g in range(d.ngx):
        part = turn(low[5, g * cx : (g + 1) * cx, :], (d.strip * g - d.halo) % cy, 1)
        packed_ids = jnp.where(lane // d.strip == g, part, packed_ids)
    strip_ids[...] = packed_ids

    levels = level_set(d, (g0, s0, i0, f0, g1, s1, i1, f1, low), mu0, fw0, mu1, fw1, mu2, fw2)
    for one in levels:
        one.clear_rim()
    descend(d, levels, f, u0, r1, u1, r2, u2, strip_ids, e2, pack, chunk)
    spread_chunk(d, big, chunk)


COLUMN = 9


def inside_of(d):
    shape = (d.cx, d.cy)
    row = lax.broadcasted_iota(jnp.int32, shape, 0)
    lane = lanes(shape)
    return (row > 0, row < d.cx - 1, lane > 0, lane < d.cy - 1)


def column_kernel(d, place, got, out, table, tmp):
    n0, cx, cy = d.layers, d.cx, d.cy
    base = d.planes - d.piece
    at_spread, at_misc = 3 * n0 - base, 4 * n0 - base
    inside = inside_of(d)
    nil = jnp.zeros((cx, cy), F32)

    def sums(g):
        total = loop(0, n0, lambda k, t: t + got[g, at_spread + k], nil)
        return total * got[g, at_misc + 2]

    s2_all = [sums(g) for g in range(d.ngx)]
    table[...] = jnp.zeros(table.shape, F32)
    for g in range(d.ngx):
        fr, cp = got[g, at_misc + 1], got[g, at_misc]
        own = (got[g, at_misc + 2], got[g, at_misc + 3], s2_all[g])

        def around(t):
            q = own[t]
            up = (got[g - 1, at_misc + 2 + t] if t < 2 else s2_all[g - 1]) if g > 0 else nil
            down = (got[g + 1, at_misc + 2 + t] if t < 2 else s2_all[g + 1]) if g + 1 < d.ngx else nil
            left, right = got[g, at_misc + 4 + t], got[g, at_misc + 7 + t]
            return (
                jnp.where(inside[0], turn(q, 1, 0), turn(up, 1, 0)),
                jnp.where(inside[1], turn(q, cx - 1, 0), turn(down, cx - 1, 0)),
                jnp.where(inside[2], turn(q, 1, 1), turn(left, 1, 1)),
                jnp.where(inside[3], turn(q, cy - 1, 1), turn(right, cy - 1, 1)),
            )

        m, ids, s2 = own
        m_d, ids_d, s_d = around(0), around(1), around(2)
        g2 = 4.0 * s2 + m * fr + n0 * (1.0 - m)
        cross = fr * cp * m
        at = slice(g * cx, (g + 1) * cx)
        out[0, at, :], out[1, at, :], out[2, at, :], out[3, at, :] = g2, s2, cross, ids
        weight3, weight4 = g2, g2
        for t in range(4):
            out[4 + t, at, :] = m_d[t] * (1.0 + ids_d[t])
            weight3 = weight3 - jnp.where(inside[t] & (ids_d[t] == ids), s2 * m_d[t], 0.0)
            weight4 = weight4 - jnp.where(inside[t], s_d[t] * m, 0.0)
            tmp[3 + t] = jnp.where(inside[t], 0.0, s_d[t] * m)
        tmp[0], tmp[1], tmp[2] = weight3, cross, weight4
        ids_row = lambda r: out[3, g * cx + r : g * cx + r + 1, :]
        acc = segment_acc(d, ids_row, lambda _, r: tmp[0, r : r + 1, :], 1)
        out[8, at, :] = jnp.broadcast_to(acc[0].T.sum(axis=0, keepdims=True), (cx, cy))

        @pl.when(place[1] == g)
        def _():
            def one(t, c):
                acc = segment_acc(d, ids_row, lambda _, r: tmp[1 + t, r : r + 1, :], 1)
                table[pl.ds(2 + t, 1), :] = acc[0].T.sum(axis=0, keepdims=True)
                return c

            loop(0, 6, one, 0, 1)


def apply_block(d, cols, pos, g, rows, tmp, inside):
    at = pl.ds(pl.multiple_of(g * d.cx, d.cx), d.cx)
    shape = (d.cx, d.cy)
    ids = cols[pos, 3, at, :].astype(jnp.int32)
    here = [pick(rows[0][v], ids) for v in range(2)]
    side = [jnp.zeros(shape, F32), jnp.zeros(shape, F32)]
    for t in range(4):
        code = cols[pos, 4 + t, at, :].astype(jnp.int32) - 1
        live = code >= 0
        code = jnp.maximum(code, 0)
        for v in range(2):
            value = jnp.where(inside[t], pick(rows[0][v], code), pick(rows[1 + t][v], code))
            side[v] = side[v] + jnp.where(live, value, 0.0)
    g2, s2, cross = cols[pos, 0, at, :], cols[pos, 1, at, :], cols[pos, 2, at, :]
    for v in range(2):
        tmp[v] = g2 * here[v] + cross * here[1 - v] - s2 * side[v]
    acc = segment_acc(
        d,
        lambda r: cols[pos, 3, pl.ds(g * d.cx + r, 1), :],
        lambda t, r: tmp[t, r : r + 1, :],
        2,
    )
    return [acc[v].T.sum(axis=0, keepdims=True) for v in range(2)]


def diagonal(d, cols, pos, g):
    x = cols[pos, 8, pl.ds(g * d.cx, 1), :]
    return jnp.where(x == 0.0, 1.0, x)


def clip(x, top):
    return jnp.clip(x, 0, top - 1)


def point_first(d, step, place, parts, extra, *rest):
    if step == 0:
        near, column, opposite, far, cols, r3, big, tmp, chunk = rest
        at_near = jnp.where(place[5] == 1, 0, 2)

        def stack(p, c):
            cols[1, p], cols[3, p] = column[p], far[p]
            cols[at_near, p], cols[2 - at_near, p] = near[p], opposite[p]
            return c

        loop(0, COLUMN, stack, 0)
    else:
        cols, r3, big, tmp, chunk = rest
    ngx, ngy = d.ngx, d.ngy
    for v in range(2):
        for g in range(ngx):
            total = parts[0:ngy, v * ngx + g, :]
            for i in range(1, ngx):
                total = total + parts[i * ngy : (i + 1) * ngy, v * ngx + g, :]
            r3[v, g * ngy : (g + 1) * ngy, :] = total
    gx, gy = place[1], place[2]
    up, down = clip(gx - 1, ngx), clip(gx + 1, ngx)
    spots = (
        (1, gx, gy),
        (1, up, gy),
        (1, down, gy),
        (0, gx, clip(gy - 1, ngy)),
        (2, gx, clip(gy + 1, ngy)),
    )
    right, diag, rows = [], [], []
    for pos, g, c in spots:
        right.append([r3[v, pl.ds(g * ngy + c, 1), :] for v in range(2)])
        diag.append(diagonal(d, cols, pos, g))
        rows.append([POINT_WEIGHT * right[-1][v] / diag[-1] for v in range(2)])
    image = apply_block(d, cols, 1, gx, rows, tmp, inside_of(d))
    count = chunk.shape[0]
    chunk[2:count, :] = extra[2:count, :]
    for v in range(2):
        chunk[v : v + 1, :] = rows[0][v] + POINT_WEIGHT * (right[0][v] - image[v]) / diag[0]
    spread_chunk(d, big, chunk)


def correct_columns(d, place, parts, table, r3, cols, low, u2, y3, y4, y5, tmp):
    n, ngx, ngy = d.n, d.ngx, d.ngy
    gy, off, is_left = place[2], place[4], place[5]
    cross, inner = table[:, 2, :], table[:, 3, :]
    sides = [table[:, 4 + t, :] for t in range(4)]
    shape = (n, d.cy)

    def total(x):
        return jnp.broadcast_to(x.sum(axis=1, keepdims=True), shape)

    def couple(values):
        return (
            turn(values[1], ngy, 0)
            + turn(values[0], n - ngy, 0)
            + turn(values[3], 1, 0)
            + turn(values[2], n - 1, 0)
        )

    y2 = [parts[:, v, :] for v in range(2)]
    right = []
    for v in range(2):
        local = total(r3[v] - (inner * y2[v] + cross * y2[1 - v]))
        right.append(local + couple([total(s * y2[v]) for s in sides]))
    diag4, cross4 = total(inner), total(cross)
    sides4 = [total(s) for s in sides]
    x = [COARSE_WEIGHT * right[v] / diag4 for v in range(2)]
    for _ in range(CSWEEPS - 1):
        x = [
            x[v]
            + COARSE_WEIGHT
            * (right[v] - (diag4 * x[v] + cross4 * x[1 - v] - couple([s * x[v] for s in sides4])))
            / diag4
            for v in range(2)
        ]
    for v in range(2):
        y3[v] = y2[v] + x[v]

    def column(pos):
        far = jnp.where(is_left == 1, -2, 2)
        return gy + jnp.where(pos == 3, far, pos - 1)

    inside = inside_of(d)

    def relax(pos, g, rows, c, q):
        image = apply_block(d, cols, pos, g, rows, tmp.at[q], inside)
        diag = diagonal(d, cols, pos, g)
        at = pl.ds(g * ngy + c, 1)
        return [
            rows[0][v] + POINT_WEIGHT * (r3[v, at, :] - image[v]) / diag for v in range(2)
        ]

    def fourth(b, carry):
        for q in range(2):
            pos, g = lax.div(2 * b + q, ngx), lax.rem(2 * b + q, ngx)
            c = column(pos)
            get = lambda g, c: [
                y3[v, pl.ds(clip(g, ngx) * ngy + clip(c, ngy), 1), :] for v in range(2)
            ]
            rows = [get(g, c), get(g - 1, c), get(g + 1, c), get(g, c - 1), get(g, c + 1)]
            new = relax(pos, g, rows, clip(c, ngy), q)
            for v in range(2):
                y4[v, pl.ds(pos * ngx + g, 1), :] = new[v]
        return carry

    def fifth(b, carry):
        for q in range(2):
            t, g = lax.div(2 * b + q, ngx), lax.rem(2 * b + q, ngx)
            pos = t + 1 - is_left
            west = jnp.where(pos == 0, 3, pos - 1)
            east = jnp.where(pos == 2, 3, pos + 1)
            get = lambda g, p: [
                y4[v, pl.ds(p * ngx + clip(g, ngx), 1), :] for v in range(2)
            ]
            rows = [get(g, pos), get(g - 1, pos), get(g + 1, pos), get(g, west), get(g, east)]
            new = relax(pos, g, rows, clip(column(pos), ngy), q)
            for v in range(2):
                y5[v, pl.ds(t * ngx + g, 1), :] = new[v]
        return carry

    lax.fori_loop(0, 2 * ngx, fourth, 0)
    lax.fori_loop(0, ngx, fifth, 0)

    block = (d.cx, d.cy)
    lane = lanes(block)
    own = jnp.where(is_left == 1, (lane >= off).astype(jnp.int32), (lane < d.cy + off).astype(jnp.int32)) == 1
    for g in range(ngx):
        at = slice(g * d.cx, (g + 1) * d.cx)
        ids = low[5, at, :].astype(jnp.int32)
        for v in range(2):
            here = pick(y5[v, pl.ds(is_left * ngx + g, 1), :], ids)
            there = pick(y5[v, pl.ds((1 - is_left) * ngx + g, 1), :], ids)
            u2[v, 0, at, :] = u2[v, 0, at, :] + jnp.where(own, here, there)


def grid_totals(d, dots, count):
    x = dots[:, 2, :].sum(axis=0, keepdims=True)
    lane = lanes((1, d.cy))
    return [
        jnp.broadcast_to(
            jnp.where(lane == t, x, 0.0).sum(axis=1, keepdims=True), (1, d.cy)
        )
        for t in range(count)
    ]


def column_of(d, dots, step, norm=None):
    values = grid_totals(d, dots, step + 2 + (step == 0))
    if step == 0:
        square = values[2]
        norm = jnp.sqrt(square)
        inner, height = [values[0] / square], values[1] / square
    else:
        inner, height = [values[0] / norm] + values[1:-1], values[-1]
    for value in inner:
        height = height - value * value
    return inner + [jnp.sqrt(height)], norm


def step_kernel(d, step, last, *refs):
    it = iter(refs)
    take = lambda count: [next(it) for _ in range(count)]
    (place,) = take(1)
    coefs = take(9)
    (strip_ids, r_in, u0i, r1i, u1i, r2i, u2i) = take(7)
    (parts, table, r3, cols) = take(4)
    norm_in = take(1)[0] if step > 1 else None
    olds_v = take(step)
    olds_z = take(step)
    if step:
        (v_out, col) = take(2)
    (z_out,) = take(1)
    if last:
        (dots_out, big) = take(2)
        w = take(1)[0]
        u0n = None
    else:
        (w, u0n, r1n, u1n, r2n, u2n, dots_out, big) = take(8)
    (u0, u1, u2, y3, y4, y5, tmp, chunk, e2, pack, mu0, fw0, mu1, fw1, mu2, fw2) = take(16)
    low = coefs[8]
    levels = level_set(d, coefs, mu0, fw0, mu1, fw1, mu2, fw2)
    for one in levels:
        one.clear_rim()
    n0, n1 = d.layers, d.layers // 2

    for v in range(2):
        u2[v, 0] = u2i[v, 0]
    correct_columns(d, place, parts, table, r3, cols, low, u2, y3, y4, y5, tmp)
    if not last and d.parts > 2 * d.ngx:
        chunk[...] = jnp.zeros(chunk.shape, F32)

    ascend(d, levels, r_in, u0, u0i, r1i, u1, u1i, r2i, u2)

    l0 = levels[0]
    if step:
        norm = norm_in[step : step + 1, :] if step > 1 else None
        column, norm = column_of(d, parts, step - 1, norm)
        height = column[-1]
        if step == 1:
            inner, scale = [column[0]], 1.0 / (height * norm)
        else:
            inner, scale = [column[0] / norm] + column[1:-1], 1.0 / height
        for t, value in enumerate(column + [norm]):
            col[t : t + 1, :] = value

    def scaled(k, c):
        for v in range(2):
            z = u0[v, k]
            if step:
                vec = r_in[v, k]
                for t in range(step):
                    vec = vec - inner[t] * olds_v[t][v, k]
                    z = z - inner[t] * olds_z[t][v, k]
                v_out[v, k] = vec * scale
                z = z * scale
            z_out[v, k] = z
            l0.put_masked(v, k, z)
        return c

    loop(0, n0, scaled, 0)
    basis = list(olds_v) + [v_out if step else r_in]

    def image(k, acc, bottom=False):
        acc = list(acc)
        for v in range(2):
            value = l0.apply(z_out, v, k, bottom)
            w[v, k] = value
            for t, vec in enumerate(basis):
                acc[t] = acc[t] + vec[v, k] * value
            acc[step + 1] = acc[step + 1] + value * value
            if step == 0:
                acc[2] = acc[2] + r_in[v, k] * r_in[v, k]
        return tuple(acc)

    nil = jnp.zeros((d.rows, d.cy), F32)
    acc = image(0, (nil,) * (step + 2 + (step == 0)), True)
    acc = loop(1, n0, image, acc)
    own = own_lanes(d, (d.rows, d.cy))
    lane = lanes((1, d.cy))
    row = jnp.zeros((1, d.cy), F32)
    for t, value in enumerate(acc):
        value = jnp.where(own, value, 0.0).sum(axis=0, keepdims=True)
        row = jnp.where(lane == t, value.sum(axis=1, keepdims=True), row)
    dots_out[...] = jnp.zeros(dots_out.shape, F32)
    dots_out[2:3, :] = row
    if last:
        spread_chunk(d, big, dots_out)
    else:
        descend(d, levels, w, u0n, r1n, u1n, r2n, u2n, strip_ids, e2, pack, chunk)
        spread_chunk(d, big, chunk)


def least_squares(columns, initial_norm):
    count = len(columns)
    rows = [[columns[c][r] for c in range(count)] for r in range(count + 1)]
    target = [initial_norm] + [jnp.zeros_like(initial_norm) for _ in range(count)]
    for p in range(count):
        top, low = rows[p][p], rows[p + 1][p]
        radius = jnp.sqrt(top * top + low * low)
        cosine, sine = top / radius, low / radius
        for c in range(p, count):
            upper, lower = rows[p][c], rows[p + 1][c]
            rows[p][c] = cosine * upper + sine * lower
            rows[p + 1][c] = cosine * lower - sine * upper
        upper, lower = target[p], target[p + 1]
        target[p] = cosine * upper + sine * lower
        target[p + 1] = cosine * lower - sine * upper
    weights = [None] * count
    for p in reversed(range(count)):
        partial = target[p]
        for c in range(p + 1, count):
            partial = partial - rows[p][c] * weights[c]
        weights[p] = partial / rows[p][p]
    return weights


def final_kernel(d, g0, s0, i0, f0, low, f, dots, *refs):
    cols, zs = refs[: ITERS - 1], refs[ITERS - 1 : 2 * ITERS - 1]
    out, x, res, mu0 = refs[2 * ITERS - 1 :]
    n0 = d.layers
    nil = jnp.zeros((1, d.cy), F32)
    columns = []
    norm = cols[0][2:3, :]
    for j in range(ITERS):
        if j + 1 < ITERS:
            column = [cols[j][t : t + 1, :] for t in range(j + 2)]
        else:
            column, _ = column_of(d, dots, j, norm)
        columns.append(column + [nil] * (ITERS - 1 - j))
    weights = least_squares(columns, norm)
    weights[0] = weights[0] / norm
    l0 = Level(d, n0, g0, s0, i0, f0, low.at[3], low.at[4], mu0, None)
    l0.clear_rim()

    def combine(k, c):
        for v in range(2):
            value = weights[0] * zs[0][v, k]
            for j in range(1, ITERS):
                value = value + weights[j] * zs[j][v, k]
            x[v, k] = value
            l0.put_masked(v, k, value)
        return c

    loop(0, n0, combine, 0)

    def rest(k, bottom):
        for v in range(2):
            res[v, k] = f[v, k] - l0.apply(x, v, k, bottom)

    rest(0, True)
    loop(1, n0, lambda k, c: (rest(k, False), c)[1], 0)

    per = 4 * n0 // d.ngx
    lane = lanes((d.cx, d.cy))
    for q in range(d.ngx):
        shift = (d.strip * q - d.halo) % d.cy
        keep = lane // d.strip == q

        def place_plane(p, c, q=q, shift=shift, keep=keep):
            plane = q * per + p
            for dest in range(d.ngx):
                at = slice(dest * d.cx, (dest + 1) * d.cx)
                source = x if (q * per) < 2 * n0 else res
                local = plane if (q * per) < 2 * n0 else plane - 2 * n0
                v = (q * per) // n0 % 2
                value = turn(source[v, local - v * n0, at, :], shift, 1)
                if q == 0:
                    out[dest, p] = value
                else:
                    out[dest, p] = jnp.where(keep, value, out[dest, p])
            return c

        loop(0, per, place_plane, 0)


def unpack_kernel(d, got, solution_out, residual_out):
    n0 = d.layers
    per = 4 * n0 // d.ngx
    lane = lanes((d.cx, d.cy))
    for q in range(d.ngx):
        def body(p, c, q=q):
            value = None
            for src in range(d.ngx):
                part = turn(got[src, p], (d.strip * (src - q)) % d.cy, 1)
                value = part if value is None else jnp.where(lane // d.strip == src, part, value)
            first = q * per
            target = solution_out if first < 2 * n0 else residual_out
            v = first // n0 % 2
            target[v, first % n0 + p] = value
            return c

        loop(0, per, body, 0)


def body(forcing, viscosity, spread, coupling, friction, ice_mask, aggregates):
    ngx, ngy = lax.axis_size("gx"), lax.axis_size("gy")
    layers, cx, cy = viscosity.shape
    d = Dims(ngx, ngy, layers, cx, cy)
    both = ("gx", "gy")
    gx, gy = lax.axis_index("gx"), lax.axis_index("gy")
    is_left = gx < ngx // 2
    off = d.halo - d.strip * gx
    first = jnp.where(is_left, cy - REACH, 0)
    place = jnp.stack([gx * ngy + gy, gx, gy, first, off, is_left.astype(jnp.int32)]).astype(jnp.int32)

    mask_f, ids_f = ice_mask.astype(F32), aggregates.astype(F32)
    mine = jnp.stack([mask_f, ids_f, spread.sum(axis=0) * mask_f])
    shift = lambda by: [(i, i + by) for i in range(ngy) if 0 <= i + by < ngy]
    left = lax.ppermute(mine, "gy", shift(1))
    right = lax.ppermute(mine, "gy", shift(-1))
    planes = [
        forcing.reshape(2 * layers, cx, cy),
        viscosity,
        spread,
        jnp.stack([coupling, friction, mask_f, ids_f]),
        left,
        right,
    ]
    pieces, start = [[] for _ in range(PIECES)], 0
    for part in planes:
        end = start + part.shape[0]
        for t in range(PIECES):
            low, high = max(start, t * d.piece), min(end, (t + 1) * d.piece)
            if low < high:
                pieces[t].append(part[low - start : high - start])
        start = end
    def sided(by):
        return [
            (i * ngy + j, i * ngy + to)
            for i in range(ngx)
            for j in range(ngy)
            for to in [j + by if i < ngx // 2 else j - by]
            if 0 <= to < ngy
        ]

    gathered, packed = [], []
    for t in range(PIECES):
        got = lax.all_gather(jnp.concatenate(pieces[t]), "gx")
        gathered.append(got)
        if t >= PIECES - 2:
            use = gathered[t:] if t == PIECES - 1 else gathered
            count = d.window - t * d.piece if t == PIECES - 1 else d.piece
            (sent,) = call(
                functools.partial(pack_kernel, d, count),
                [(len(use) * count * d.packed, 8, cy)],
                [place, *use],
                name="pack",
            )
            packed.append(lax.ppermute(sent, both, sided(1)))
    column, table_own = call(
        functools.partial(column_kernel, d),
        [(COLUMN, d.rows, cy), (8, cy)],
        [place, gathered[-1]],
        [(7, cx, cy)],
        name="column",
    )
    near = lax.ppermute(column, both, sided(1))
    opposite = lax.ppermute(column, both, sided(-1))
    far = lax.ppermute(column, both, sided(2))

    n0, n1, rows = layers, layers // 2, d.rows
    fields = [field(d, n0), field(d, n1), field(d, n1), field(d, 1), field(d, 1)]
    big_shape = lambda count: (d.n, count, cy)
    state_work = [(2, rows, cy), (2, cx, cy)] + work_shapes(d)
    outs = call(
        functools.partial(setup_kernel, d),
        [field(d, n0)] + coef_shapes(d) + [(cx, cy)] + fields + [big_shape(d.parts)],
        [place, *gathered, *packed],
        [(2 * n0 + 4, rows, cy), (d.parts, cy)] + state_work,
        name="setup",
    )
    f, coefs, strip_ids, state, big = outs[0], outs[1:10], outs[10], outs[11:16], outs[16]

    def share(x):
        return lax.all_to_all(x, both, 0, 0)

    big, near, opposite, far = lax.optimization_barrier((big, near, opposite, far))
    parts = share(big)
    extra = table_own
    vs, zs, norms = [f], [], []
    pair = (2, d.n, cy)
    r_in = f
    for step in range(ITERS):
        count = 4 if step else 8
        outs = call(
            functools.partial(point_first, d, step),
            ([] if step else [(4, COLUMN, rows, cy)]) + [pair, big_shape(count)],
            [place, parts, extra] + ([cols] if step else [near, column, opposite, far]),
            [(2, cx, cy), (count, cy)],
            name="point_first",
        )
        r3, big = outs[-2:]
        parts = share(big)
        if step == 0:
            cols, table = outs[0], parts
        last = step + 1 == ITERS
        outs_shapes = [field(d, n0), (8, cy)] if step else []
        outs_shapes += [field(d, n0)]
        if last:
            outs_shapes += [(4, cy), big_shape(4)]
        else:
            outs_shapes += [field(d, n0)] + fields + [(4, cy), big_shape(d.parts)]
        scratch = [field(d, n0)] if last else []
        scratch += [field(d, n0), field(d, n1), field(d, 1), pair]
        scratch += [(2, 4 * ngx, cy), (2, 2 * ngx, cy), (2, 2, cx, cy), (d.parts, cy)] + state_work
        outs = call(
            functools.partial(step_kernel, d, step, last),
            outs_shapes,
            [place, *coefs, strip_ids, r_in, *state, parts, table, r3, cols]
            + norms[step - 2 : step - 1 if step > 1 else 0]
            + (vs[:step] + zs),
            scratch,
            name="step",
        )
        if step:
            vs.append(outs[0])
            norms.append(outs[1])
            outs = outs[2:]
        zs.append(outs[0])
        if last:
            dots_all = share(outs[2])
        else:
            r_in, state, extra = outs[1], outs[2:7], outs[7]
            parts = share(outs[8])

    (out,) = call(
        functools.partial(final_kernel, d),
        [(ngx, 4 * n0 // ngx, cx, cy)],
        [*coefs[:4], coefs[8], f, dots_all, *norms, *zs],
        [field(d, n0), field(d, n0), (2, n0, rows + 16, cy)],
        name="final",
    )
    got = lax.all_to_all(out, "gx", 0, 0)
    return tuple(
        call(
            functools.partial(unpack_kernel, d),
            [forcing.shape, forcing.shape],
            [got],
            name="unpack",
        )
    )


def solution(mesh):
    return jax.shard_map(
        body,
        mesh=mesh,
        in_specs=(
            P(None, None, "gx", "gy"),
            P(None, "gx", "gy"),
            P(None, "gx", "gy"),
            P("gx", "gy"),
            P("gx", "gy"),
            P("gx", "gy"),
            P("gx", "gy"),
        ),
        out_specs=(P(None, None, "gx", "gy"), P(None, None, "gx", "gy")),
        check_vma=False,
    )
```

```python
import functools

import jax
import jax.numpy as jnp
from jax import lax
from jax.experimental import pallas as pl
from jax.experimental.pallas import tpu as pltpu
from jax.sharding import PartitionSpec as P

ITERS = 3
LINE_WEIGHT = 0.8
POINT_WEIGHT = 0.7
COARSE_WEIGHT = 0.7
CSWEEPS = 4
REACH = 13 * ITERS + 1

VMEM = pl.BlockSpec(memory_space=pltpu.VMEM)
SMEM = pl.BlockSpec(memory_space=pltpu.SMEM)
F32 = jnp.float32


MOST_VMEM = 60 * 1024 * 1024
UNROLL = 6
PIECES = 3


def size_of(shape):
    count = 4
    for extent in shape[:-2]:
        count *= extent
    return count * (-(-shape[-2] // 8) * 8) * (-(-shape[-1] // 128) * 128)


def call(kernel, outs, args, scratch=(), name=None):
    specs = [SMEM if a.dtype == jnp.int32 and a.ndim == 1 else VMEM for a in args]
    shapes = [a.shape for a in args if a.ndim > 1] + list(outs) + list(scratch)
    room = sum(size_of(shape) for shape in shapes) * 9 // 8 + 4 * 1024 * 1024
    return pl.pallas_call(
        kernel,
        out_shape=[jax.ShapeDtypeStruct(s, F32) for s in outs],
        in_specs=specs,
        out_specs=[VMEM] * len(outs),
        scratch_shapes=[pltpu.VMEM(s, F32) for s in scratch],
        compiler_params=pltpu.CompilerParams(vmem_limit_bytes=min(room, MOST_VMEM)),
        name=name,
    )(*args)


class Dims:
    def __init__(self, ngx, ngy, layers, cx, cy):
        self.ngx, self.ngy, self.n = ngx, ngy, ngx * ngy
        self.layers, self.cx, self.cy = layers, cx, cy
        self.rows = ngx * cx
        self.strip = cy // ngx
        self.halo = (cy - self.strip) // 2
        self.groups = self.rows // 8
        self.slots = cy // REACH
        self.packed = -(-self.groups // self.slots)
        self.window = 4 * layers + 4
        self.planes = self.window + 6
        self.parts = -(-2 * ngx // 8) * 8
        self.piece = self.planes // PIECES
        assert self.piece * PIECES == self.planes and self.piece >= layers + 10


def loop(lo, hi, step, init, by=None):
    if by is None:
        by = UNROLL
    trips = (hi - lo) // by

    def trip(t, carry):
        for q in range(by):
            carry = step(lo + t * by + q, carry)
        return carry

    carry = lax.fori_loop(0, trips, trip, init)
    for k in range(lo + trips * by, hi):
        carry = step(k, carry)
    return carry


def lanes(shape):
    return lax.broadcasted_iota(jnp.int32, shape, len(shape) - 1)


def turn(x, shift, axis):
    return pltpu.roll(x, shift, axis)


class Level:
    def __init__(self, d, n, g, s, inv, face, cross, mask, mu, fw):
        self.d, self.n, self.g, self.s, self.inv, self.face = d, n, g, s, inv, face
        self.cross, self.mask, self.mu, self.fw = cross, mask, mu, fw

    def clear_rim(self):
        rows, cy = self.d.rows, self.d.cy
        for v in range(2):
            self.mu[v, :, 0:8, :] = jnp.zeros((self.n, 8, cy), F32)
            self.mu[v, :, 8 + rows : 16 + rows, :] = jnp.zeros((self.n, 8, cy), F32)

    def put_masked(self, v, k, value):
        self.mu[v, k, 8 : 8 + self.d.rows, :] = self.mask[...] * value

    def beside(self, v, k):
        rows, cy = self.d.rows, self.d.cy
        here = self.mu[v, k, 8 : 8 + rows, :]
        return (
            self.mu[v, k, 7 : 7 + rows, :]
            + self.mu[v, k, 9 : 9 + rows, :]
            + (turn(here, 1, 1) + turn(here, cy - 1, 1))
        )

    def apply(self, u, v, k, bottom=False):
        out = self.g[k] * u[v, k] - self.s[k] * self.beside(v, k)
        if self.n > 1:
            pick_int = isinstance(k, int)
            above = min(k + 1, self.n - 1) if pick_int else jnp.minimum(k + 1, self.n - 1)
            below = max(k - 1, 0) if pick_int else jnp.maximum(k - 1, 0)
            out = out - (self.face[k + 1] * u[v, above] + self.face[k] * u[v, below])
        if bottom:
            out = out + self.cross[...] * u[1 - v, k]
        return out

    def sweep(self, r, u, first=False):
        n = self.n
        start = []
        for v in range(2):
            right = r[v, 0]
            if not first:
                right = right + self.s[0] * self.beside(v, 0) - self.cross[...] * u[1 - v, 0]
            start.append(right * self.inv[0])
        for v in range(2):
            self.fw[v, 0] = start[v]

        def forward(k, carry):
            out = []
            for v in range(2):
                right = r[v, k]
                if not first:
                    right = right + self.s[k] * self.beside(v, k)
                value = (right + self.face[k] * carry[v]) * self.inv[k]
                self.fw[v, k] = value
                out.append(value)
            return tuple(out)

        last = loop(1, n, forward, tuple(start)) if n > 1 else tuple(start)

        def store(v, k, value):
            new = LINE_WEIGHT * value
            if not first:
                new = (1.0 - LINE_WEIGHT) * u[v, k] + new
            u[v, k] = new
            self.put_masked(v, k, new)

        for v in range(2):
            store(v, n - 1, last[v])

        def backward(t, carry):
            k = n - 1 - t
            out = []
            factor = self.face[k + 1] * self.inv[k]
            for v in range(2):
                value = self.fw[v, k] + factor * carry[v]
                store(v, k, value)
                out.append(value)
            return tuple(out)

        if n > 1:
            loop(1, n, backward, last)


def level_set(d, coefs, mu0, fw0, mu1, fw1, mu2, fw2):
    g0, s0, i0, f0, g1, s1, i1, f1, low = coefs
    cross, mask = low.at[3], low.at[4]
    rows = d.rows
    one = lambda at: low.at[at : at + 1]
    return (
        Level(d, d.layers, g0, s0, i0, f0, cross, mask, mu0, fw0),
        Level(d, d.layers // 2, g1, s1, i1, f1, cross, mask, mu1, fw1),
        Level(d, 1, one(0), one(1), one(2), None, cross, mask, mu2, fw2),
    )


def coef_shapes(d):
    n0, n1, r, c = d.layers, d.layers // 2, d.rows, d.cy
    plane = lambda n: (n, r, c)
    return [
        plane(n0), plane(n0), plane(n0), plane(n0 + 1),
        plane(n1), plane(n1), plane(n1), plane(n1 + 1),
        plane(6),
    ]


def field(d, n):
    return (2, n, d.rows, d.cy)


def work_shapes(d):
    out = []
    for n in (d.layers, d.layers // 2, 1):
        out += [(2, n, d.rows + 16, d.cy), field(d, n)]
    return out


def own_lanes(d, shape):
    lane = lanes(shape)
    return (lane >= d.halo) & (lane < d.halo + d.strip)


def segment_acc(d, ids_row, fetch, count):
    cy = d.cy
    wanted = lax.broadcasted_iota(jnp.int32, (cy, cy), 0).astype(F32)
    acc = [jnp.zeros((cy, cy), F32) for _ in range(count)]
    for r in range(d.cx):
        hit = ids_row(r) == wanted
        for t in range(count):
            acc[t] = acc[t] + jnp.where(hit, fetch(t, r), 0.0)
    return acc


def restrict_strip(d, strip_ids, e_ref, pack, chunk):
    lane = lanes((d.cx, d.cy))
    for v in range(2):
        out = jnp.zeros((d.cx, d.cy), F32)
        for g in range(d.ngx):
            shift = (d.strip * g - d.halo) % d.cy
            part = turn(e_ref[v, g * d.cx : (g + 1) * d.cx, :], shift, 1)
            out = jnp.where(lane // d.strip == g, part, out)
        pack[v] = out
    acc = segment_acc(d, lambda r: strip_ids[r : r + 1, :], lambda t, r: pack[t, r : r + 1, :], 2)
    for v in range(2):
        sums = acc[v].T.reshape(d.ngx, d.strip, d.cy).sum(axis=1)
        chunk[v * d.ngx : (v + 1) * d.ngx, :] = sums


def descend(d, levels, r0, u0, r1, u1, r2, u2, strip_ids, e2, pack, chunk):
    l0, l1, l2 = levels
    half = l0.n // 2
    l0.sweep(r0, u0, first=True)
    l0.sweep(r0, u0)

    def residual_pair(kk, bottom):
        for v in range(2):
            low = r0[v, 2 * kk] - l0.apply(u0, v, 2 * kk, bottom)
            high = r0[v, 2 * kk + 1] - l0.apply(u0, v, 2 * kk + 1)
            r1[v, kk] = low + high

    residual_pair(0, True)
    loop(1, half, lambda k, c: (residual_pair(k, False), c)[1], 0)
    l1.sweep(r1, u1, first=True)
    l1.sweep(r1, u1)
    zero = tuple(r1[v, 0] - l1.apply(u1, v, 0, True) for v in range(2))
    total = loop(
        1,
        half,
        lambda k, c: tuple(c[v] + (r1[v, k] - l1.apply(u1, v, k)) for v in range(2)),
        zero,
    )
    for v in range(2):
        r2[v, 0] = total[v]
    l2.sweep(r2, u2, first=True)
    l2.sweep(r2, u2)
    for v in range(2):
        e2[v] = r2[v, 0] - l2.apply(u2, v, 0, True)
    restrict_strip(d, strip_ids, e2, pack, chunk)


def ascend(d, levels, r0, u0, u0i, r1, u1, u1i, r2, u2):
    l0, l1, l2 = levels
    for v in range(2):
        l2.put_masked(v, 0, u2[v, 0])
    for _ in range(2):
        l2.sweep(r2, u2)

    def add1(k, c):
        for v in range(2):
            value = u1i[v, k] + u2[v, 0]
            u1[v, k] = value
            l1.put_masked(v, k, value)
        return c

    loop(0, l1.n, add1, 0)
    for _ in range(2):
        l1.sweep(r1, u1)

    def add0(k, c):
        for v in range(2):
            for p in range(2):
                value = u0i[v, 2 * k + p] + u1[v, k]
                u0[v, 2 * k + p] = value
                l0.put_masked(v, 2 * k + p, value)
        return c

    loop(0, l1.n, add0, 0)
    for _ in range(2):
        l0.sweep(r0, u0)


def pick(row, ids):
    return jnp.take_along_axis(
        jnp.broadcast_to(row, ids.shape), ids, axis=1, mode="promise_in_bounds"
    )


def spread_chunk(d, out, chunk):
    value = chunk[...]
    for i in range(d.n):
        out[i] = value


def pack_planes(d, place, gathered, count, put):
    first = place[3]

    def body(p, c):
        lane = lanes((8, d.cy))
        for o in range(d.packed):
            value = jnp.zeros((8, d.cy), F32)
            for s in range(d.slots):
                rg = o * d.slots + s
                if rg >= d.groups:
                    break
                block, at = rg * 8 // d.cx, rg * 8 % d.cx
                x = gathered[block, p, at : at + 8, :]
                x = turn(x, lax.rem(REACH * s - first + d.cy, d.cy), 1)
                keep = (lane >= REACH * s) & (lane < REACH * (s + 1))
                value = jnp.where(keep, x, value)
            put(p * d.packed + o, value)
        return c

    loop(0, count, body, 0)


def pack_kernel(d, count, place, *refs):
    *pieces, out = refs
    for t, piece in enumerate(pieces):
        def put(at, value, t=t):
            out[t * d.piece * d.packed + at] = value
        pack_planes(d, place, piece, count, put)


def segments(d):
    n0, out = d.layers, []
    for piece in range(PIECES):
        at, end = piece * d.piece, min((piece + 1) * d.piece, d.window)
        while at < end:
            part = min(at // n0, 2)
            stop = min(end, (part + 1) * n0 if part < 2 else d.window)
            out.append((piece, at - piece * d.piece, stop - at, part if part < 2 else None, at - part * n0))
            at = stop
    return out


def setup_kernel(d, place, *rest):
    all_gathered, bulk, last_ref, rest = rest[:PIECES], rest[PIECES], rest[PIECES + 1], rest[PIECES + 2 :]
    (f, g0, s0, i0, f0, g1, s1, i1, f1, low, strip_ids) = rest[:11]
    (u0, r1, u1, r2, u2, big) = rest[11:17]
    (win, chunk, e2, pack, mu0, fw0, mu1, fw1, mu2, fw2) = rest[17:]
    n0, n1, rows, cy, cx = d.layers, d.layers // 2, d.rows, d.cy, d.cx
    off, is_left = place[4], place[5]
    if d.parts > 2 * d.ngx:
        chunk[...] = jnp.zeros(chunk.shape, F32)

    def window(gathered, packed, p, put):
        lane = lanes((8, cy))
        off_own = lax.rem(off + cy, cy)
        own = jnp.where(is_left == 1, (lane >= off).astype(jnp.int32), (lane < cy + off).astype(jnp.int32)) == 1
        lo = jnp.where(is_left == 1, off - REACH, cy + off)
        near = (lane >= lo) & (lane < lo + REACH)
        for rg in range(d.groups):
            block, at = rg * 8 // cx, rg * 8 % cx
            mid = turn(gathered[block, p, at : at + 8, :], off_own, 1)
            o, s = rg // d.slots, rg % d.slots
            side = turn(packed[p * d.packed + o], lax.rem(lo - REACH * s + 2 * cy, cy), 1)
            put(slice(rg * 8, rg * 8 + 8), jnp.where(own, mid, jnp.where(near, side, 0.0)))

    for piece, first, count, v, there in segments(d):
        def fill(t, c, piece=piece, first=first, v=v, there=there):
            def put(at, value):
                if v is None:
                    win[there + t, at, :] = value
                else:
                    f[v, there + t, at, :] = value
            packed = last_ref if piece == PIECES - 1 else bulk.at[pl.ds(piece * d.piece * d.packed, d.piece * d.packed)]
            window(all_gathered[piece], packed, first + t, put)
            return c

        loop(0, count, fill, 0)

    cpl, frc, msk = win[2 * n0], win[2 * n0 + 1], win[2 * n0 + 2]
    low[4] = msk
    low[5] = win[2 * n0 + 3]
    low[3] = frc * cpl * msk
    mask = low.at[4]
    nil = jnp.zeros((rows, cy), F32)
    f0[0] = nil
    f0[n0] = nil

    def faces(k, c):
        f0[k + 1] = 0.5 * (win[k] + win[k + 1]) * mask[...]
        return c

    loop(0, n0 - 1, faces, 0)

    def diag(k, extra):
        m = mask[...]
        sp = win[n0 + k]
        s0[k] = sp * m
        inner = f0[k] + f0[k + 1] + 4.0 * sp
        if extra is not None:
            inner = inner + extra
        value = m * inner + (1.0 - m)
        g0[k] = value
        return value

    i0[0] = 1.0 / diag(0, frc)

    def factor0(k, prev):
        face = f0[k]
        inv = 1.0 / (diag(k, None) - face * face * prev)
        i0[k] = inv
        return inv

    loop(1, n0, factor0, i0[0])

    def fold(k, total):
        g1[k] = g0[2 * k] + g0[2 * k + 1] - 2.0 * f0[2 * k + 1]
        s = s0[2 * k] + s0[2 * k + 1]
        s1[k] = s
        f1[k] = f0[2 * k]
        return total + s

    low[1] = loop(0, n1, fold, nil)
    f1[n1] = nil
    i1[0] = 1.0 / g1[0]

    def factor1(k, prev):
        face = f1[k]
        inv = 1.0 / (g1[k] - face * face * prev)
        i1[k] = inv
        return inv

    loop(1, n1, factor1, i1[0])
    diag2 = 4.0 * low[1] + mask[...] * win[2 * n0 + 1] + n0 * (1.0 - mask[...])
    low[0] = diag2
    low[2] = 1.0 / diag2

    lane = lanes((cx, cy))
    packed_ids = jnp.zeros((cx, cy), F32)
    for g in range(d.ngx):
        part = turn(low[5, g * cx : (g + 1) * cx, :], (d.strip * g - d.halo) % cy, 1)
        packed_ids = jnp.where(lane // d.strip == g, part, packed_ids)
    strip_ids[...] = packed_ids

    levels = level_set(d, (g0, s0, i0, f0, g1, s1, i1, f1, low), mu0, fw0, mu1, fw1, mu2, fw2)
    for one in levels:
        one.clear_rim()
    descend(d, levels, f, u0, r1, u1, r2, u2, strip_ids, e2, pack, chunk)
    spread_chunk(d, big, chunk)


COLUMN = 9


def inside_of(d):
    shape = (d.cx, d.cy)
    row = lax.broadcasted_iota(jnp.int32, shape, 0)
    lane = lanes(shape)
    return (row > 0, row < d.cx - 1, lane > 0, lane < d.cy - 1)


def column_kernel(d, place, got, out, table, tmp):
    n0, cx, cy = d.layers, d.cx, d.cy
    base = d.planes - d.piece
    at_spread, at_misc = 3 * n0 - base, 4 * n0 - base
    inside = inside_of(d)
    nil = jnp.zeros((cx, cy), F32)

    def sums(g):
        total = loop(0, n0, lambda k, t: t + got[g, at_spread + k], nil)
        return total * got[g, at_misc + 2]

    s2_all = [sums(g) for g in range(d.ngx)]
    table[...] = jnp.zeros(table.shape, F32)
    for g in range(d.ngx):
        fr, cp = got[g, at_misc + 1], got[g, at_misc]
        own = (got[g, at_misc + 2], got[g, at_misc + 3], s2_all[g])

        def around(t):
            q = own[t]
            up = (got[g - 1, at_misc + 2 + t] if t < 2 else s2_all[g - 1]) if g > 0 else nil
            down = (got[g + 1, at_misc + 2 + t] if t < 2 else s2_all[g + 1]) if g + 1 < d.ngx else nil
            left, right = got[g, at_misc + 4 + t], got[g, at_misc + 7 + t]
            return (
                jnp.where(inside[0], turn(q, 1, 0), turn(up, 1, 0)),
                jnp.where(inside[1], turn(q, cx - 1, 0), turn(down, cx - 1, 0)),
                jnp.where(inside[2], turn(q, 1, 1), turn(left, 1, 1)),
                jnp.where(inside[3], turn(q, cy - 1, 1), turn(right, cy - 1, 1)),
            )

        m, ids, s2 = own
        m_d, ids_d, s_d = around(0), around(1), around(2)
        g2 = 4.0 * s2 + m * fr + n0 * (1.0 - m)
        cross = fr * cp * m
        at = slice(g * cx, (g + 1) * cx)
        out[0, at, :], out[1, at, :], out[2, at, :], out[3, at, :] = g2, s2, cross, ids
        weight3, weight4 = g2, g2
        for t in range(4):
            out[4 + t, at, :] = m_d[t] * (1.0 + ids_d[t])
            weight3 = weight3 - jnp.where(inside[t] & (ids_d[t] == ids), s2 * m_d[t], 0.0)
            weight4 = weight4 - jnp.where(inside[t], s_d[t] * m, 0.0)
            tmp[3 + t] = jnp.where(inside[t], 0.0, s_d[t] * m)
        tmp[0], tmp[1], tmp[2] = weight3, cross, weight4
        ids_row = lambda r: out[3, g * cx + r : g * cx + r + 1, :]
        acc = segment_acc(d, ids_row, lambda _, r: tmp[0, r : r + 1, :], 1)
        out[8, at, :] = jnp.broadcast_to(acc[0].T.sum(axis=0, keepdims=True), (cx, cy))

        @pl.when(place[1] == g)
        def _():
            def one(t, c):
                acc = segment_acc(d, ids_row, lambda _, r: tmp[1 + t, r : r + 1, :], 1)
                table[pl.ds(2 + t, 1), :] = acc[0].T.sum(axis=0, keepdims=True)
                return c

            loop(0, 6, one, 0, 1)


def apply_block(d, cols, pos, g, rows, tmp, inside):
    at = pl.ds(pl.multiple_of(g * d.cx, d.cx), d.cx)
    shape = (d.cx, d.cy)
    ids = cols[pos, 3, at, :].astype(jnp.int32)
    here = [pick(rows[0][v], ids) for v in range(2)]
    side = [jnp.zeros(shape, F32), jnp.zeros(shape, F32)]
    for t in range(4):
        code = cols[pos, 4 + t, at, :].astype(jnp.int32) - 1
        live = code >= 0
        code = jnp.maximum(code, 0)
        for v in range(2):
            value = jnp.where(inside[t], pick(rows[0][v], code), pick(rows[1 + t][v], code))
            side[v] = side[v] + jnp.where(live, value, 0.0)
    g2, s2, cross = cols[pos, 0, at, :], cols[pos, 1, at, :], cols[pos, 2, at, :]
    for v in range(2):
        tmp[v] = g2 * here[v] + cross * here[1 - v] - s2 * side[v]
    acc = segment_acc(
        d,
        lambda r: cols[pos, 3, pl.ds(g * d.cx + r, 1), :],
        lambda t, r: tmp[t, r : r + 1, :],
        2,
    )
    return [acc[v].T.sum(axis=0, keepdims=True) for v in range(2)]


def diagonal(d, cols, pos, g):
    x = cols[pos, 8, pl.ds(g * d.cx, 1), :]
    return jnp.where(x == 0.0, 1.0, x)


def clip(x, top):
    return jnp.clip(x, 0, top - 1)


def point_first(d, step, place, parts, extra, *rest):
    if step == 0:
        near, column, opposite, far, cols, r3, big, tmp, chunk = rest
        at_near = jnp.where(place[5] == 1, 0, 2)

        def stack(p, c):
            cols[1, p], cols[3, p] = column[p], far[p]
            cols[at_near, p], cols[2 - at_near, p] = near[p], opposite[p]
            return c

        loop(0, COLUMN, stack, 0)
    else:
        cols, r3, big, tmp, chunk = rest
    ngx, ngy = d.ngx, d.ngy
    for v in range(2):
        for g in range(ngx):
            total = parts[0:ngy, v * ngx + g, :]
            for i in range(1, ngx):
                total = total + parts[i * ngy : (i + 1) * ngy, v * ngx + g, :]
            r3[v, g * ngy : (g + 1) * ngy, :] = total
    gx, gy = place[1], place[2]
    up, down = clip(gx - 1, ngx), clip(gx + 1, ngx)
    spots = (
        (1, gx, gy),
        (1, up, gy),
        (1, down, gy),
        (0, gx, clip(gy - 1, ngy)),
        (2, gx, clip(gy + 1, ngy)),
    )
    right, diag, rows = [], [], []
    for pos, g, c in spots:
        right.append([r3[v, pl.ds(g * ngy + c, 1), :] for v in range(2)])
        diag.append(diagonal(d, cols, pos, g))
        rows.append([POINT_WEIGHT * right[-1][v] / diag[-1] for v in range(2)])
    image = apply_block(d, cols, 1, gx, rows, tmp, inside_of(d))
    count = chunk.shape[0]
    chunk[2:count, :] = extra[2:count, :]
    for v in range(2):
        chunk[v : v + 1, :] = rows[0][v] + POINT_WEIGHT * (right[0][v] - image[v]) / diag[0]
    spread_chunk(d, big, chunk)


def correct_columns(d, place, parts, table, r3, cols, low, u2, y3, y4, y5, tmp):
    n, ngx, ngy = d.n, d.ngx, d.ngy
    gy, off, is_left = place[2], place[4], place[5]
    cross, inner = table[:, 2, :], table[:, 3, :]
    sides = [table[:, 4 + t, :] for t in range(4)]
    shape = (n, d.cy)

    def total(x):
        return jnp.broadcast_to(x.sum(axis=1, keepdims=True), shape)

    def couple(values):
        return (
            turn(values[1], ngy, 0)
            + turn(values[0], n - ngy, 0)
            + turn(values[3], 1, 0)
            + turn(values[2], n - 1, 0)
        )

    y2 = [parts[:, v, :] for v in range(2)]
    right = []
    for v in range(2):
        local = total(r3[v] - (inner * y2[v] + cross * y2[1 - v]))
        right.append(local + couple([total(s * y2[v]) for s in sides]))
    diag4, cross4 = total(inner), total(cross)
    sides4 = [total(s) for s in sides]
    x = [COARSE_WEIGHT * right[v] / diag4 for v in range(2)]
    for _ in range(CSWEEPS - 1):
        x = [
            x[v]
            + COARSE_WEIGHT
            * (right[v] - (diag4 * x[v] + cross4 * x[1 - v] - couple([s * x[v] for s in sides4])))
            / diag4
            for v in range(2)
        ]
    for v in range(2):
        y3[v] = y2[v] + x[v]

    def column(pos):
        far = jnp.where(is_left == 1, -2, 2)
        return gy + jnp.where(pos == 3, far, pos - 1)

    inside = inside_of(d)

    def relax(pos, g, rows, c, q):
        image = apply_block(d, cols, pos, g, rows, tmp.at[q], inside)
        diag = diagonal(d, cols, pos, g)
        at = pl.ds(g * ngy + c, 1)
        return [
            rows[0][v] + POINT_WEIGHT * (r3[v, at, :] - image[v]) / diag for v in range(2)
        ]

    def fourth(b, carry):
        for q in range(2):
            pos, g = lax.div(2 * b + q, ngx), lax.rem(2 * b + q, ngx)
            c = column(pos)
            get = lambda g, c: [
                y3[v, pl.ds(clip(g, ngx) * ngy + clip(c, ngy), 1), :] for v in range(2)
            ]
            rows = [get(g, c), get(g - 1, c), get(g + 1, c), get(g, c - 1), get(g, c + 1)]
            new = relax(pos, g, rows, clip(c, ngy), q)
            for v in range(2):
                y4[v, pl.ds(pos * ngx + g, 1), :] = new[v]
        return carry

    def fifth(b, carry):
        for q in range(2):
            t, g = lax.div(2 * b + q, ngx), lax.rem(2 * b + q, ngx)
            pos = t + 1 - is_left
            west = jnp.where(pos == 0, 3, pos - 1)
            east = jnp.where(pos == 2, 3, pos + 1)
            get = lambda g, p: [
                y4[v, pl.ds(p * ngx + clip(g, ngx), 1), :] for v in range(2)
            ]
            rows = [get(g, pos), get(g - 1, pos), get(g + 1, pos), get(g, west), get(g, east)]
            new = relax(pos, g, rows, clip(column(pos), ngy), q)
            for v in range(2):
                y5[v, pl.ds(t * ngx + g, 1), :] = new[v]
        return carry

    lax.fori_loop(0, 2 * ngx, fourth, 0)
    lax.fori_loop(0, ngx, fifth, 0)

    block = (d.cx, d.cy)
    lane = lanes(block)
    own = jnp.where(is_left == 1, (lane >= off).astype(jnp.int32), (lane < d.cy + off).astype(jnp.int32)) == 1
    for g in range(ngx):
        at = slice(g * d.cx, (g + 1) * d.cx)
        ids = low[5, at, :].astype(jnp.int32)
        for v in range(2):
            here = pick(y5[v, pl.ds(is_left * ngx + g, 1), :], ids)
            there = pick(y5[v, pl.ds((1 - is_left) * ngx + g, 1), :], ids)
            u2[v, 0, at, :] = u2[v, 0, at, :] + jnp.where(own, here, there)


def grid_totals(d, dots, count):
    x = dots[:, 2, :].sum(axis=0, keepdims=True)
    lane = lanes((1, d.cy))
    return [
        jnp.broadcast_to(
            jnp.where(lane == t, x, 0.0).sum(axis=1, keepdims=True), (1, d.cy)
        )
        for t in range(count)
    ]


def column_of(d, dots, step, norm=None):
    values = grid_totals(d, dots, step + 2 + (step == 0))
    if step == 0:
        square = values[2]
        norm = jnp.sqrt(square)
        inner, height = [values[0] / square], values[1] / square
    else:
        inner, height = [values[0] / norm] + values[1:-1], values[-1]
    for value in inner:
        height = height - value * value
    return inner + [jnp.sqrt(height)], norm


def step_kernel(d, step, last, *refs):
    it = iter(refs)
    take = lambda count: [next(it) for _ in range(count)]
    (place,) = take(1)
    coefs = take(9)
    (strip_ids, r_in, u0i, r1i, u1i, r2i, u2i) = take(7)
    (parts, table, r3, cols) = take(4)
    norm_in = take(1)[0] if step > 1 else None
    olds_v = take(step)
    olds_z = take(step)
    if step:
        (v_out, col) = take(2)
    (z_out,) = take(1)
    if last:
        (dots_out, big) = take(2)
        w = take(1)[0]
        u0n = None
    else:
        (w, u0n, r1n, u1n, r2n, u2n, dots_out, big) = take(8)
    (u0, u1, u2, y3, y4, y5, tmp, chunk, e2, pack, mu0, fw0, mu1, fw1, mu2, fw2) = take(16)
    low = coefs[8]
    levels = level_set(d, coefs, mu0, fw0, mu1, fw1, mu2, fw2)
    for one in levels:
        one.clear_rim()
    n0, n1 = d.layers, d.layers // 2

    for v in range(2):
        u2[v, 0] = u2i[v, 0]
    correct_columns(d, place, parts, table, r3, cols, low, u2, y3, y4, y5, tmp)
    if not last and d.parts > 2 * d.ngx:
        chunk[...] = jnp.zeros(chunk.shape, F32)

    ascend(d, levels, r_in, u0, u0i, r1i, u1, u1i, r2i, u2)

    l0 = levels[0]
    if step:
        norm = norm_in[step : step + 1, :] if step > 1 else None
        column, norm = column_of(d, parts, step - 1, norm)
        height = column[-1]
        if step == 1:
            inner, scale = [column[0]], 1.0 / (height * norm)
        else:
            inner, scale = [column[0] / norm] + column[1:-1], 1.0 / height
        for t, value in enumerate(column + [norm]):
            col[t : t + 1, :] = value

    def scaled(k, c):
        for v in range(2):
            z = u0[v, k]
            if step:
                vec = r_in[v, k]
                for t in range(step):
                    vec = vec - inner[t] * olds_v[t][v, k]
                    z = z - inner[t] * olds_z[t][v, k]
                v_out[v, k] = vec * scale
                z = z * scale
            z_out[v, k] = z
            l0.put_masked(v, k, z)
        return c

    loop(0, n0, scaled, 0)
    basis = list(olds_v) + [v_out if step else r_in]

    own = own_lanes(d, (8, d.cy))

    def fold(x):
        total = x[0:8]
        for t in range(1, d.groups):
            total = total + x[8 * t : 8 * t + 8]
        return total

    def image(k, acc, bottom=False):
        acc = list(acc)
        for v in range(2):
            value = l0.apply(z_out, v, k, bottom)
            w[v, k] = value
            for t, vec in enumerate(basis):
                acc[t] = acc[t] + fold(vec[v, k] * value)
            acc[step + 1] = acc[step + 1] + fold(value * value)
            if step == 0:
                acc[2] = acc[2] + fold(r_in[v, k] * r_in[v, k])
        return tuple(acc)

    nil = jnp.zeros((8, d.cy), F32)
    acc = image(0, (nil,) * (step + 2 + (step == 0)), True)
    acc = loop(1, n0, image, acc)
    lane = lanes((1, d.cy))
    row = jnp.zeros((1, d.cy), F32)
    for t, value in enumerate(acc):
        value = jnp.where(own, value, 0.0).sum(axis=0, keepdims=True)
        row = jnp.where(lane == t, value.sum(axis=1, keepdims=True), row)
    dots_out[...] = jnp.zeros(dots_out.shape, F32)
    dots_out[2:3, :] = row
    if last:
        spread_chunk(d, big, dots_out)
    else:
        descend(d, levels, w, u0n, r1n, u1n, r2n, u2n, strip_ids, e2, pack, chunk)
        spread_chunk(d, big, chunk)


def least_squares(columns, initial_norm):
    count = len(columns)
    rows = [[columns[c][r] for c in range(count)] for r in range(count + 1)]
    target = [initial_norm] + [jnp.zeros_like(initial_norm) for _ in range(count)]
    for p in range(count):
        top, low = rows[p][p], rows[p + 1][p]
        radius = jnp.sqrt(top * top + low * low)
        cosine, sine = top / radius, low / radius
        for c in range(p, count):
            upper, lower = rows[p][c], rows[p + 1][c]
            rows[p][c] = cosine * upper + sine * lower
            rows[p + 1][c] = cosine * lower - sine * upper
        upper, lower = target[p], target[p + 1]
        target[p] = cosine * upper + sine * lower
        target[p + 1] = cosine * lower - sine * upper
    weights = [None] * count
    for p in reversed(range(count)):
        partial = target[p]
        for c in range(p + 1, count):
            partial = partial - rows[p][c] * weights[c]
        weights[p] = partial / rows[p][p]
    return weights


def final_kernel(d, g0, s0, i0, f0, low, f, dots, *refs):
    cols, zs = refs[: ITERS - 1], refs[ITERS - 1 : 2 * ITERS - 1]
    out, x, res, mu0 = refs[2 * ITERS - 1 :]
    n0 = d.layers
    nil = jnp.zeros((1, d.cy), F32)
    columns = []
    norm = cols[0][2:3, :]
    for j in range(ITERS):
        if j + 1 < ITERS:
            column = [cols[j][t : t + 1, :] for t in range(j + 2)]
        else:
            column, _ = column_of(d, dots, j, norm)
        columns.append(column + [nil] * (ITERS - 1 - j))
    weights = least_squares(columns, norm)
    weights[0] = weights[0] / norm
    l0 = Level(d, n0, g0, s0, i0, f0, low.at[3], low.at[4], mu0, None)
    l0.clear_rim()

    def combine(k, c):
        for v in range(2):
            value = weights[0] * zs[0][v, k]
            for j in range(1, ITERS):
                value = value + weights[j] * zs[j][v, k]
            x[v, k] = value
            l0.put_masked(v, k, value)
        return c

    loop(0, n0, combine, 0)

    def rest(k, bottom):
        for v in range(2):
            res[v, k] = f[v, k] - l0.apply(x, v, k, bottom)

    rest(0, True)
    loop(1, n0, lambda k, c: (rest(k, False), c)[1], 0)

    per = 4 * n0 // d.ngx
    lane = lanes((d.cx, d.cy))
    for q in range(d.ngx):
        shift = (d.strip * q - d.halo) % d.cy
        keep = lane // d.strip == q

        def place_plane(p, c, q=q, shift=shift, keep=keep):
            plane = q * per + p
            for dest in range(d.ngx):
                at = slice(dest * d.cx, (dest + 1) * d.cx)
                source = x if (q * per) < 2 * n0 else res
                local = plane if (q * per) < 2 * n0 else plane - 2 * n0
                v = (q * per) // n0 % 2
                value = turn(source[v, local - v * n0, at, :], shift, 1)
                if q == 0:
                    out[dest, p] = value
                else:
                    out[dest, p] = jnp.where(keep, value, out[dest, p])
            return c

        loop(0, per, place_plane, 0)


def unpack_kernel(d, got, solution_out, residual_out):
    n0 = d.layers
    per = 4 * n0 // d.ngx
    lane = lanes((d.cx, d.cy))
    for q in range(d.ngx):
        def body(p, c, q=q):
            value = None
            for src in range(d.ngx):
                part = turn(got[src, p], (d.strip * (src - q)) % d.cy, 1)
                value = part if value is None else jnp.where(lane // d.strip == src, part, value)
            first = q * per
            target = solution_out if first < 2 * n0 else residual_out
            v = first // n0 % 2
            target[v, first % n0 + p] = value
            return c

        loop(0, per, body, 0)


def body(forcing, viscosity, spread, coupling, friction, ice_mask, aggregates):
    ngx, ngy = lax.axis_size("gx"), lax.axis_size("gy")
    layers, cx, cy = viscosity.shape
    d = Dims(ngx, ngy, layers, cx, cy)
    both = ("gx", "gy")
    gx, gy = lax.axis_index("gx"), lax.axis_index("gy")
    is_left = gx < ngx // 2
    off = d.halo - d.strip * gx
    first = jnp.where(is_left, cy - REACH, 0)
    place = jnp.stack([gx * ngy + gy, gx, gy, first, off, is_left.astype(jnp.int32)]).astype(jnp.int32)

    mask_f, ids_f = ice_mask.astype(F32), aggregates.astype(F32)
    mine = jnp.stack([mask_f, ids_f, spread.sum(axis=0) * mask_f])
    shift = lambda by: [(i, i + by) for i in range(ngy) if 0 <= i + by < ngy]
    left = lax.ppermute(mine, "gy", shift(1))
    right = lax.ppermute(mine, "gy", shift(-1))
    planes = [
        forcing.reshape(2 * layers, cx, cy),
        viscosity,
        spread,
        jnp.stack([coupling, friction, mask_f, ids_f]),
        left,
        right,
    ]
    pieces, start = [[] for _ in range(PIECES)], 0
    for part in planes:
        end = start + part.shape[0]
        for t in range(PIECES):
            low, high = max(start, t * d.piece), min(end, (t + 1) * d.piece)
            if low < high:
                pieces[t].append(part[low - start : high - start])
        start = end
    def sided(by):
        return [
            (i * ngy + j, i * ngy + to)
            for i in range(ngx)
            for j in range(ngy)
            for to in [j + by if i < ngx // 2 else j - by]
            if 0 <= to < ngy
        ]

    gathered, packed = [], []
    for t in range(PIECES):
        got = lax.all_gather(jnp.concatenate(pieces[t]), "gx")
        gathered.append(got)
        if t >= PIECES - 2:
            use = gathered[t:] if t == PIECES - 1 else gathered
            count = d.window - t * d.piece if t == PIECES - 1 else d.piece
            (sent,) = call(
                functools.partial(pack_kernel, d, count),
                [(len(use) * count * d.packed, 8, cy)],
                [place, *use],
                name="pack",
            )
            packed.append(lax.ppermute(sent, both, sided(1)))
    column, table_own = call(
        functools.partial(column_kernel, d),
        [(COLUMN, d.rows, cy), (8, cy)],
        [place, gathered[-1]],
        [(7, cx, cy)],
        name="column",
    )
    near = lax.ppermute(column, both, sided(1))
    opposite = lax.ppermute(column, both, sided(-1))
    far = lax.ppermute(column, both, sided(2))

    n0, n1, rows = layers, layers // 2, d.rows
    fields = [field(d, n0), field(d, n1), field(d, n1), field(d, 1), field(d, 1)]
    big_shape = lambda count: (d.n, count, cy)
    state_work = [(2, rows, cy), (2, cx, cy)] + work_shapes(d)
    outs = call(
        functools.partial(setup_kernel, d),
        [field(d, n0)] + coef_shapes(d) + [(cx, cy)] + fields + [big_shape(d.parts)],
        [place, *gathered, *packed],
        [(2 * n0 + 4, rows, cy), (d.parts, cy)] + state_work,
        name="setup",
    )
    f, coefs, strip_ids, state, big = outs[0], outs[1:10], outs[10], outs[11:16], outs[16]

    def share(x):
        return lax.all_to_all(x, both, 0, 0)

    big, near, opposite, far = lax.optimization_barrier((big, near, opposite, far))
    parts = share(big)
    extra = table_own
    vs, zs, norms = [f], [], []
    pair = (2, d.n, cy)
    r_in = f
    for step in range(ITERS):
        count = 4 if step else 8
        outs = call(
            functools.partial(point_first, d, step),
            ([] if step else [(4, COLUMN, rows, cy)]) + [pair, big_shape(count)],
            [place, parts, extra] + ([cols] if step else [near, column, opposite, far]),
            [(2, cx, cy), (count, cy)],
            name="point_first",
        )
        r3, big = outs[-2:]
        parts = share(big)
        if step == 0:
            cols, table = outs[0], parts
        last = step + 1 == ITERS
        outs_shapes = [field(d, n0), (8, cy)] if step else []
        outs_shapes += [field(d, n0)]
        if last:
            outs_shapes += [(4, cy), big_shape(4)]
        else:
            outs_shapes += [field(d, n0)] + fields + [(4, cy), big_shape(d.parts)]
        scratch = [field(d, n0)] if last else []
        scratch += [field(d, n0), field(d, n1), field(d, 1), pair]
        scratch += [(2, 4 * ngx, cy), (2, 2 * ngx, cy), (2, 2, cx, cy), (d.parts, cy)] + state_work
        outs = call(
            functools.partial(step_kernel, d, step, last),
            outs_shapes,
            [place, *coefs, strip_ids, r_in, *state, parts, table, r3, cols]
            + norms[step - 2 : step - 1 if step > 1 else 0]
            + (vs[:step] + zs),
            scratch,
            name="step",
        )
        if step:
            vs.append(outs[0])
            norms.append(outs[1])
            outs = outs[2:]
        zs.append(outs[0])
        if last:
            dots_all = share(outs[2])
        else:
            r_in, state, extra = outs[1], outs[2:7], outs[7]
            parts = share(outs[8])

    (out,) = call(
        functools.partial(final_kernel, d),
        [(ngx, 4 * n0 // ngx, cx, cy)],
        [*coefs[:4], coefs[8], f, dots_all, *norms, *zs],
        [field(d, n0), field(d, n0), (2, n0, rows + 16, cy)],
        name="final",
    )
    got = lax.all_to_all(out, "gx", 0, 0)
    return tuple(
        call(
            functools.partial(unpack_kernel, d),
            [forcing.shape, forcing.shape],
            [got],
            name="unpack",
        )
    )


def solution(mesh):
    return jax.shard_map(
        body,
        mesh=mesh,
        in_specs=(
            P(None, None, "gx", "gy"),
            P(None, "gx", "gy"),
            P(None, "gx", "gy"),
            P("gx", "gy"),
            P("gx", "gy"),
            P("gx", "gy"),
            P("gx", "gy"),
        ),
        out_specs=(P(None, None, "gx", "gy"), P(None, None, "gx", "gy")),
        check_vma=False,
    )
```

```python
import functools

import jax
import jax.numpy as jnp
from jax import lax
from jax.experimental import pallas as pl
from jax.experimental.pallas import tpu as pltpu
from jax.sharding import PartitionSpec as P

ITERS = 3
LINE_WEIGHT = 0.8
POINT_WEIGHT = 0.7
COARSE_WEIGHT = 0.7
CSWEEPS = 4
REACH = 13 * ITERS + 1

VMEM = pl.BlockSpec(memory_space=pltpu.VMEM)
SMEM = pl.BlockSpec(memory_space=pltpu.SMEM)
F32 = jnp.float32


MOST_VMEM = 60 * 1024 * 1024
UNROLL = 6
PIECES = 3


def size_of(shape):
    count = 4
    for extent in shape[:-2]:
        count *= extent
    return count * (-(-shape[-2] // 8) * 8) * (-(-shape[-1] // 128) * 128)


def call(kernel, outs, args, scratch=(), name=None):
    specs = [SMEM if a.dtype == jnp.int32 and a.ndim == 1 else VMEM for a in args]
    shapes = [a.shape for a in args if a.ndim > 1] + list(outs) + list(scratch)
    room = sum(size_of(shape) for shape in shapes) * 9 // 8 + 4 * 1024 * 1024
    return pl.pallas_call(
        kernel,
        out_shape=[jax.ShapeDtypeStruct(s, F32) for s in outs],
        in_specs=specs,
        out_specs=[VMEM] * len(outs),
        scratch_shapes=[pltpu.VMEM(s, F32) for s in scratch],
        compiler_params=pltpu.CompilerParams(vmem_limit_bytes=min(room, MOST_VMEM)),
        name=name,
    )(*args)


class Dims:
    def __init__(self, ngx, ngy, layers, cx, cy):
        self.ngx, self.ngy, self.n = ngx, ngy, ngx * ngy
        self.layers, self.cx, self.cy = layers, cx, cy
        self.rows = ngx * cx
        self.strip = cy // ngx
        self.halo = (cy - self.strip) // 2
        self.groups = self.rows // 8
        self.slots = cy // REACH
        self.packed = -(-self.groups // self.slots)
        self.planes = 4 * layers + 4
        self.parts = -(-2 * ngx // 8) * 8
        self.piece = self.planes // PIECES
        assert self.piece * PIECES == self.planes and self.piece >= layers + 4


def loop(lo, hi, step, init, by=None):
    if by is None:
        by = UNROLL
    trips = (hi - lo) // by

    def trip(t, carry):
        for q in range(by):
            carry = step(lo + t * by + q, carry)
        return carry

    carry = lax.fori_loop(0, trips, trip, init)
    for k in range(lo + trips * by, hi):
        carry = step(k, carry)
    return carry


def lanes(shape):
    return lax.broadcasted_iota(jnp.int32, shape, len(shape) - 1)


def turn(x, shift, axis):
    return pltpu.roll(x, shift, axis)


class Level:
    def __init__(self, d, n, g, s, inv, face, cross, mask, mu, fw):
        self.d, self.n, self.g, self.s, self.inv, self.face = d, n, g, s, inv, face
        self.cross, self.mask, self.mu, self.fw = cross, mask, mu, fw

    def clear_rim(self):
        rows, cy = self.d.rows, self.d.cy
        for v in range(2):
            self.mu[v, :, 0:8, :] = jnp.zeros((self.n, 8, cy), F32)
            self.mu[v, :, 8 + rows : 16 + rows, :] = jnp.zeros((self.n, 8, cy), F32)

    def put_masked(self, v, k, value):
        self.mu[v, k, 8 : 8 + self.d.rows, :] = self.mask[...] * value

    def beside(self, v, k):
        rows, cy = self.d.rows, self.d.cy
        here = self.mu[v, k, 8 : 8 + rows, :]
        return (
            self.mu[v, k, 7 : 7 + rows, :]
            + self.mu[v, k, 9 : 9 + rows, :]
            + (turn(here, 1, 1) + turn(here, cy - 1, 1))
        )

    def apply(self, u, v, k, bottom=False):
        out = self.g[k] * u[v, k] - self.s[k] * self.beside(v, k)
        if self.n > 1:
            pick_int = isinstance(k, int)
            above = min(k + 1, self.n - 1) if pick_int else jnp.minimum(k + 1, self.n - 1)
            below = max(k - 1, 0) if pick_int else jnp.maximum(k - 1, 0)
            out = out - (self.face[k + 1] * u[v, above] + self.face[k] * u[v, below])
        if bottom:
            out = out + self.cross[...] * u[1 - v, k]
        return out

    def sweep(self, r, u, first=False):
        n = self.n
        start = []
        for v in range(2):
            right = r[v, 0]
            if not first:
                right = right + self.s[0] * self.beside(v, 0) - self.cross[...] * u[1 - v, 0]
            start.append(right * self.inv[0])
        for v in range(2):
            self.fw[v, 0] = start[v]

        def forward(k, carry):
            out = []
            for v in range(2):
                right = r[v, k]
                if not first:
                    right = right + self.s[k] * self.beside(v, k)
                value = (right + self.face[k] * carry[v]) * self.inv[k]
                self.fw[v, k] = value
                out.append(value)
            return tuple(out)

        last = loop(1, n, forward, tuple(start)) if n > 1 else tuple(start)

        def store(v, k, value):
            new = LINE_WEIGHT * value
            if not first:
                new = (1.0 - LINE_WEIGHT) * u[v, k] + new
            u[v, k] = new
            self.put_masked(v, k, new)

        for v in range(2):
            store(v, n - 1, last[v])

        def backward(t, carry):
            k = n - 1 - t
            out = []
            factor = self.face[k + 1] * self.inv[k]
            for v in range(2):
                value = self.fw[v, k] + factor * carry[v]
                store(v, k, value)
                out.append(value)
            return tuple(out)

        if n > 1:
            loop(1, n, backward, last)


def level_set(d, coefs, mu0, fw0, mu1, fw1, mu2, fw2):
    g0, s0, i0, f0, g1, s1, i1, f1, low = coefs
    cross, mask = low.at[3], low.at[4]
    rows = d.rows
    one = lambda at: low.at[at : at + 1]
    return (
        Level(d, d.layers, g0, s0, i0, f0, cross, mask, mu0, fw0),
        Level(d, d.layers // 2, g1, s1, i1, f1, cross, mask, mu1, fw1),
        Level(d, 1, one(0), one(1), one(2), None, cross, mask, mu2, fw2),
    )


def coef_shapes(d):
    n0, n1, r, c = d.layers, d.layers // 2, d.rows, d.cy
    plane = lambda n: (n, r, c)
    return [
        plane(n0), plane(n0), plane(n0), plane(n0 + 1),
        plane(n1), plane(n1), plane(n1), plane(n1 + 1),
        plane(6),
    ]


def field(d, n):
    return (2, n, d.rows, d.cy)


def work_shapes(d):
    out = []
    for n in (d.layers, d.layers // 2, 1):
        out += [(2, n, d.rows + 16, d.cy), field(d, n)]
    return out


def own_lanes(d, shape):
    lane = lanes(shape)
    return (lane >= d.halo) & (lane < d.halo + d.strip)


def segment_acc(d, ids_row, fetch, count):
    cy = d.cy
    wanted = lax.broadcasted_iota(jnp.int32, (cy, cy), 0).astype(F32)
    acc = [jnp.zeros((cy, cy), F32) for _ in range(count)]
    for r in range(d.cx):
        hit = ids_row(r) == wanted
        for t in range(count):
            acc[t] = acc[t] + jnp.where(hit, fetch(t, r), 0.0)
    return acc


def restrict_strip(d, strip_ids, e_ref, pack, chunk):
    lane = lanes((d.cx, d.cy))
    for v in range(2):
        out = jnp.zeros((d.cx, d.cy), F32)
        for g in range(d.ngx):
            shift = (d.strip * g - d.halo) % d.cy
            part = turn(e_ref[v, g * d.cx : (g + 1) * d.cx, :], shift, 1)
            out = jnp.where(lane // d.strip == g, part, out)
        pack[v] = out
    acc = segment_acc(d, lambda r: strip_ids[r : r + 1, :], lambda t, r: pack[t, r : r + 1, :], 2)
    for v in range(2):
        sums = acc[v].T.reshape(d.ngx, d.strip, d.cy).sum(axis=1)
        chunk[v * d.ngx : (v + 1) * d.ngx, :] = sums


def descend(d, levels, r0, u0, r1, u1, r2, u2, strip_ids, e2, pack, chunk):
    l0, l1, l2 = levels
    half = l0.n // 2
    l0.sweep(r0, u0, first=True)
    l0.sweep(r0, u0)

    def residual_pair(kk, bottom):
        for v in range(2):
            low = r0[v, 2 * kk] - l0.apply(u0, v, 2 * kk, bottom)
            high = r0[v, 2 * kk + 1] - l0.apply(u0, v, 2 * kk + 1)
            r1[v, kk] = low + high

    residual_pair(0, True)
    loop(1, half, lambda k, c: (residual_pair(k, False), c)[1], 0)
    l1.sweep(r1, u1, first=True)
    l1.sweep(r1, u1)
    zero = tuple(r1[v, 0] - l1.apply(u1, v, 0, True) for v in range(2))
    total = loop(
        1,
        half,
        lambda k, c: tuple(c[v] + (r1[v, k] - l1.apply(u1, v, k)) for v in range(2)),
        zero,
    )
    for v in range(2):
        r2[v, 0] = total[v]
    l2.sweep(r2, u2, first=True)
    l2.sweep(r2, u2)
    for v in range(2):
        e2[v] = r2[v, 0] - l2.apply(u2, v, 0, True)
    restrict_strip(d, strip_ids, e2, pack, chunk)


def ascend(d, levels, r0, u0, u0i, r1, u1, u1i, r2, u2):
    l0, l1, l2 = levels
    for v in range(2):
        l2.put_masked(v, 0, u2[v, 0])
    for _ in range(2):
        l2.sweep(r2, u2)

    def add1(k, c):
        for v in range(2):
            value = u1i[v, k] + u2[v, 0]
            u1[v, k] = value
            l1.put_masked(v, k, value)
        return c

    loop(0, l1.n, add1, 0)
    for _ in range(2):
        l1.sweep(r1, u1)

    def add0(k, c):
        for v in range(2):
            for p in range(2):
                value = u0i[v, 2 * k + p] + u1[v, k]
                u0[v, 2 * k + p] = value
                l0.put_masked(v, 2 * k + p, value)
        return c

    loop(0, l1.n, add0, 0)
    for _ in range(2):
        l0.sweep(r0, u0)


def pick(row, ids):
    return jnp.take_along_axis(
        jnp.broadcast_to(row, ids.shape), ids, axis=1, mode="promise_in_bounds"
    )


def spread_chunk(d, out, chunk):
    value = chunk[...]
    for i in range(d.n):
        out[i] = value


def pack_planes(d, place, gathered, count, put):
    first = place[3]

    def body(p, c):
        lane = lanes((8, d.cy))
        for o in range(d.packed):
            value = jnp.zeros((8, d.cy), F32)
            for s in range(d.slots):
                rg = o * d.slots + s
                if rg >= d.groups:
                    break
                block, at = rg * 8 // d.cx, rg * 8 % d.cx
                x = gathered[block, p, at : at + 8, :]
                x = turn(x, lax.rem(REACH * s - first + d.cy, d.cy), 1)
                keep = (lane >= REACH * s) & (lane < REACH * (s + 1))
                value = jnp.where(keep, x, value)
            put(p * d.packed + o, value)
        return c

    loop(0, count, body, 0)


def pack_kernel(d, place, *refs):
    *pieces, out = refs
    for t, piece in enumerate(pieces):
        def put(at, value, t=t):
            out[t * d.piece * d.packed + at] = value
        pack_planes(d, place, piece, d.piece, put)


def layout(d):
    n0 = d.layers
    return [(n0, None, n0), (4, None, 2 * n0), (n0, 0, 0), (n0, 1, 0), (n0, None, 0)]


def segments(d):
    out, start = [], 0
    for count, v, there in layout(d):
        at, end = start, start + count
        while at < end:
            piece = at // d.piece
            stop = min(end, (piece + 1) * d.piece)
            out.append((piece, at - piece * d.piece, stop - at, v, there + at - start))
            at = stop
        start = end
    return out


def edge_kernel(d, got, out):
    n0, cx = d.layers, d.cx
    for g in range(d.ngx):
        at = slice(g * cx, (g + 1) * cx)
        total = loop(0, n0, lambda k, t: t + got[g, k], jnp.zeros((cx, d.cy), F32))
        mask = got[g, n0 + 2]
        out[0, at, :], out[1, at, :], out[2, at, :] = mask, got[g, n0 + 3], total * mask


def setup_kernel(d, place, *rest):
    all_gathered, bulk, last_ref, rest = rest[:PIECES], rest[PIECES], rest[PIECES + 1], rest[PIECES + 2 :]
    (f, g0, s0, i0, f0, g1, s1, i1, f1, low, strip_ids) = rest[:11]
    (u0, r1, u1, r2, u2, big) = rest[11:17]
    (win, chunk, e2, pack, mu0, fw0, mu1, fw1, mu2, fw2) = rest[17:]
    n0, n1, rows, cy, cx = d.layers, d.layers // 2, d.rows, d.cy, d.cx
    off, is_left = place[4], place[5]
    if d.parts > 2 * d.ngx:
        chunk[...] = jnp.zeros(chunk.shape, F32)

    def window(gathered, packed, p, put):
        lane = lanes((8, cy))
        off_own = lax.rem(off + cy, cy)
        own = jnp.where(is_left == 1, (lane >= off).astype(jnp.int32), (lane < cy + off).astype(jnp.int32)) == 1
        lo = jnp.where(is_left == 1, off - REACH, cy + off)
        near = (lane >= lo) & (lane < lo + REACH)
        for rg in range(d.groups):
            block, at = rg * 8 // cx, rg * 8 % cx
            mid = turn(gathered[block, p, at : at + 8, :], off_own, 1)
            o, s = rg // d.slots, rg % d.slots
            side = turn(packed[p * d.packed + o], lax.rem(lo - REACH * s + 2 * cy, cy), 1)
            put(slice(rg * 8, rg * 8 + 8), jnp.where(own, mid, jnp.where(near, side, 0.0)))

    for piece, first, count, v, there in segments(d):
        def fill(t, c, piece=piece, first=first, v=v, there=there):
            def put(at, value):
                if v is None:
                    win[there + t, at, :] = value
                else:
                    f[v, there + t, at, :] = value
            packed = last_ref if piece == PIECES - 1 else bulk.at[pl.ds(piece * d.piece * d.packed, d.piece * d.packed)]
            window(all_gathered[piece], packed, first + t, put)
            return c

        loop(0, count, fill, 0)

    cpl, frc, msk = win[2 * n0], win[2 * n0 + 1], win[2 * n0 + 2]
    low[4] = msk
    low[5] = win[2 * n0 + 3]
    low[3] = frc * cpl * msk
    mask = low.at[4]
    nil = jnp.zeros((rows, cy), F32)
    f0[0] = nil
    f0[n0] = nil

    def faces(k, c):
        f0[k + 1] = 0.5 * (win[k] + win[k + 1]) * mask[...]
        return c

    loop(0, n0 - 1, faces, 0)

    def diag(k, extra):
        m = mask[...]
        sp = win[n0 + k]
        s0[k] = sp * m
        inner = f0[k] + f0[k + 1] + 4.0 * sp
        if extra is not None:
            inner = inner + extra
        value = m * inner + (1.0 - m)
        g0[k] = value
        return value

    i0[0] = 1.0 / diag(0, frc)

    def factor0(k, prev):
        face = f0[k]
        inv = 1.0 / (diag(k, None) - face * face * prev)
        i0[k] = inv
        return inv

    loop(1, n0, factor0, i0[0])

    def fold(k, total):
        g1[k] = g0[2 * k] + g0[2 * k + 1] - 2.0 * f0[2 * k + 1]
        s = s0[2 * k] + s0[2 * k + 1]
        s1[k] = s
        f1[k] = f0[2 * k]
        return total + s

    low[1] = loop(0, n1, fold, nil)
    f1[n1] = nil
    i1[0] = 1.0 / g1[0]

    def factor1(k, prev):
        face = f1[k]
        inv = 1.0 / (g1[k] - face * face * prev)
        i1[k] = inv
        return inv

    loop(1, n1, factor1, i1[0])
    diag2 = 4.0 * low[1] + mask[...] * win[2 * n0 + 1] + n0 * (1.0 - mask[...])
    low[0] = diag2
    low[2] = 1.0 / diag2

    lane = lanes((cx, cy))
    packed_ids = jnp.zeros((cx, cy), F32)
    for g in range(d.ngx):
        part = turn(low[5, g * cx : (g + 1) * cx, :], (d.strip * g - d.halo) % cy, 1)
        packed_ids = jnp.where(lane // d.strip == g, part, packed_ids)
    strip_ids[...] = packed_ids

    levels = level_set(d, (g0, s0, i0, f0, g1, s1, i1, f1, low), mu0, fw0, mu1, fw1, mu2, fw2)
    for one in levels:
        one.clear_rim()
    descend(d, levels, f, u0, r1, u1, r2, u2, strip_ids, e2, pack, chunk)
    spread_chunk(d, big, chunk)


COLUMN = 9
SENT = 6
SOME = 256.0


def inside_of(d):
    shape = (d.cx, d.cy)
    row = lax.broadcasted_iota(jnp.int32, shape, 0)
    lane = lanes(shape)
    return (row > 0, row < d.cx - 1, lane > 0, lane < d.cy - 1)


def column_kernel(d, place, got, own_edges, near_edges, opposite, out, table, tmp):
    n0, cx, cy = d.layers, d.cx, d.cy
    at_misc = n0
    inside = inside_of(d)
    nil = jnp.zeros((cx, cy), F32)
    is_left = place[5]
    table[...] = jnp.zeros(table.shape, F32)
    for g in range(d.ngx):
        fr, cp = got[g, at_misc + 1], got[g, at_misc]
        rows_of = lambda g: slice(g * cx, (g + 1) * cx)
        own = [own_edges[t, rows_of(g), :] for t in range(3)]

        def around(t):
            q = own[t]
            up = own_edges[t, rows_of(g - 1), :] if g > 0 else nil
            down = own_edges[t, rows_of(g + 1), :] if g + 1 < d.ngx else nil
            near = near_edges[t, rows_of(g), :]
            other = opposite[t, rows_of(g), :]
            left = jnp.where(is_left == 1, near, other)
            right = jnp.where(is_left == 1, other, near)
            return (
                jnp.where(inside[0], turn(q, 1, 0), turn(up, 1, 0)),
                jnp.where(inside[1], turn(q, cx - 1, 0), turn(down, cx - 1, 0)),
                jnp.where(inside[2], turn(q, 1, 1), turn(left, 1, 1)),
                jnp.where(inside[3], turn(q, cy - 1, 1), turn(right, cy - 1, 1)),
            )

        m, ids, s2 = own
        m_d, ids_d, s_d = around(0), around(1), around(2)
        g2 = 4.0 * s2 + m * fr + n0 * (1.0 - m)
        cross = fr * cp * m
        at = slice(g * cx, (g + 1) * cx)
        out[0, at, :], out[1, at, :], out[2, at, :] = g2, s2, cross
        out[3, at, :] = ids + SOME * m
        out[4, at, :] = jnp.where(inside[2], m_d[3] * (1.0 + ids_d[3]), m_d[2] * (1.0 + ids_d[2]))
        weight3, weight4 = g2, g2
        for t in range(4):
            weight3 = weight3 - jnp.where(inside[t] & (ids_d[t] == ids), s2 * m_d[t], 0.0)
            weight4 = weight4 - jnp.where(inside[t], s_d[t] * m, 0.0)
            tmp[3 + t] = jnp.where(inside[t], 0.0, s_d[t] * m)
        tmp[0], tmp[1], tmp[2] = weight3, cross, weight4
        ids_row = lambda r: own_edges[1, g * cx + r : g * cx + r + 1, :]
        acc = segment_acc(d, ids_row, lambda _, r: tmp[0, r : r + 1, :], 1)
        out[5, at, :] = jnp.broadcast_to(acc[0].T.sum(axis=0, keepdims=True), (cx, cy))

        @pl.when(place[1] == g)
        def _():
            def one(t, c):
                acc = segment_acc(d, ids_row, lambda _, r: tmp[1 + t, r : r + 1, :], 1)
                table[pl.ds(2 + t, 1), :] = acc[0].T.sum(axis=0, keepdims=True)
                return c

            loop(0, 6, one, 0, 1)


def apply_block(d, cols, pos, g, rows, tmp, inside):
    at = pl.ds(pl.multiple_of(g * d.cx, d.cx), d.cx)
    shape = (d.cx, d.cy)
    ids = cols[pos, 3, at, :].astype(jnp.int32)
    here = [pick(rows[0][v], ids) for v in range(2)]
    side = [jnp.zeros(shape, F32), jnp.zeros(shape, F32)]
    for t in range(4):
        code = cols[pos, 4 + t, at, :].astype(jnp.int32) - 1
        live = code >= 0
        code = jnp.maximum(code, 0)
        for v in range(2):
            value = jnp.where(inside[t], pick(rows[0][v], code), pick(rows[1 + t][v], code))
            side[v] = side[v] + jnp.where(live, value, 0.0)
    g2, s2, cross = cols[pos, 0, at, :], cols[pos, 1, at, :], cols[pos, 2, at, :]
    for v in range(2):
        tmp[v] = g2 * here[v] + cross * here[1 - v] - s2 * side[v]
    acc = segment_acc(
        d,
        lambda r: cols[pos, 3, pl.ds(g * d.cx + r, 1), :],
        lambda t, r: tmp[t, r : r + 1, :],
        2,
    )
    return [acc[v].T.sum(axis=0, keepdims=True) for v in range(2)]


def diagonal(d, cols, pos, g):
    x = cols[pos, 8, pl.ds(g * d.cx, 1), :]
    return jnp.where(x == 0.0, 1.0, x)


def clip(x, top):
    return jnp.clip(x, 0, top - 1)


def point_first(d, step, place, parts, extra, *rest):
    if step == 0:
        near, column, opposite, far, cols, r3, big, tmp, chunk = rest
        at_near = jnp.where(place[5] == 1, 0, 2)

        rows, cy = d.rows, d.cy
        line = lax.broadcasted_iota(jnp.int32, (rows, cy), 0)
        lane = lanes((rows, cy))
        for source, pos in ((column, 1), (far, 3), (near, at_near), (opposite, 2 - at_near)):
            cols[pos, 0], cols[pos, 1], cols[pos, 2] = source[0], source[1], source[2]
            cols[pos, 8] = source[5]
            both = source[3]
            live = both >= SOME
            ids = both - jnp.where(live, SOME, 0.0)
            code = jnp.where(live, 1.0 + ids, 0.0)
            cols[pos, 3] = ids
            cols[pos, 4] = jnp.where(line == 0, 0.0, turn(code, 1, 0))
            cols[pos, 5] = jnp.where(line == rows - 1, 0.0, turn(code, rows - 1, 0))
            cols[pos, 6] = jnp.where(lane == 0, source[4], turn(code, 1, 1))
            cols[pos, 7] = jnp.where(lane == cy - 1, source[4], turn(code, cy - 1, 1))
    else:
        cols, r3, big, tmp, chunk = rest
    ngx, ngy = d.ngx, d.ngy
    for v in range(2):
        for g in range(ngx):
            total = parts[0:ngy, v * ngx + g, :]
            for i in range(1, ngx):
                total = total + parts[i * ngy : (i + 1) * ngy, v * ngx + g, :]
            r3[v, g * ngy : (g + 1) * ngy, :] = total
    gx, gy = place[1], place[2]
    up, down = clip(gx - 1, ngx), clip(gx + 1, ngx)
    spots = (
        (1, gx, gy),
        (1, up, gy),
        (1, down, gy),
        (0, gx, clip(gy - 1, ngy)),
        (2, gx, clip(gy + 1, ngy)),
    )
    right, diag, rows = [], [], []
    for pos, g, c in spots:
        right.append([r3[v, pl.ds(g * ngy + c, 1), :] for v in range(2)])
        diag.append(diagonal(d, cols, pos, g))
        rows.append([POINT_WEIGHT * right[-1][v] / diag[-1] for v in range(2)])
    image = apply_block(d, cols, 1, gx, rows, tmp, inside_of(d))
    count = chunk.shape[0]
    chunk[2:count, :] = extra[2:count, :]
    for v in range(2):
        chunk[v : v + 1, :] = rows[0][v] + POINT_WEIGHT * (right[0][v] - image[v]) / diag[0]
    spread_chunk(d, big, chunk)


def correct_columns(d, place, parts, table, r3, cols, low, u2, y3, y4, y5, tmp):
    n, ngx, ngy = d.n, d.ngx, d.ngy
    gy, off, is_left = place[2], place[4], place[5]
    cross, inner = table[:, 2, :], table[:, 3, :]
    sides = [table[:, 4 + t, :] for t in range(4)]
    shape = (n, d.cy)

    def total(x):
        return jnp.broadcast_to(x.sum(axis=1, keepdims=True), shape)

    def couple(values):
        return (
            turn(values[1], ngy, 0)
            + turn(values[0], n - ngy, 0)
            + turn(values[3], 1, 0)
            + turn(values[2], n - 1, 0)
        )

    y2 = [parts[:, v, :] for v in range(2)]
    right = []
    for v in range(2):
        local = total(r3[v] - (inner * y2[v] + cross * y2[1 - v]))
        right.append(local + couple([total(s * y2[v]) for s in sides]))
    diag4, cross4 = total(inner), total(cross)
    sides4 = [total(s) for s in sides]
    x = [COARSE_WEIGHT * right[v] / diag4 for v in range(2)]
    for _ in range(CSWEEPS - 1):
        x = [
            x[v]
            + COARSE_WEIGHT
            * (right[v] - (diag4 * x[v] + cross4 * x[1 - v] - couple([s * x[v] for s in sides4])))
            / diag4
            for v in range(2)
        ]
    for v in range(2):
        y3[v] = y2[v] + x[v]

    def column(pos):
        far = jnp.where(is_left == 1, -2, 2)
        return gy + jnp.where(pos == 3, far, pos - 1)

    inside = inside_of(d)

    def relax(pos, g, rows, c, q):
        image = apply_block(d, cols, pos, g, rows, tmp.at[q], inside)
        diag = diagonal(d, cols, pos, g)
        at = pl.ds(g * ngy + c, 1)
        return [
            rows[0][v] + POINT_WEIGHT * (r3[v, at, :] - image[v]) / diag for v in range(2)
        ]

    def fourth(b, carry):
        for q in range(2):
            pos, g = lax.div(2 * b + q, ngx), lax.rem(2 * b + q, ngx)
            c = column(pos)
            get = lambda g, c: [
                y3[v, pl.ds(clip(g, ngx) * ngy + clip(c, ngy), 1), :] for v in range(2)
            ]
            rows = [get(g, c), get(g - 1, c), get(g + 1, c), get(g, c - 1), get(g, c + 1)]
            new = relax(pos, g, rows, clip(c, ngy), q)
            for v in range(2):
                y4[v, pl.ds(pos * ngx + g, 1), :] = new[v]
        return carry

    def fifth(b, carry):
        for q in range(2):
            t, g = lax.div(2 * b + q, ngx), lax.rem(2 * b + q, ngx)
            pos = t + 1 - is_left
            west = jnp.where(pos == 0, 3, pos - 1)
            east = jnp.where(pos == 2, 3, pos + 1)
            get = lambda g, p: [
                y4[v, pl.ds(p * ngx + clip(g, ngx), 1), :] for v in range(2)
            ]
            rows = [get(g, pos), get(g - 1, pos), get(g + 1, pos), get(g, west), get(g, east)]
            new = relax(pos, g, rows, clip(column(pos), ngy), q)
            for v in range(2):
                y5[v, pl.ds(t * ngx + g, 1), :] = new[v]
        return carry

    lax.fori_loop(0, 2 * ngx, fourth, 0)
    lax.fori_loop(0, ngx, fifth, 0)

    block = (d.cx, d.cy)
    lane = lanes(block)
    own = jnp.where(is_left == 1, (lane >= off).astype(jnp.int32), (lane < d.cy + off).astype(jnp.int32)) == 1
    for g in range(ngx):
        at = slice(g * d.cx, (g + 1) * d.cx)
        ids = low[5, at, :].astype(jnp.int32)
        for v in range(2):
            here = pick(y5[v, pl.ds(is_left * ngx + g, 1), :], ids)
            there = pick(y5[v, pl.ds((1 - is_left) * ngx + g, 1), :], ids)
            u2[v, 0, at, :] = u2[v, 0, at, :] + jnp.where(own, here, there)


def grid_totals(d, dots, count):
    x = dots[:, 2, :].sum(axis=0, keepdims=True)
    lane = lanes((1, d.cy))
    return [
        jnp.broadcast_to(
            jnp.where(lane == t, x, 0.0).sum(axis=1, keepdims=True), (1, d.cy)
        )
        for t in range(count)
    ]


def column_of(d, dots, step, norm=None):
    values = grid_totals(d, dots, step + 2 + (step == 0))
    if step == 0:
        square = values[2]
        norm = jnp.sqrt(square)
        inner, height = [values[0] / square], values[1] / square
    else:
        inner, height = [values[0] / norm] + values[1:-1], values[-1]
    for value in inner:
        height = height - value * value
    return inner + [jnp.sqrt(height)], norm


def step_kernel(d, step, last, *refs):
    it = iter(refs)
    take = lambda count: [next(it) for _ in range(count)]
    (place,) = take(1)
    coefs = take(9)
    (strip_ids, r_in, u0i, r1i, u1i, r2i, u2i) = take(7)
    (parts, table, r3, cols) = take(4)
    norm_in = take(1)[0] if step > 1 else None
    olds_v = take(step)
    olds_z = take(step)
    if step:
        (v_out, col) = take(2)
    (z_out,) = take(1)
    if last:
        (dots_out, big) = take(2)
        w = take(1)[0]
        u0n = None
    else:
        (w, u0n, r1n, u1n, r2n, u2n, dots_out, big) = take(8)
    (u0, u1, u2, y3, y4, y5, tmp, chunk, e2, pack, mu0, fw0, mu1, fw1, mu2, fw2) = take(16)
    low = coefs[8]
    levels = level_set(d, coefs, mu0, fw0, mu1, fw1, mu2, fw2)
    for one in levels:
        one.clear_rim()
    n0, n1 = d.layers, d.layers // 2

    for v in range(2):
        u2[v, 0] = u2i[v, 0]
    correct_columns(d, place, parts, table, r3, cols, low, u2, y3, y4, y5, tmp)
    if not last and d.parts > 2 * d.ngx:
        chunk[...] = jnp.zeros(chunk.shape, F32)

    ascend(d, levels, r_in, u0, u0i, r1i, u1, u1i, r2i, u2)

    l0 = levels[0]
    if step:
        norm = norm_in[step : step + 1, :] if step > 1 else None
        column, norm = column_of(d, parts, step - 1, norm)
        height = column[-1]
        if step == 1:
            inner, scale = [column[0]], 1.0 / (height * norm)
        else:
            inner, scale = [column[0] / norm] + column[1:-1], 1.0 / height
        for t, value in enumerate(column + [norm]):
            col[t : t + 1, :] = value

    def scaled(k, c):
        for v in range(2):
            z = u0[v, k]
            if step:
                vec = r_in[v, k]
                for t in range(step):
                    vec = vec - inner[t] * olds_v[t][v, k]
                    z = z - inner[t] * olds_z[t][v, k]
                v_out[v, k] = vec * scale
                z = z * scale
            z_out[v, k] = z
            l0.put_masked(v, k, z)
        return c

    loop(0, n0, scaled, 0)
    basis = list(olds_v) + [v_out if step else r_in]

    own = own_lanes(d, (8, d.cy))

    def fold(x):
        total = x[0:8]
        for t in range(1, d.groups):
            total = total + x[8 * t : 8 * t + 8]
        return total

    def image(k, acc, bottom=False):
        acc = list(acc)
        for v in range(2):
            value = l0.apply(z_out, v, k, bottom)
            w[v, k] = value
            for t, vec in enumerate(basis):
                acc[t] = acc[t] + fold(vec[v, k] * value)
            acc[step + 1] = acc[step + 1] + fold(value * value)
            if step == 0:
                acc[2] = acc[2] + fold(r_in[v, k] * r_in[v, k])
        return tuple(acc)

    nil = jnp.zeros((8, d.cy), F32)
    acc = image(0, (nil,) * (step + 2 + (step == 0)), True)
    acc = loop(1, n0, image, acc)
    lane = lanes((1, d.cy))
    row = jnp.zeros((1, d.cy), F32)
    for t, value in enumerate(acc):
        value = jnp.where(own, value, 0.0).sum(axis=0, keepdims=True)
        row = jnp.where(lane == t, value.sum(axis=1, keepdims=True), row)
    dots_out[...] = jnp.zeros(dots_out.shape, F32)
    dots_out[2:3, :] = row
    if last:
        spread_chunk(d, big, dots_out)
    else:
        descend(d, levels, w, u0n, r1n, u1n, r2n, u2n, strip_ids, e2, pack, chunk)
        spread_chunk(d, big, chunk)


def least_squares(columns, initial_norm):
    count = len(columns)
    rows = [[columns[c][r] for c in range(count)] for r in range(count + 1)]
    target = [initial_norm] + [jnp.zeros_like(initial_norm) for _ in range(count)]
    for p in range(count):
        top, low = rows[p][p], rows[p + 1][p]
        radius = jnp.sqrt(top * top + low * low)
        cosine, sine = top / radius, low / radius
        for c in range(p, count):
            upper, lower = rows[p][c], rows[p + 1][c]
            rows[p][c] = cosine * upper + sine * lower
            rows[p + 1][c] = cosine * lower - sine * upper
        upper, lower = target[p], target[p + 1]
        target[p] = cosine * upper + sine * lower
        target[p + 1] = cosine * lower - sine * upper
    weights = [None] * count
    for p in reversed(range(count)):
        partial = target[p]
        for c in range(p + 1, count):
            partial = partial - rows[p][c] * weights[c]
        weights[p] = partial / rows[p][p]
    return weights


def final_kernel(d, g0, s0, i0, f0, low, f, dots, *refs):
    cols, zs = refs[: ITERS - 1], refs[ITERS - 1 : 2 * ITERS - 1]
    out, x, res, mu0 = refs[2 * ITERS - 1 :]
    n0 = d.layers
    nil = jnp.zeros((1, d.cy), F32)
    columns = []
    norm = cols[0][2:3, :]
    for j in range(ITERS):
        if j + 1 < ITERS:
            column = [cols[j][t : t + 1, :] for t in range(j + 2)]
        else:
            column, _ = column_of(d, dots, j, norm)
        columns.append(column + [nil] * (ITERS - 1 - j))
    weights = least_squares(columns, norm)
    weights[0] = weights[0] / norm
    l0 = Level(d, n0, g0, s0, i0, f0, low.at[3], low.at[4], mu0, None)
    l0.clear_rim()

    def combine(k, c):
        for v in range(2):
            value = weights[0] * zs[0][v, k]
            for j in range(1, ITERS):
                value = value + weights[j] * zs[j][v, k]
            x[v, k] = value
            l0.put_masked(v, k, value)
        return c

    loop(0, n0, combine, 0)

    def rest(k, bottom):
        for v in range(2):
            res[v, k] = f[v, k] - l0.apply(x, v, k, bottom)

    rest(0, True)
    loop(1, n0, lambda k, c: (rest(k, False), c)[1], 0)

    per = 4 * n0 // d.ngx
    lane = lanes((d.cx, d.cy))
    for q in range(d.ngx):
        shift = (d.strip * q - d.halo) % d.cy
        keep = lane // d.strip == q

        def place_plane(p, c, q=q, shift=shift, keep=keep):
            plane = q * per + p
            for dest in range(d.ngx):
                at = slice(dest * d.cx, (dest + 1) * d.cx)
                source = x if (q * per) < 2 * n0 else res
                local = plane if (q * per) < 2 * n0 else plane - 2 * n0
                v = (q * per) // n0 % 2
                value = turn(source[v, local - v * n0, at, :], shift, 1)
                if q == 0:
                    out[dest, p] = value
                else:
                    out[dest, p] = jnp.where(keep, value, out[dest, p])
            return c

        loop(0, per, place_plane, 0)


def unpack_kernel(d, got, solution_out, residual_out):
    n0 = d.layers
    per = 4 * n0 // d.ngx
    lane = lanes((d.cx, d.cy))
    for q in range(d.ngx):
        def body(p, c, q=q):
            value = None
            for src in range(d.ngx):
                part = turn(got[src, p], (d.strip * (src - q)) % d.cy, 1)
                value = part if value is None else jnp.where(lane // d.strip == src, part, value)
            first = q * per
            target = solution_out if first < 2 * n0 else residual_out
            v = first // n0 % 2
            target[v, first % n0 + p] = value
            return c

        loop(0, per, body, 0)


def body(forcing, viscosity, spread, coupling, friction, ice_mask, aggregates):
    ngx, ngy = lax.axis_size("gx"), lax.axis_size("gy")
    layers, cx, cy = viscosity.shape
    d = Dims(ngx, ngy, layers, cx, cy)
    both = ("gx", "gy")
    gx, gy = lax.axis_index("gx"), lax.axis_index("gy")
    is_left = gx < ngx // 2
    off = d.halo - d.strip * gx
    first = jnp.where(is_left, cy - REACH, 0)
    place = jnp.stack([gx * ngy + gy, gx, gy, first, off, is_left.astype(jnp.int32)]).astype(jnp.int32)

    def sided(by):
        return [
            (i * ngy + j, i * ngy + to)
            for i in range(ngx)
            for j in range(ngy)
            for to in [j + by if i < ngx // 2 else j - by]
            if 0 <= to < ngy
        ]

    small = jnp.stack([coupling, friction, ice_mask.astype(F32), aggregates.astype(F32)])
    pieces, start = [[] for _ in range(PIECES)], 0
    for part in [spread, small, forcing.reshape(2 * layers, cx, cy), viscosity]:
        end = start + part.shape[0]
        for t in range(PIECES):
            low, high = max(start, t * d.piece), min(end, (t + 1) * d.piece)
            if low < high:
                pieces[t].append(part[low - start : high - start])
        start = end
    gathered, packed = [], []
    for t in range(PIECES):
        got = lax.all_gather(jnp.concatenate(pieces[t]), "gx")
        if t == 1:
            got, near_edges, opposite_edges = lax.optimization_barrier(
                (got, near_edges, opposite_edges)
            )
        gathered.append(got)
        if t == 0:
            (edges,) = call(
                functools.partial(edge_kernel, d), [(3, d.rows, cy)], [got], name="edge"
            )
            opposite_edges = lax.ppermute(edges, both, sided(-1))
            near_edges = lax.ppermute(edges, both, sided(1))
        if t >= PIECES - 2:
            use = gathered[t:] if t == PIECES - 1 else gathered
            tiles = len(use) * d.piece * d.packed
            (sent,) = call(
                functools.partial(pack_kernel, d),
                [(tiles, 8, cy)],
                [place, *use],
                name="pack",
            )
            packed.append(lax.ppermute(sent, both, sided(1)))
    column, table_own = call(
        functools.partial(column_kernel, d),
        [(SENT, d.rows, cy), (8, cy)],
        [place, gathered[0], edges, near_edges, opposite_edges],
        [(7, cx, cy)],
        name="column",
    )
    near = lax.ppermute(column, both, sided(1))
    opposite = lax.ppermute(column, both, sided(-1))
    far = lax.ppermute(column, both, sided(2))

    n0, n1, rows = layers, layers // 2, d.rows
    fields = [field(d, n0), field(d, n1), field(d, n1), field(d, 1), field(d, 1)]
    big_shape = lambda count: (d.n, count, cy)
    state_work = [(2, rows, cy), (2, cx, cy)] + work_shapes(d)
    outs = call(
        functools.partial(setup_kernel, d),
        [field(d, n0)] + coef_shapes(d) + [(cx, cy)] + fields + [big_shape(d.parts)],
        [place, *gathered, *packed],
        [(2 * n0 + 4, rows, cy), (d.parts, cy)] + state_work,
        name="setup",
    )
    f, coefs, strip_ids, state, big = outs[0], outs[1:10], outs[10], outs[11:16], outs[16]

    def share(x):
        return lax.all_to_all(x, both, 0, 0)

    big, near, opposite, far = lax.optimization_barrier((big, near, opposite, far))
    parts = share(big)
    extra = table_own
    vs, zs, norms = [f], [], []
    pair = (2, d.n, cy)
    r_in = f
    for step in range(ITERS):
        count = 4 if step else 8
        outs = call(
            functools.partial(point_first, d, step),
            ([] if step else [(4, COLUMN, rows, cy)]) + [pair, big_shape(count)],
            [place, parts, extra] + ([cols] if step else [near, column, opposite, far]),
            [(2, cx, cy), (count, cy)],
            name="point_first",
        )
        r3, big = outs[-2:]
        parts = share(big)
        if step == 0:
            cols, table = outs[0], parts
        last = step + 1 == ITERS
        outs_shapes = [field(d, n0), (8, cy)] if step else []
        outs_shapes += [field(d, n0)]
        if last:
            outs_shapes += [(4, cy), big_shape(4)]
        else:
            outs_shapes += [field(d, n0)] + fields + [(4, cy), big_shape(d.parts)]
        scratch = [field(d, n0)] if last else []
        scratch += [field(d, n0), field(d, n1), field(d, 1), pair]
        scratch += [(2, 4 * ngx, cy), (2, 2 * ngx, cy), (2, 2, cx, cy), (d.parts, cy)] + state_work
        outs = call(
            functools.partial(step_kernel, d, step, last),
            outs_shapes,
            [place, *coefs, strip_ids, r_in, *state, parts, table, r3, cols]
            + norms[step - 2 : step - 1 if step > 1 else 0]
            + (vs[:step] + zs),
            scratch,
            name="step",
        )
        if step:
            vs.append(outs[0])
            norms.append(outs[1])
            outs = outs[2:]
        zs.append(outs[0])
        if last:
            dots_all = share(outs[2])
        else:
            r_in, state, extra = outs[1], outs[2:7], outs[7]
            parts = share(outs[8])

    (out,) = call(
        functools.partial(final_kernel, d),
        [(ngx, 4 * n0 // ngx, cx, cy)],
        [*coefs[:4], coefs[8], f, dots_all, *norms, *zs],
        [field(d, n0), field(d, n0), (2, n0, rows + 16, cy)],
        name="final",
    )
    got = lax.all_to_all(out, "gx", 0, 0)
    return tuple(
        call(
            functools.partial(unpack_kernel, d),
            [forcing.shape, forcing.shape],
            [got],
            name="unpack",
        )
    )


def solution(mesh):
    return jax.shard_map(
        body,
        mesh=mesh,
        in_specs=(
            P(None, None, "gx", "gy"),
            P(None, "gx", "gy"),
            P(None, "gx", "gy"),
            P("gx", "gy"),
            P("gx", "gy"),
            P("gx", "gy"),
            P("gx", "gy"),
        ),
        out_specs=(P(None, None, "gx", "gy"), P(None, None, "gx", "gy")),
        check_vma=False,
    )
```
